32 devices in a mesh: rep: 1 (over z), kv2: 4 (over y), kv: 8 (over x, core).
Axes of the slice: x: 4, y: 4, z: 1, core: 2. Of those that a mesh axis runs over, the one named last changes fastest.
The devices are a block of a 4x4x8 slice.
Arguments:
- x_embed: bfloat16 [2, 1024, 2048], P(None, ('rep', 'kv2', 'kv'))
- w_query: bfloat16 [2, 2048, 2048], replicated
- w_key: bfloat16 [2, 2048, 512], replicated
- w_value: bfloat16 [2, 2048, 512], replicated
- w_out: bfloat16 [2, 2048, 2048], replicated
- w_up: bfloat16 [2, 2048, 8192], replicated
- w_down: bfloat16 [2, 8192, 2048], replicated
- k_pool: bfloat16 [6656, 2, 16, 8, 64], P(('rep', 'kv2', 'kv'))
- v_pool: bfloat16 [6656, 2, 16, 8, 64], P(('rep', 'kv2', 'kv'))
- old_table: int32 [1024, 3], P(('rep', 'kv2', 'kv'))
- seq_len: int32 [1024], P(('rep', 'kv2', 'kv'))
- src_slot: int32 [512], P(('rep', 'kv2', 'kv'))
- dst_slot: int32 [512], P(('rep', 'kv2', 'kv'))
Outputs:
- output 1: bfloat16 [2, 1024, 2048], P(None, ('rep', 'kv2', 'kv'))
- output 2: bfloat16 [6656, 2, 16, 8, 64], P(('rep', 'kv2', 'kv'))
- output 3: bfloat16 [6656, 2, 16, 8, 64], P(('rep', 'kv2', 'kv'))
All inputs are finite; a program needn't handle non-finite values.
Results may differ from the reference program's by a relative error of at most 0.0135625.
Values are sent between devices in bfloat16 or wider.
A program may use at most 768 MiB of HBM per device.

```python
import jax
import jax.numpy as jnp
from jax import lax

MESH_ROWS = 4
MESH_COLS = 8
SEQ_DEV = 32
PAGES = 3
MIG_DEV = 16
D = 2048
HEADS = 32
KV_HEADS = 8
HEAD = 64
FF = 8192
PAGE = 16
LAYERS = 2
DEVICES_PART = MESH_ROWS * MESH_COLS
ROW_SEQS = MESH_COLS * SEQ_DEV
BATCH = DEVICES_PART * SEQ_DEV
SLOTS = 2 * SEQ_DEV * PAGES + MIG_DEV
MOVES = DEVICES_PART * MIG_DEV
ALL_SLOTS = DEVICES_PART * SLOTS


def draw_layout(key):
    keys_list = jax.random.split(key, 7)
    n_pages = jax.random.randint(keys_list[0], (BATCH,), 2, PAGES + 1).at[0].set(PAGES)
    fill_len = jax.random.randint(keys_list[1], (BATCH,), 0, PAGE - 1).at[0].set(PAGE - 2)
    seq_len = (n_pages - 1) * PAGE + fill_len
    dev_ids = jnp.arange(DEVICES_PART, dtype=jnp.int32)
    local_ids = jnp.arange(SLOTS, dtype=jnp.int32)
    slot_caps = jnp.where(dev_ids % MESH_COLS % 2 == 0, SLOTS - MIG_DEV, (SLOTS - MIG_DEV) // 4)
    move_ids = jnp.arange(MOVES, dtype=jnp.int32)
    src_dev = move_ids // MIG_DEV
    target = 2 * (jax.random.permutation(keys_list[2], MOVES) // (2 * MIG_DEV))
    target = jnp.where(target == src_dev, (target + 2) % DEVICES_PART, target)
    order_t = jnp.argsort(target * MOVES + move_ids)
    group_start = jnp.searchsorted(target[order_t], target)
    rank_in = jnp.argsort(order_t) - group_start
    outside = (local_ids[None, :] >= slot_caps[:, None]).astype(jnp.int32)
    prio_dst = jax.random.permutation(keys_list[3], ALL_SLOTS).reshape(DEVICES_PART, SLOTS) + outside * ALL_SLOTS
    dst_slot = target * SLOTS + jnp.argsort(prio_dst, axis=1)[target, rank_in]
    prio_src = jax.random.permutation(keys_list[4], ALL_SLOTS).reshape(DEVICES_PART, SLOTS) + (1 - outside) * ALL_SLOTS
    src_slot = (dev_ids[:, None] * SLOTS + jnp.argsort(prio_src, axis=1)[:, :MIG_DEV]).reshape(MOVES)
    marked = jnp.zeros((ALL_SLOTS,), jnp.int32).at[dst_slot].set(1).reshape(MESH_ROWS, MESH_COLS * SLOTS)
    inside = (1 - outside).reshape(MESH_ROWS, MESH_COLS * SLOTS)
    prio_new = jax.random.permutation(keys_list[5], ALL_SLOTS).reshape(MESH_ROWS, MESH_COLS * SLOTS) + jnp.where(marked == 1, 0, jnp.where(inside == 1, ALL_SLOTS, 2 * ALL_SLOTS))
    slot_order = jnp.argsort(prio_new, axis=1)
    pages_row = n_pages.reshape(MESH_ROWS, ROW_SEQS, 1)
    page_ids = jnp.arange(PAGES, dtype=jnp.int32)[None, None, :]
    is_valid = (page_ids < pages_row).reshape(MESH_ROWS, ROW_SEQS * PAGES)
    is_last = (page_ids == pages_row - 1).reshape(MESH_ROWS, ROW_SEQS * PAGES)
    n_cells = BATCH * PAGES
    cell_key = jax.random.permutation(keys_list[6], n_cells).reshape(MESH_ROWS, ROW_SEQS * PAGES) + jnp.where(is_last, 0, jnp.where(is_valid, n_cells, 2 * n_cells))
    cell_rank = jnp.argsort(jnp.argsort(cell_key, axis=1), axis=1)
    row_base = jnp.arange(MESH_ROWS, dtype=jnp.int32)[:, None] * (MESH_COLS * SLOTS)
    new_slot = jnp.take_along_axis(slot_order, cell_rank, axis=1) + row_base
    new_table = jnp.where(is_valid, new_slot, -1).reshape(BATCH, PAGES)
    slot_move = jnp.full((ALL_SLOTS,), -1, jnp.int32).at[dst_slot].set(move_ids)
    move_idx = slot_move[jnp.maximum(new_table, 0)]
    old_table = jnp.where((new_table >= 0) & (move_idx >= 0), src_slot[jnp.maximum(move_idx, 0)], new_table)
    return old_table.astype(jnp.int32), seq_len.astype(jnp.int32), src_slot.astype(jnp.int32), dst_slot.astype(jnp.int32)


def weight_draw(key, shape):
    return (jax.random.normal(key, shape, jnp.float32) * shape[1] ** -0.5).astype(jnp.bfloat16)


def setup_inputs(seed: int = 0, part: int = 0) -> dict:
    root = jax.random.key(seed)
    shared = jax.random.split(root, 6)
    own = jax.random.split(jax.random.fold_in(root, part), 4)
    pool_shape = (ALL_SLOTS, LAYERS, PAGE, KV_HEADS, HEAD)
    old_table, seq_len, src_slot, dst_slot = draw_layout(own[3])
    return dict(
        x_embed=jax.random.normal(own[0], (2, BATCH, D), jnp.float32).astype(jnp.bfloat16),
        w_query=weight_draw(shared[0], (LAYERS, D, HEADS * HEAD)),
        w_key=weight_draw(shared[1], (LAYERS, D, KV_HEADS * HEAD)),
        w_value=weight_draw(shared[2], (LAYERS, D, KV_HEADS * HEAD)),
        w_out=weight_draw(shared[3], (LAYERS, HEADS * HEAD, D)),
        w_up=weight_draw(shared[4], (LAYERS, D, FF)),
        w_down=weight_draw(shared[5], (LAYERS, FF, D)),
        k_pool=jax.random.normal(own[1], pool_shape, jnp.float32).astype(jnp.bfloat16),
        v_pool=jax.random.normal(own[2], pool_shape, jnp.float32).astype(jnp.bfloat16),
        old_table=old_table,
        seq_len=seq_len,
        src_slot=src_slot,
        dst_slot=dst_slot,
    )


def reference(x_embed, w_query, w_key, w_value, w_out, w_up, w_down, k_pool, v_pool, old_table, seq_len, src_slot, dst_slot):
    move_ids = jnp.arange(MOVES, dtype=jnp.int32)
    slot_move = jnp.full((ALL_SLOTS,), -1, jnp.int32).at[src_slot].set(move_ids)
    move_idx = slot_move[jnp.maximum(old_table, 0)]
    new_table = jnp.where((old_table >= 0) & (move_idx >= 0), dst_slot[jnp.maximum(move_idx, 0)], old_table)
    k_pool = k_pool.at[dst_slot].set(k_pool[src_slot])
    v_pool = v_pool.at[dst_slot].set(v_pool[src_slot])
    seq_ids = jnp.arange(BATCH)
    tok_pos = jnp.arange(PAGES * PAGE)
    q_group = HEADS // KV_HEADS
    step_outs = []
    for step_idx in range(2):
        cur_pos = seq_len + step_idx
        w_slot = new_table[seq_ids, cur_pos // PAGE]
        w_off = cur_pos % PAGE

        def layer_body(layer_state, layer_in):
            hidden, k_cache, v_cache = layer_state
            layer_idx, wq_l, wk_l, wv_l, wo_l, up_l, down_l = layer_in
            query = jnp.dot(hidden, wq_l, preferred_element_type=jnp.float32).astype(jnp.bfloat16)
            k_new = jnp.dot(hidden, wk_l, preferred_element_type=jnp.float32).astype(jnp.bfloat16).reshape(BATCH, KV_HEADS, HEAD)
            v_new = jnp.dot(hidden, wv_l, preferred_element_type=jnp.float32).astype(jnp.bfloat16).reshape(BATCH, KV_HEADS, HEAD)
            k_cache = k_cache.at[w_slot, layer_idx, w_off].set(k_new)
            v_cache = v_cache.at[w_slot, layer_idx, w_off].set(v_new)

            def attend(seq_in):
                q_row, table_row, limit_pos = seq_in
                page_sel = jnp.maximum(table_row, 0)
                page_keys = k_cache[page_sel, layer_idx].reshape(PAGES * PAGE, KV_HEADS, HEAD).astype(jnp.float32)
                page_vals = v_cache[page_sel, layer_idx].reshape(PAGES * PAGE, KV_HEADS, HEAD).astype(jnp.float32)
                q_heads = q_row.reshape(KV_HEADS, q_group, HEAD).astype(jnp.float32)
                scores = jnp.einsum('grd,tgd->grt', q_heads, page_keys) * HEAD ** -0.5
                scores = jnp.where(tok_pos <= limit_pos, scores, -1e30)
                attn_w = jax.nn.softmax(scores, axis=-1)
                return jnp.einsum('grt,tgd->grd', attn_w, page_vals).reshape(HEADS * HEAD).astype(jnp.bfloat16)

            attn_out = lax.map(attend, (query, new_table, cur_pos))
            hidden = (hidden.astype(jnp.float32) + jnp.dot(attn_out, wo_l, preferred_element_type=jnp.float32)).astype(jnp.bfloat16)
            up_act = jax.nn.gelu(jnp.dot(hidden, up_l, preferred_element_type=jnp.float32)).astype(jnp.bfloat16)
            hidden = (hidden.astype(jnp.float32) + jnp.dot(up_act, down_l, preferred_element_type=jnp.float32)).astype(jnp.bfloat16)
            return (hidden, k_cache, v_cache), None

        layer_xs = (jnp.arange(LAYERS), w_query, w_key, w_value, w_out, w_up, w_down)
        (hidden, k_pool, v_pool), _ = lax.scan(layer_body, (x_embed[step_idx], k_pool, v_pool), layer_xs)
        step_outs.append(hidden)
    return jnp.stack(step_outs), k_pool, v_pool
```

```python
import functools

import jax
import jax.numpy as jnp
from jax import lax
from jax.experimental import pallas as pl
from jax.experimental.pallas import tpu as pltpu
from jax.sharding import PartitionSpec as P

F32 = jnp.float32
BF16 = jnp.bfloat16
NEG = -1e30
NN = (((1,), (0,)), ((), ()))
NT = (((1,), (1,)), ((), ()))
TN = (((0,), (0,)), ((), ()))


def _dot(a, b, dims):
    return lax.dot_general(a, b, dims, preferred_element_type=F32)


def _split(x):
    hi = x.astype(BF16)
    rest = x - hi.astype(F32)
    mid = rest.astype(BF16)
    low = (rest - mid.astype(F32)).astype(BF16)
    return hi, mid, low


def _pick_lhs(x, sel, dims):
    hi, mid, low = _split(x)
    return _dot(hi, sel, dims) + _dot(mid, sel, dims) + _dot(low, sel, dims)


def _pick_rhs(sel, x, dims):
    hi, mid, low = _split(x)
    return _dot(sel, hi, dims) + _dot(sel, mid, dims) + _dot(sel, low, dims)


def _prep_kernel(n_pages, page, old_ref, src_ref, dstr_ref, dstc_ref, len_ref, base_ref, qsel_ref, wsel_ref, cell_ref, mig_ref, info_ref):
    n_slots = qsel_ref.shape[1]
    n_seq = len_ref.shape[0]
    base = base_ref[0]
    found = jnp.sum(jnp.where(old_ref[...] == src_ref[...], dstr_ref[...] + 1, 0).astype(F32), axis=1, keepdims=True).astype(jnp.int32)
    new = jnp.where(found > 0, found - 1, old_ref[...])
    local = new - base
    slot_ids = lax.broadcasted_iota(jnp.int32, (1, n_slots), 1)
    lens = len_ref[...]
    last = lens // page
    q_sel = jnp.zeros((n_seq, n_slots), F32)
    w_sel = jnp.zeros((n_seq, n_slots), F32)
    first = jnp.zeros((1, n_slots), F32)
    for j in range(n_pages):
        eq = (local[j * n_seq:(j + 1) * n_seq] == slot_ids).astype(F32)
        cell_ref[j * n_seq:(j + 1) * n_seq, :] = eq.astype(BF16)
        q_sel = q_sel + eq
        w_sel = w_sel + jnp.where(last == j, eq, 0.0)
        first = first + jnp.sum(eq, axis=0, keepdims=True) * float(j * page)
    qsel_ref[...] = q_sel.astype(BF16)
    wsel_ref[...] = w_sel.astype(BF16)
    used = jnp.sum(q_sel, axis=0, keepdims=True)
    slot_len = jnp.sum(q_sel * lens.astype(F32), axis=0, keepdims=True)
    written = jnp.sum(w_sel, axis=0, keepdims=True)
    w_off = jnp.sum(w_sel * (lens - last * page).astype(F32), axis=0, keepdims=True)
    mig = ((dstc_ref[...] - base) == slot_ids).astype(F32)
    mig_ref[...] = mig.astype(BF16)
    moved = jnp.sum(mig, axis=0, keepdims=True)
    info_ref[0:1, :] = used
    info_ref[1:2, :] = jnp.where(used > 0, slot_len - first, -100.0)
    info_ref[2:3, :] = jnp.where(written > 0, w_off, -100.0)
    info_ref[3:4, :] = moved
    info_ref[4:8, :] = jnp.zeros((4, n_slots), F32)


def _pack_kernel(heads, onehot_ref, k_ref, v_ref, ko_ref, vo_ref):
    page, _, dim, n_slots = k_ref.shape[1:]
    width = page * dim
    for h in range(heads):
        for src, out in ((k_ref, ko_ref), (v_ref, vo_ref)):
            rows = src[0, :, h].reshape(width, n_slots)
            out[:, h * width:(h + 1) * width] = _dot(onehot_ref[...], rows, NT).astype(BF16)


def _attn_kernel(steps, group, layer, heads, n_alias, *refs):
    (q_ref, kn_ref, vn_ref, k_ref, v_ref, mk_ref, mv_ref, qsel_ref, wsel_ref, cell_ref, mig_ref, info_ref) = refs[:12]
    ko_ref, vo_ref, o_ref, ml_ref, q_s, kv_s, kf_s, vf_s, s_s, os_s, ml_s = refs[12 + n_alias:]
    page, _, dim, n_slots = k_ref.shape[1:]
    n_seq = qsel_ref.shape[0]
    n_home = o_ref.shape[0]
    home = n_seq // n_home
    pid = pl.program_id(0)
    n_rt = steps * group
    used = info_ref[0:1, :]
    limit = info_ref[1:2, :]
    w_off = info_ref[2:3, :]
    moved = info_ref[3:4, :] > 0
    cells = cell_ref[...]
    owned = _dot(jnp.ones((8, n_slots), BF16), cells, NT)[0:1] > 0
    scale = dim ** -0.5
    q_sel = qsel_ref[...]
    w_sel = wsel_ref[...]
    for t in range(steps):
        rows = q_ref[:, t].reshape(n_seq, heads * group * dim)
        q_s[t] = _dot(rows, q_sel, TN)
        kv_s[0, t] = _dot(kn_ref[:, t].reshape(n_seq, heads * dim), w_sel, TN)
        kv_s[1, t] = _dot(vn_ref[:, t].reshape(n_seq, heads * dim), w_sel, TN)
    for h in range(heads):
        for which, (pool, pages, out, full) in enumerate(((k_ref, mk_ref, ko_ref, kf_s), (v_ref, mv_ref, vo_ref, vf_s))):
            width = page * dim
            full[...] = _dot(pages[:, h * width:(h + 1) * width], mig_ref[...], TN).reshape(page, dim, n_slots)

            def fill(tok, _, which=which, pool=pool, out=out, full=full, h=h):
                val = jnp.where(moved, full[tok], pool[0, tok, h].astype(F32))
                at = w_off - tok.astype(F32)
                for t in range(steps):
                    val = jnp.where(at == -float(t), kv_s[which, t, h * dim:(h + 1) * dim, :], val)
                full[tok] = val
                out[0, tok, h] = val.astype(BF16)
                return 0

            lax.fori_loop(0, page, fill, 0)

        def score(tok, _, h=h):
            keys = kf_s[tok]
            for t in range(steps):
                for r in range(group):
                    q_row = q_s[t, (h * group + r) * dim:(h * group + r + 1) * dim, :]
                    s_s[t * group + r, pl.ds(tok, 1), :] = jnp.sum(keys * q_row, axis=0, keepdims=True)
            return 0

        lax.fori_loop(0, page, score, 0)
        tok_ids = lax.broadcasted_iota(jnp.int32, (page, n_slots), 0).astype(F32)
        for t in range(steps):
            visible = tok_ids <= limit + float(t)
            for r in range(group):
                sc = jnp.where(visible, s_s[t * group + r] * scale, NEG)
                top = jnp.max(sc, axis=0, keepdims=True)
                ex = jnp.exp(sc - top)
                s_s[t * group + r] = ex
                ml_s[t * group + r:t * group + r + 1, :] = jnp.where(used > 0, top, 0.0)
                ml_s[n_rt + t * group + r:n_rt + t * group + r + 1, :] = jnp.sum(ex, axis=0, keepdims=True)
        m_slot = ml_s[0:n_rt]
        l_slot = ml_s[n_rt:2 * n_rt]
        m_cell = jnp.where(owned, _pick_lhs(m_slot, cells, NT), NEG)
        m_seq = m_cell[:, 0:n_seq]
        for j in range(1, cells.shape[0] // n_seq):
            m_seq = jnp.maximum(m_seq, m_cell[:, j * n_seq:(j + 1) * n_seq])
        has = m_seq > NEG
        m_back = _pick_lhs(jnp.where(has, m_seq, 0.0), q_sel, NN)
        w_slot = jnp.where(used > 0, jnp.exp(m_slot - m_back), 0.0)
        l_seq = _pick_lhs(l_slot * w_slot, q_sel, NT)
        row = (pid * heads + h) * n_rt
        ml_ref[pl.ds(row, n_rt), :] = m_seq
        ml_ref[pl.ds(pl.num_programs(0) * heads * n_rt + row, n_rt), :] = l_seq
        for rt in range(n_rt):
            s_s[rt] = s_s[rt] * w_slot[rt:rt + 1]

        for t in range(steps):
            def weigh(c, _, t=t):
                at = pl.multiple_of(c * 8, 8)
                acc = [jnp.zeros((8, n_slots), F32) for _ in range(group)]
                for tok in range(page):
                    vals = vf_s[tok, pl.ds(at, 8), :]
                    for r in range(group):
                        acc[r] = acc[r] + s_s[t * group + r, tok:tok + 1, :] * vals
                for r in range(group):
                    os_s[pl.ds(r * dim + at, 8), :] = acc[r]
                return 0

            lax.fori_loop(0, dim // 8, weigh, 0)
            part = _pick_rhs(q_sel, os_s[...], NT)
            o_ref[:, t, :, h * group * dim:(h + 1) * group * dim] = part.reshape(n_home, home, group * dim)


def _merge_kernel(heads, dim, group, o_ref, ml_ref, out_ref):
    n_home, steps, home, _ = o_ref.shape
    half = ml_ref.shape[2] // 2
    m = ml_ref[:, :, 0:half]
    l = ml_ref[:, :, half:2 * half]
    top = jnp.max(m, axis=0, keepdims=True)
    w = jnp.exp(m - top)
    total = jnp.sum(w * l, axis=0, keepdims=True)
    w = w / total
    for t in range(steps):
        lane = lax.broadcasted_iota(jnp.int32, (half, heads * dim), 1) // dim
        src = lax.broadcasted_iota(jnp.int32, (half, heads * dim), 0)
        want = (lane // group) * (steps * group) + t * group + lane % group
        spread = (src == want).astype(BF16)
        acc = jnp.zeros((home, heads * dim), F32)
        for k in range(n_home):
            acc = acc + _pick_lhs(w[k], spread, NN) * o_ref[k, t]
        out_ref[t] = acc.astype(BF16)


def solution(mesh):
    n_cols = mesh.shape['kv']
    dev_axes = ('rep', 'kv2', 'kv')
    group_axes = ('kv2', 'kv')
    seq_spec = P(None, dev_axes, None)
    pool_spec = P(dev_axes, None, None, None, None)
    table_spec = P(dev_axes, None)
    vec_spec = P(dev_axes)
    full_spec = P()
    pair = 2

    def per_device(x_embed, w_query, w_key, w_value, w_out, w_up, w_down, k_pool, v_pool, old_table, seq_len, src_slot, dst_slot):
        n_slots, layers, page, kv_heads, dim = k_pool.shape
        steps, seq_dev, width = x_embed.shape
        heads = w_query.shape[2] // dim
        group = heads // kv_heads
        n_pages = old_table.shape[1]
        n_seq = seq_dev * n_cols
        n_move = src_slot.shape[0]
        n_rt = steps * group
        n_grid = kv_heads // pair
        page_w = page * dim
        me = lax.axis_index('kv2') * n_cols + lax.axis_index('kv')
        slot_base = me * n_slots
        k_t = jnp.transpose(k_pool, (1, 2, 3, 4, 0))
        v_t = jnp.transpose(v_pool, (1, 2, 3, 4, 0))

        src_hot = ((src_slot - slot_base)[:, None] == jnp.arange(n_slots, dtype=jnp.int32)[None, :]).astype(BF16)

        def pack(layer):
            blk = pl.BlockSpec((1, page, pair, dim, n_slots), lambda i: (layer, 0, i, 0, 0))
            out = pl.BlockSpec((n_move, pair * page_w), lambda i: (0, i))
            shape = jax.ShapeDtypeStruct((n_move, kv_heads * page_w), BF16)
            return pl.pallas_call(
                functools.partial(_pack_kernel, pair),
                grid=(n_grid,),
                in_specs=[pl.BlockSpec((n_move, n_slots), lambda i: (0, 0)), blk, blk],
                out_specs=[out, out],
                out_shape=[shape, shape],
                cost_estimate=pl.CostEstimate(flops=4 * 256 * n_slots * kv_heads * page_w, bytes_accessed=8 * 2**20, transcendentals=0),
                name='pack_pages',
            )(src_hot, k_t, v_t)

        packed = [pack(layer) for layer in range(layers)]
        moved = [lax.all_gather(jnp.concatenate(p, axis=1), group_axes, tiled=True) for p in packed]

        meta = jnp.concatenate([old_table.T.reshape(-1), seq_len, src_slot, dst_slot])
        meta_all = lax.all_gather(meta, group_axes)
        n_tab = n_pages * seq_dev
        row = lax.dynamic_slice_in_dim(meta_all, lax.axis_index('kv2') * n_cols, n_cols, axis=0)
        old_col = row[:, :n_tab].reshape(n_cols, n_pages, seq_dev).transpose(1, 0, 2).reshape(-1, 1)
        len_col = row[:, n_tab:n_tab + seq_dev].reshape(-1, 1)
        src_all = meta_all[:, n_tab + seq_dev:n_tab + seq_dev + n_move].reshape(1, -1)
        dst_all = meta_all[:, n_tab + seq_dev + n_move:].reshape(1, -1)
        n_all = src_all.shape[1]
        vmem = pl.BlockSpec(memory_space=pltpu.VMEM)
        q_sel, w_sel, cells, mig, info = pl.pallas_call(
            functools.partial(_prep_kernel, n_pages, page),
            in_specs=[vmem] * 5 + [pl.BlockSpec(memory_space=pltpu.SMEM)],
            out_specs=[vmem] * 5,
            out_shape=[
                jax.ShapeDtypeStruct((n_seq, n_slots), BF16),
                jax.ShapeDtypeStruct((n_seq, n_slots), BF16),
                jax.ShapeDtypeStruct((n_pages * n_seq, n_slots), BF16),
                jax.ShapeDtypeStruct((n_all, n_slots), BF16),
                jax.ShapeDtypeStruct((8, n_slots), F32),
            ],
            name='prep_tables',
        )(old_col, src_all, dst_all, dst_all.reshape(-1, 1), len_col, slot_base.reshape(1))

        def attend(layer, qkv, k_prev, v_prev):
            blk = pl.BlockSpec((1, page, pair, dim, n_slots), lambda i: (layer, 0, i, 0, 0))
            q_w, kv_w, m_w = pair * group * dim, pair * dim, pair * page_w
            k_at, v_at = heads * dim // kv_w, (heads + kv_heads) * dim // kv_w

            def fixed(shape):
                return pl.BlockSpec(shape, lambda i: (0,) * len(shape), pipeline_mode=pl.Buffered(1))

            qkv4 = qkv.reshape(n_cols, steps, seq_dev, qkv.shape[-1])
            in_specs = [
                pl.BlockSpec((n_cols, steps, seq_dev, q_w), lambda i: (0, 0, 0, i)),
                pl.BlockSpec((n_cols, steps, seq_dev, kv_w), lambda i: (0, 0, 0, k_at + i)),
                pl.BlockSpec((n_cols, steps, seq_dev, kv_w), lambda i: (0, 0, 0, v_at + i)),
                blk, blk,
                pl.BlockSpec((n_all, m_w), lambda i: (0, i)),
                pl.BlockSpec((n_all, m_w), lambda i: (0, n_grid + i)),
                fixed(q_sel.shape), fixed(w_sel.shape), fixed(cells.shape), fixed(mig.shape), fixed(info.shape),
            ]
            args = [qkv4, qkv4, qkv4, k_t, v_t, moved[layer], moved[layer], q_sel, w_sel, cells, mig, info]
            aliases = {}
            if k_prev is not None:
                in_specs += [pl.BlockSpec(memory_space=pl.ANY)] * 2
                aliases = {len(args): 0, len(args) + 1: 1}
                args += [k_prev, v_prev]
            ml_rows = 2 * kv_heads * n_rt
            return pl.pallas_call(
                functools.partial(_attn_kernel, steps, group, layer, pair, len(aliases)),
                grid=(n_grid,),
                in_specs=in_specs,
                out_specs=[
                    blk, blk,
                    pl.BlockSpec((n_cols, steps, seq_dev, q_w), lambda i: (0, 0, 0, i)),
                    pl.BlockSpec((ml_rows, n_seq), lambda i: (0, 0)),
                ],
                out_shape=[
                    jax.ShapeDtypeStruct(k_t.shape, BF16),
                    jax.ShapeDtypeStruct(v_t.shape, BF16),
                    jax.ShapeDtypeStruct((n_cols, steps, seq_dev, heads * dim), F32),
                    jax.ShapeDtypeStruct((ml_rows, n_seq), F32),
                ],
                scratch_shapes=[
                    pltpu.VMEM((steps, q_w, n_slots), F32),
                    pltpu.VMEM((2, steps, kv_w, n_slots), F32),
                    pltpu.VMEM((page, dim, n_slots), F32),
                    pltpu.VMEM((page, dim, n_slots), F32),
                    pltpu.VMEM((n_rt, page, n_slots), F32),
                    pltpu.VMEM((group * dim, n_slots), F32),
                    pltpu.VMEM((2 * n_rt, n_slots), F32),
                ],
                input_output_aliases=aliases,
                compiler_params=pltpu.CompilerParams(vmem_limit_bytes=48 * 2**20),
                cost_estimate=pl.CostEstimate(flops=40 * 10**9, bytes_accessed=40 * 2**20, transcendentals=0),
                name='slot_attention',
            )(*args)

        hidden = x_embed.reshape(steps * seq_dev, width)
        k_out = v_out = None
        for layer in range(layers):
            qkv = jnp.concatenate([jnp.dot(hidden, w[layer], preferred_element_type=F32).astype(BF16) for w in (w_query, w_key, w_value)], axis=1)
            qkv_row = lax.all_gather(qkv, 'kv', tiled=True)
            k_out, v_out, part, ml = attend(layer, qkv_row, k_out, v_out)
            ml = ml.T.reshape(n_cols, seq_dev, -1)
            part = lax.all_to_all(part, 'kv', 0, 0, tiled=True)
            ml = lax.all_to_all(ml, 'kv', 0, 0, tiled=True)
            attn = pl.pallas_call(
                functools.partial(_merge_kernel, heads, dim, group),
                in_specs=[vmem] * 2,
                out_specs=vmem,
                out_shape=jax.ShapeDtypeStruct((steps, seq_dev, heads * dim), BF16),
                compiler_params=pltpu.CompilerParams(vmem_limit_bytes=32 * 2**20),
                name='merge_partials',
            )(part, ml).reshape(steps * seq_dev, heads * dim)
            hidden = (hidden.astype(F32) + jnp.dot(attn, w_out[layer], preferred_element_type=F32)).astype(BF16)
            up_act = jax.nn.gelu(jnp.dot(hidden, w_up[layer], preferred_element_type=F32)).astype(BF16)
            hidden = (hidden.astype(F32) + jnp.dot(up_act, w_down[layer], preferred_element_type=F32)).astype(BF16)
        y_out = hidden.reshape(steps, seq_dev, width)
        back = (4, 0, 1, 2, 3)
        return y_out, jnp.transpose(k_out, back), jnp.transpose(v_out, back)

    return jax.shard_map(per_device, mesh=mesh, in_specs=(seq_spec, full_spec, full_spec, full_spec, full_spec, full_spec, full_spec, pool_spec, pool_spec, table_spec, vec_spec, vec_spec, vec_spec), out_specs=(seq_spec, pool_spec, pool_spec), check_vma=False)
```

```python
import functools

import jax
import jax.numpy as jnp
from jax import lax
from jax.experimental import pallas as pl
from jax.experimental.pallas import tpu as pltpu
from jax.sharding import PartitionSpec as P

F32 = jnp.float32
BF16 = jnp.bfloat16
I32 = jnp.int32
NEG = -1e30
NN = (((1,), (0,)), ((), ()))
NT = (((1,), (1,)), ((), ()))
TN = (((0,), (0,)), ((), ()))
MESH = pl.DeviceIdType.MESH
LANES = 256
I0, I1, I2, I3, I4, I5 = range(6)


def _dot(a, b, dims):
    return lax.dot_general(a, b, dims, preferred_element_type=F32)


def _split(x):
    hi = x.astype(BF16)
    rest = x - hi.astype(F32)
    mid = rest.astype(BF16)
    low = (rest - mid.astype(F32)).astype(BF16)
    return hi, mid, low


def _pick_lhs(x, sel, dims):
    hi, mid, low = _split(x)
    return _dot(hi, sel, dims) + _dot(mid, sel, dims) + _dot(low, sel, dims)


def _pick_rhs(sel, x, dims):
    hi, mid, low = _split(x)
    return _dot(sel, hi, dims) + _dot(sel, mid, dims) + _dot(sel, low, dims)


def _prep_kernel(n_pages, page, n_cols, n_slots, old_ref, src_ref, dstr_ref, dstc_ref, len_ref, mysrc_ref, mysrcc_ref, pos_ref, qsel_ref, cell_ref, arr_ref, info_ref, wsel_ref, mig_ref, winfo_ref):
    base = pos_ref[0]
    my_col = pos_ref[1]
    n_seq = len_ref.shape[0]
    n_all = src_ref.shape[1]
    n_move = mysrc_ref.shape[1]
    n_arr = arr_ref.shape[0]
    spare = LANES - n_slots
    old = old_ref[...]
    hit = old == src_ref[...]
    entry = jnp.sum(jnp.where(hit, lax.broadcasted_iota(I32, (1, n_all), 1) + 1, 0).astype(F32), axis=1, keepdims=True).astype(I32)
    dst = jnp.sum(jnp.where(hit, dstr_ref[...] + 1, 0).astype(F32), axis=1, keepdims=True).astype(I32) - 1
    is_moved = entry > 0
    entry = entry - 1
    dev = entry // n_move
    nth = entry - dev * n_move
    arrival = (dev // n_cols) * n_move + nth
    free = jnp.sum(jnp.where(nth == lax.broadcasted_iota(I32, (1, n_move), 1), mysrc_ref[...] - base, 0).astype(F32), axis=1, keepdims=True).astype(I32)
    arr_lane = jnp.where(arrival < spare, n_slots + arrival, free)
    here = old - base
    here = jnp.where((here >= 0) & (here < n_slots), here, -1)
    lane = jnp.where(is_moved, jnp.where(dev % n_cols == my_col, arr_lane, -1), here)
    final = jnp.where(is_moved, dst, old) - base
    lane_ids = lax.broadcasted_iota(I32, (1, LANES), 1)
    slot_ids = lax.broadcasted_iota(I32, (1, n_slots), 1)
    lens = len_ref[...]
    last = lens // page
    q_sel = jnp.zeros((n_seq, LANES), F32)
    w_sel = jnp.zeros((n_seq, n_slots), F32)
    first = jnp.zeros((1, LANES), F32)
    for j in range(n_pages):
        eq = (lane[j * n_seq:(j + 1) * n_seq] == lane_ids).astype(F32)
        cell_ref[j * n_seq:(j + 1) * n_seq, :] = eq.astype(BF16)
        q_sel = q_sel + eq
        first = first + jnp.sum(eq, axis=0, keepdims=True) * float(j * page)
        w_sel = w_sel + jnp.where((final[j * n_seq:(j + 1) * n_seq] == slot_ids) & (last == j), 1.0, 0.0)
    qsel_ref[...] = q_sel.astype(BF16)
    wsel_ref[...] = w_sel.astype(BF16)
    used = jnp.sum(q_sel, axis=0, keepdims=True)
    slot_len = jnp.sum(q_sel * lens.astype(F32), axis=0, keepdims=True)
    arr_ids = lax.broadcasted_iota(I32, (n_arr, LANES), 0)
    at_spare = jnp.where(lane_ids == n_slots + arr_ids, 1.0, 0.0)
    arr_ref[...] = at_spare.astype(BF16)
    mine = mysrcc_ref[...] - base
    for k in range(n_arr - spare):
        arr_ref[spare + k:spare + k + 1, :] = jnp.where(lane_ids == mine[k:k + 1], 1.0, 0.0).astype(BF16)
    out_lanes = jnp.sum(jnp.where(mine == lane_ids, 1.0, 0.0), axis=0, keepdims=True)
    info_ref[0:1, :] = used
    info_ref[1:2, :] = jnp.where(used > 0, slot_len - first - 1.0, -100.0)
    info_ref[2:3, :] = jnp.where(lane_ids >= n_slots, 1.0, out_lanes)
    info_ref[3:8, :] = jnp.zeros((5, LANES), F32)
    written = jnp.sum(w_sel, axis=0, keepdims=True)
    w_off = jnp.sum(w_sel * (lens - last * page).astype(F32), axis=0, keepdims=True)
    mig = ((dstc_ref[...] - base) == slot_ids).astype(F32)
    mig_ref[...] = mig.astype(BF16)
    winfo_ref[0:1, :] = jnp.sum(mig, axis=0, keepdims=True)
    winfo_ref[1:2, :] = jnp.where(written > 0, w_off, -100.0)
    winfo_ref[2:8, :] = jnp.zeros((6, n_slots), F32)


def _pack_kernel(heads, onehot_ref, k_ref, v_ref, out_ref):
    page, _, dim, n_slots = k_ref.shape[1:]
    width = page * dim
    for h in range(heads):
        for which, src in enumerate((k_ref, v_ref)):
            rows = src[0, :, h].reshape(width, n_slots)
            out_ref[which, :, h * width:(h + 1) * width] = _dot(onehot_ref[...], rows, NT).astype(BF16)


def _copy(src, dst, sems, k, dev):
    return pltpu.make_async_remote_copy(src_ref=src, dst_ref=dst, send_sem=sems.at[0, k], recv_sem=sems.at[1, k], device_id=dev, device_id_type=MESH)


def _rows_on_y(own, out, sems, halves):
    n = out.shape[I0]
    y = lax.axis_index('kv2')
    up, dn, far = (y + I1) % n, (y + n - I1) % n, (y + I2) % n
    to_up, to_dn = {'kv2': up}, {'kv2': dn}
    first = [
        _copy(halves(own, I0), halves(out.at[y], I0), sems, I0, to_up),
        _copy(halves(own, I1), halves(out.at[y], I1), sems, I1, to_up),
        _copy(halves(own, I1), halves(out.at[y], I1), sems, I2, to_dn),
        _copy(halves(own, I0), halves(out.at[y], I0), sems, I3, to_dn),
    ]
    relay = [
        _copy(halves(out.at[dn], I0), halves(out.at[dn], I0), sems, I4, to_up),
        _copy(halves(out.at[up], I1), halves(out.at[up], I1), sems, I5, to_dn),
    ]
    lands = [(dn, I0), (dn, I1), (up, I1), (up, I0), (far, I0), (far, I1)]

    def got(k):
        at, h = lands[k]
        _copy(halves(out.at[at], h), halves(out.at[at], h), sems, k, to_up).wait_recv()

    def start():
        for k in (I0, I2, I1, I3):
            first[k].start()

    def forward():
        got(I0)
        relay[I0].start()
        got(I2)
        relay[I1].start()

    def finish():
        for k in (I1, I3, I4, I5):
            got(k)
        for c in first + relay:
            c.wait_send()

    return start, forward, finish


def _signal_all(devs):
    barrier = pltpu.get_barrier_semaphore()
    for dev in devs:
        pl.semaphore_signal(barrier, inc=1, device_id=dev, device_id_type=MESH)
    pl.semaphore_wait(barrier, len(devs))


def _q_gather(n_cols, q_ref, q_all, x_sem):
    n_x = n_cols // I2
    at = lax.axis_index('kv')
    x, core = at // I2, at % I2
    up, dn, far = (x + I1) % n_x, (x + n_x - I1) % n_x, (x + I2) % n_x
    to_up, to_dn, to_pal = {'kv': up * I2 + core}, {'kv': dn * I2 + core}, {'kv': x * I2 + I1 - core}
    n_half = q_ref.shape[I0] // I2

    def half(ref, h):
        return ref.at[pl.ds(h * n_half, n_half)]

    def slot(pos, c):
        return q_all.at[pos * I2 + c]

    first = [
        _copy(half(q_ref, I0), half(slot(x, core), I0), x_sem, I0, to_up),
        _copy(half(q_ref, I1), half(slot(x, core), I1), x_sem, I1, to_up),
        _copy(half(q_ref, I1), half(slot(x, core), I1), x_sem, I2, to_dn),
        _copy(half(q_ref, I0), half(slot(x, core), I0), x_sem, I3, to_dn),
    ]
    relay = [
        _copy(half(slot(dn, core), I0), half(slot(dn, core), I0), x_sem, I4, to_up),
        _copy(half(slot(up, core), I1), half(slot(up, core), I1), x_sem, I5, to_dn),
    ]
    lands = [(dn, I0), (dn, I1), (up, I1), (up, I0), (far, I0), (far, I1)]
    pal = [_copy(half(slot(p, core), h), half(slot(p, core), h), x_sem, 6 + k, to_pal) for k, (p, h) in enumerate(lands)]
    own = _copy(q_ref, slot(x, core), x_sem, 12, to_pal)

    def got(k):
        p, h = lands[k]
        _copy(half(slot(p, core), h), half(slot(p, core), h), x_sem, k, to_up).wait_recv()

    for k in (I0, I2, I1, I3):
        first[k].start()
    own.start()
    q_all[at] = q_ref[...]
    yield
    got(I0)
    relay[I0].start()
    pal[I0].start()
    got(I2)
    relay[I1].start()
    pal[I2].start()
    yield
    for k in (I1, I3, I4, I5):
        got(k)
        pal[k].start()
    yield
    _copy(q_ref, slot(x, I1 - core), x_sem, 12, to_pal).wait_recv()
    for k, (p, h) in enumerate(lands):
        _copy(half(slot(p, I1 - core), h), half(slot(p, I1 - core), h), x_sem, 6 + k, to_pal).wait_recv()
    for c in first + relay + pal + [own]:
        c.wait_send()


def _x_peers(n_cols):
    n_x = n_cols // I2
    at = lax.axis_index('kv')
    x, core = at // I2, at % I2
    return [{'kv': ((x + I1) % n_x) * I2 + core}, {'kv': ((x + n_x - I1) % n_x) * I2 + core}, {'kv': x * I2 + I1 - core}]


def _y_peers(n_rows):
    y = lax.axis_index('kv2')
    return [{'kv2': (y + I1) % n_rows}, {'kv2': (y + n_rows - I1) % n_rows}]


def _half0(ref, h):
    return ref.at[h]


def _head_kernel(n_rows, n_cols, meta_ref, pages_ref, q_ref, meta_all, pages_all, q_all, m_sem, y_sem, x_sem):
    y, at = lax.axis_index('kv2'), lax.axis_index('kv')
    offsets = [(a, b) for a in range(n_rows) for b in range(n_cols) if (a, b) != (0, 0)]
    peers = [{'kv2': (y + a) % n_rows, 'kv': (at + b) % n_cols} for a, b in offsets]
    _signal_all(peers)
    me = y * n_cols + at
    metas = [_copy(meta_ref, meta_all.at[me], m_sem, k, peers[k]) for k in range(len(peers))]
    for c in metas:
        c.start()
    start, forward, finish = _rows_on_y(pages_ref, pages_all, y_sem, _half0)
    start()
    steps = _q_gather(n_cols, q_ref, q_all, x_sem)
    next(steps)
    meta_all[me] = meta_ref[...]
    pages_all[y] = pages_ref[...]
    next(steps)
    forward()
    next(steps)
    finish()
    for _ in steps:
        pass
    for k, (a, b) in enumerate(offsets):
        frm = ((y + n_rows - a) % n_rows) * n_cols + (at + n_cols - b) % n_cols
        _copy(meta_ref, meta_all.at[frm], m_sem, k, peers[k]).wait_recv()
    for c in metas:
        c.wait_send()


def _query_kernel(n_cols, q_ref, q_all, x_sem):
    _signal_all(_x_peers(n_cols))
    for _ in _q_gather(n_cols, q_ref, q_all, x_sem):
        pass


def _attn_kernel(steps, group, heads, q_ref, k_ref, v_ref, mk_ref, mv_ref, qsel_ref, cell_ref, arr_ref, info_ref, o_ref, ml_ref, q_s, mk_s, mv_s, s_s, os_s, ml_s, ml_all):
    page, _, dim, n_slots = k_ref.shape[1:]
    n_seq = qsel_ref.shape[0]
    n_core, n_x, _, home = o_ref.shape[:4]
    n_arr = arr_ref.shape[0]
    pid = pl.program_id(0)
    n_rt = steps * group
    width = page * dim
    used = info_ref[0:1, :]
    limit = info_ref[1:2, :]
    freed = info_ref[2:3, 0:n_slots] > 0
    cells = cell_ref[...]
    owned = _dot(jnp.ones((8, LANES), BF16), cells, NT)[0:1] > 0
    scale = dim ** -0.5
    q_sel = qsel_ref[...]

    @pl.when(pid == 0)
    def _():
        ml_all[...] = jnp.zeros_like(ml_all)

    for t in range(steps):
        q_s[t] = _dot(q_ref[:, t].reshape(n_seq, heads * group * dim), q_sel, TN)
    tops, sums = [[] for _ in range(steps)], [[] for _ in range(steps)]
    for h in range(heads):
        for pages, full in ((mk_ref, mk_s), (mv_ref, mv_s)):
            full[...] = _dot(pages[:, 0, :, h * width:(h + 1) * width].reshape(n_arr, width), arr_ref[...], TN).reshape(page, dim, LANES)

        def join(tok, _, h=h):
            for pool, full in ((k_ref, mk_s), (v_ref, mv_s)):
                full[tok, :, 0:n_slots] = jnp.where(freed, full[tok, :, 0:n_slots], pool[0, tok, h].astype(F32))
            return 0

        lax.fori_loop(0, page, join, 0)

        def score(pair, _, h=h):
            toks = [pair * 2, pair * 2 + 1]
            keys = [mk_s[tok] for tok in toks]
            for t in range(steps):
                for r in range(group):
                    q_row = q_s[t, (h * group + r) * dim:(h * group + r + 1) * dim, :]
                    for tok, key in zip(toks, keys):
                        s_s[t * group + r, pl.ds(tok, 1), :] = jnp.sum(key * q_row, axis=0, keepdims=True)
            return 0

        lax.fori_loop(0, page // 2, score, 0)
        visible = lax.broadcasted_iota(I32, (page, LANES), 0).astype(F32) <= limit
        for rt in range(n_rt):
            sc = jnp.where(visible, s_s[rt] * scale, NEG)
            top = jnp.max(sc, axis=0, keepdims=True)
            ex = jnp.where(visible, jnp.exp(sc - top), 0.0)
            s_s[rt] = ex
            ml_s[rt:rt + 1, :] = top
            ml_s[n_rt + rt:n_rt + rt + 1, :] = jnp.sum(ex, axis=0, keepdims=True)
        live = (used > 0) & (limit >= 0)
        m_slot = ml_s[0:n_rt]
        l_slot = ml_s[n_rt:2 * n_rt]
        m_cell = jnp.where(owned, _pick_lhs(m_slot, cells, NT), NEG)
        m_seq = m_cell[:, 0:n_seq]
        for j in range(1, cells.shape[0] // n_seq):
            m_seq = jnp.maximum(m_seq, m_cell[:, j * n_seq:(j + 1) * n_seq])
        m_back = _pick_lhs(m_seq, q_sel, NN)
        w_slot = jnp.where(live, jnp.exp(jnp.minimum(m_slot - m_back, 0.0)), 0.0)
        l_seq = _pick_lhs(l_slot * w_slot, q_sel, NT)
        for t in range(steps):
            tops[t].append(m_seq[t * group:(t + 1) * group])
            sums[t].append(l_seq[t * group:(t + 1) * group])
        for rt in range(n_rt):
            s_s[rt] = s_s[rt] * w_slot[rt:rt + 1]

        def weigh(c, _):
            row = pl.multiple_of(c * 8, 8)
            acc = [jnp.zeros((8, LANES), F32) for _ in range(n_rt)]
            for tok in range(page):
                vals = mv_s[tok, pl.ds(row, 8), :]
                for rt in range(n_rt):
                    acc[rt] = acc[rt] + s_s[rt, tok:tok + 1, :] * vals
            for rt in range(n_rt):
                os_s[pl.ds(rt * dim + row, 8), :] = acc[rt]
            return 0

        lax.fori_loop(0, dim // 8, weigh, 0)
        for t in range(steps):
            part = _pick_rhs(q_sel, os_s[t * group * dim:(t + 1) * group * dim, :], NT).reshape(n_x, n_core, home, group * dim)
            for c in range(n_core):
                o_ref[c, :, t, :, h * group * dim:(h + 1) * group * dim] = part[:, c]

    n_row = heads * group
    for t in range(steps):
        ml_all[t, pl.ds(pl.multiple_of(pid * n_row, n_row), n_row), :] = jnp.concatenate(tops[t], axis=0)
        ml_all[t, pl.ds(pl.multiple_of((pl.num_programs(0) + pid) * n_row, n_row), n_row), :] = jnp.concatenate(sums[t], axis=0)

    @pl.when(pid == pl.num_programs(0) - 1)
    def _():
        for t in range(steps):
            flat = ml_all[t].T.reshape(n_x, n_core, home, ml_all.shape[1])
            for c in range(n_core):
                ml_ref[c, :, t] = flat[:, c]


def _exchange_kernel(n_cols, n_rows, heads, dim, has_pages, *refs):
    o_ref, ml_ref, q_ref, kv_ref = refs[:I4]
    n_in = I5 if has_pages else I4
    n_out = I2 if has_pages else I1
    out_ref = refs[n_in]
    rp_o, rp_ml, cur_o, cur_ml, rel_o, rel_ml, fin_o, fin_ml, spread, expand, p_sem, r_sem, y_sem = refs[n_in + n_out:]
    n_x = n_cols // I2
    home = q_ref.shape[I0] // I2
    width = heads * dim
    at = lax.axis_index('kv')
    x, core = at // I2, at % I2
    up, dn, far = (x + I1) % n_x, (x + n_x - I1) % n_x, (x + I2) % n_x
    to_up, to_dn, to_pal = {'kv': up * I2 + core}, {'kv': dn * I2 + core}, {'kv': x * I2 + I1 - core}
    _signal_all(_x_peers(n_cols) + (_y_peers(n_rows) if has_pages else []))
    order = [far, up, dn, x]
    pals = []
    for i, pos in enumerate(order):
        pals.append(_copy(o_ref.at[I1 - core, pos], rp_o.at[i], p_sem, i, to_pal))
        pals.append(_copy(ml_ref.at[I1 - core, pos], rp_ml.at[i], p_sem, I4 + i, to_pal))
    for c in pals:
        c.start()
    if has_pages:
        pages_ref, pages_all = refs[I4], refs[n_in + I1]
        y_start, y_forward, y_finish = _rows_on_y(pages_ref, pages_all, y_sem, _half0)
        y_start()
        pages_all[lax.axis_index('kv2')] = pages_ref[...]

    n_chunk = I4
    cw = width // n_chunk
    kv_w = kv_ref.shape[I1] // I2
    kw = kv_w // n_chunk
    spread[...] = (lax.broadcasted_iota(I32, spread.shape, I1) // dim == lax.broadcasted_iota(I32, spread.shape, I0)).astype(F32).astype(BF16)
    lane = lax.broadcasted_iota(I32, expand.shape, I1)
    row = lax.broadcasted_iota(I32, expand.shape, I0)
    group = cw // kw
    expand[...] = ((lane // (dim * group) == row // dim) & (lane % dim == row % dim)).astype(F32).astype(BF16)

    def widen(w, c):
        return _pick_lhs(w, spread[:, c * cw:(c + I1) * cw], NN)

    s = jnp.zeros((I3 * home, heads), F32)
    for c in range(n_chunk):
        q_c = q_ref[:, c * cw:(c + I1) * cw].astype(F32)
        k_c = _dot(kv_ref[:, c * kw:(c + I1) * kw], expand[...], NN)
        prod = jnp.concatenate([q_c[I0:home] * k_c[I0:home], q_c[home:] * k_c[I0:home], q_c[home:] * k_c[home:]], axis=I0)
        s = s + _pick_lhs(prod, spread[:, c * cw:(c + I1) * cw], NT)
    s = s * dim ** -0.5
    s00, s10, s11 = s[I0:home], s[home:I2 * home], s[I2 * home:]
    m1 = jnp.maximum(s10, s11)
    e10, e11 = jnp.exp(s10 - m1), jnp.exp(s11 - m1)
    self_m = [s00, m1]
    self_l = [jnp.ones_like(s00), e10 + e11]
    self_w = [[(I0, None)], [(I0, e10), (I1, e11)]]

    def stats(ref):
        return ref[:, I0:heads], ref[:, heads:I2 * heads]

    def fold(a_o, a_ml, b_o, b_ml, out_o, out_ml):
        am, al = stats(a_ml)
        bm, bl = stats(b_ml)
        top = jnp.maximum(am, bm)
        aw, bw = jnp.exp(am - top), jnp.exp(bm - top)
        out_ml[:, I0:heads] = top
        out_ml[:, heads:I2 * heads] = aw * al + bw * bl
        w = jnp.concatenate([aw, bw], axis=I0)
        for c in range(n_chunk):
            wx = widen(w, c)
            sl = slice(c * cw, (c + I1) * cw)
            out_o[:, sl] = a_o[:, sl] * wx[I0:home] + b_o[:, sl] * wx[home:]

    cur_ml[...] = jnp.zeros_like(cur_ml)

    def fold_pal(i):
        _copy(o_ref.at[I1 - core, order[i]], rp_o.at[i], p_sem, i, to_pal).wait_recv()
        _copy(ml_ref.at[I1 - core, order[i]], rp_ml.at[i], p_sem, I4 + i, to_pal).wait_recv()
        for t in range(I2):
            fold(o_ref.at[core, order[i], t], ml_ref.at[core, order[i], t], rp_o.at[i, t], rp_ml.at[i, t], cur_o.at[i, t], cur_ml.at[i, t])

    sends = []

    def send(i, t, dst_o, dst_ml, k, dev):
        a = _copy(cur_o.at[i, t], dst_o, r_sem, I2 * k, dev)
        b = _copy(cur_ml.at[i, t], dst_ml, r_sem, I2 * k + I1, dev)
        a.start()
        b.start()
        sends.extend([a, b])

    def got(dst_o, dst_ml, k):
        _copy(dst_o, dst_o, r_sem, I2 * k, to_up).wait_recv()
        _copy(dst_ml, dst_ml, r_sem, I2 * k + I1, to_up).wait_recv()

    fold_pal(I0)
    send(I0, I0, rel_o.at[I0], rel_ml.at[I0], I0, to_up)
    send(I0, I1, rel_o.at[I1], rel_ml.at[I1], I1, to_dn)
    fold_pal(I1)
    send(I1, I1, fin_o.at[I0, I1], fin_ml.at[I0, I1], I2, to_up)
    fold_pal(I2)
    send(I2, I0, fin_o.at[I1, I0], fin_ml.at[I1, I0], I3, to_dn)
    got(rel_o.at[I0], rel_ml.at[I0], I0)
    fold(cur_o.at[I1, I0], cur_ml.at[I1, I0], rel_o.at[I0], rel_ml.at[I0], cur_o.at[I4, I0], cur_ml.at[I4, I0])
    send(I4, I0, fin_o.at[I0, I0], fin_ml.at[I0, I0], I4, to_up)
    got(rel_o.at[I1], rel_ml.at[I1], I1)
    fold(cur_o.at[I2, I1], cur_ml.at[I2, I1], rel_o.at[I1], rel_ml.at[I1], cur_o.at[I4, I1], cur_ml.at[I4, I1])
    send(I4, I1, fin_o.at[I1, I1], fin_ml.at[I1, I1], I5, to_dn)
    fold_pal(I3)
    if has_pages:
        y_forward()
    for side, t, k in ((I0, I1, I2), (I1, I0, I3), (I0, I0, I4), (I1, I1, I5)):
        got(fin_o.at[side, t], fin_ml.at[side, t], k)
    for t in range(I2):
        parts = [(cur_o.at[I3, t], cur_ml.at[I3, t]), (fin_o.at[I0, t], fin_ml.at[I0, t]), (fin_o.at[I1, t], fin_ml.at[I1, t])]
        ms = [stats(ml)[I0] for _, ml in parts] + [self_m[t]]
        ls = [stats(ml)[I1] for _, ml in parts] + [self_l[t]]
        top = functools.reduce(jnp.maximum, ms)
        ws = [jnp.exp(m - top) for m in ms]
        total = functools.reduce(jnp.add, [w * l for w, l in zip(ws, ls)])
        ws = [w / total for w in ws]
        own = ws.pop()
        ws += [own if e is None else own * e for _, e in self_w[t]]
        w = jnp.concatenate(ws, axis=I0)
        for c in range(n_chunk):
            wx = widen(w, c)
            sl = slice(c * cw, (c + I1) * cw)
            v_c = _dot(kv_ref[:, kv_w + c * kw:kv_w + (c + I1) * kw], expand[...], NN)
            acc = jnp.zeros((home, cw), F32)
            for i, (o, _) in enumerate(parts):
                acc = acc + o[:, sl] * wx[i * home:(i + I1) * home]
            for i, (step, _) in enumerate(self_w[t]):
                acc = acc + v_c[step * home:(step + I1) * home] * wx[(I3 + i) * home:(I4 + i) * home]
            out_ref[t * home:(t + I1) * home, sl] = acc.astype(BF16)
    if has_pages:
        y_finish()
    for c in pals + sends:
        c.wait_send()


def _place_kernel(steps, heads, n_alias, *refs):
    kn_ref, vn_ref, k_ref, v_ref, mk_ref, mv_ref, wsel_ref, mig_ref, info_ref = refs[:9]
    ko_ref, vo_ref, kv_s, full = refs[9 + n_alias:]
    page, _, dim, n_slots = k_ref.shape[1:]
    n_seq = wsel_ref.shape[0]
    width = page * dim
    n_all = mig_ref.shape[0]
    moved = info_ref[0:1, :] > 0
    w_off = info_ref[1:2, :]
    for t in range(steps):
        for which, ref in enumerate((kn_ref, vn_ref)):
            kv_s[which, t] = _dot(ref[:, t].reshape(n_seq, heads * dim), wsel_ref[...], TN)
    for h in range(heads):
        for which, (pool, pages, out) in enumerate(((k_ref, mk_ref, ko_ref), (v_ref, mv_ref, vo_ref))):
            full[...] = _dot(pages[:, 0, :, h * width:(h + 1) * width].reshape(n_all, width), mig_ref[...], TN).reshape(page, dim, n_slots)

            def fill(tok, _, which=which, pool=pool, out=out, h=h):
                val = jnp.where(moved, full[tok], pool[0, tok, h].astype(F32))
                at = w_off - tok.astype(F32)
                for t in range(steps):
                    val = jnp.where(at == -float(t), kv_s[which, t, h * dim:(h + 1) * dim, :], val)
                out[0, tok, h] = val.astype(BF16)
                return 0

            lax.fori_loop(0, page, fill, 0)


def solution(mesh):
    n_rows, n_cols = mesh.shape['kv2'], mesh.shape['kv']
    dev_axes = ('rep', 'kv2', 'kv')
    group_axes = ('kv2', 'kv')
    seq_spec = P(None, dev_axes, None)
    pool_spec = P(dev_axes, None, None, None, None)
    table_spec = P(dev_axes, None)
    vec_spec = P(dev_axes)
    full_spec = P()
    pair = 2
    vmem = pl.BlockSpec(memory_space=pltpu.VMEM)
    dma = pltpu.SemaphoreType.DMA

    def per_device(x_embed, w_query, w_key, w_value, w_out, w_up, w_down, k_pool, v_pool, old_table, seq_len, src_slot, dst_slot):
        n_slots, layers, page, kv_heads, dim = k_pool.shape
        steps, seq_dev, width = x_embed.shape
        heads = w_query.shape[2] // dim
        group = heads // kv_heads
        n_pages = old_table.shape[1]
        n_seq = seq_dev * n_cols
        n_move = src_slot.shape[0]
        n_rt = steps * group
        n_grid = kv_heads // pair
        page_w = page * dim
        n_x = n_cols // 2
        n_dev = n_rows * n_cols
        rows = steps * seq_dev
        me = lax.axis_index('kv2') * n_cols + lax.axis_index('kv')
        slot_base = me * n_slots
        k_t = jnp.transpose(k_pool, (1, 2, 3, 4, 0))
        v_t = jnp.transpose(v_pool, (1, 2, 3, 4, 0))
        q_w, kv_w, m_w = pair * group * dim, pair * dim, pair * page_w

        def fixed(shape):
            return pl.BlockSpec(shape, lambda i: (0,) * len(shape), pipeline_mode=pl.Buffered(1))

        src_hot = ((src_slot - slot_base)[:, None] == jnp.arange(n_slots, dtype=I32)[None, :]).astype(BF16)
        page_shape = (2, n_move, kv_heads * page_w)

        def pool_blk(layer):
            return pl.BlockSpec((1, page, pair, dim, n_slots), lambda i: (layer, 0, i, 0, 0))

        def pack(layer):
            blk = pool_blk(layer)
            return pl.pallas_call(
                functools.partial(_pack_kernel, pair),
                grid=(n_grid,),
                in_specs=[pl.BlockSpec((n_move, n_slots), lambda i: (0, 0)), blk, blk],
                out_specs=pl.BlockSpec((2, n_move, m_w), lambda i: (0, 0, i)),
                out_shape=jax.ShapeDtypeStruct(page_shape, BF16),
                cost_estimate=pl.CostEstimate(flops=4 * 10**9, bytes_accessed=8 * 2**20, transcendentals=0),
                name='pack_pages',
            )(src_hot, k_t, v_t)

        packed = [pack(layer) for layer in range(layers)]
        moved = [lax.all_gather(p, group_axes) for p in packed]

        def project(hidden, layer):
            q = jnp.dot(hidden, w_query[layer], preferred_element_type=F32).astype(BF16)
            kv = jnp.concatenate([jnp.dot(hidden, w[layer], preferred_element_type=F32).astype(BF16) for w in (w_key, w_value)], axis=1)
            return q, kv

        hidden = x_embed.reshape(rows, width)
        q, kv = project(hidden, 0)
        meta = jnp.concatenate([old_table.T.reshape(-1), seq_len, src_slot, dst_slot])
        n_meta = meta.shape[0]
        meta = jnp.pad(meta, (0, 8 * 128 - n_meta)).reshape(8, 128)
        pages_all_shape = jax.ShapeDtypeStruct((n_rows,) + page_shape, BF16)
        q_all_shape = jax.ShapeDtypeStruct((n_cols, rows, heads * dim), BF16)
        meta_all, pages_y, q_all = pl.pallas_call(
            functools.partial(_head_kernel, n_rows, n_cols),
            in_specs=[vmem] * 3,
            out_specs=[vmem] * 3,
            out_shape=[jax.ShapeDtypeStruct((n_dev, 8, 128), I32), pages_all_shape, q_all_shape],
            scratch_shapes=[dma((2, n_dev - 1)), dma((2, 6)), dma((2, 13))],
            compiler_params=pltpu.CompilerParams(collective_id=0, has_side_effects=True, vmem_limit_bytes=24 * 2**20),
            cost_estimate=pl.CostEstimate(flops=10**10, bytes_accessed=2**22, transcendentals=0),
            name='head_gather',
        )(meta, packed[0], q)

        meta_all = meta_all.reshape(n_dev, 8 * 128)[:, :n_meta]
        n_tab = n_pages * seq_dev
        row = lax.dynamic_slice_in_dim(meta_all, lax.axis_index('kv2') * n_cols, n_cols, axis=0)
        old_col = row[:, :n_tab].reshape(n_cols, n_pages, seq_dev).transpose(1, 0, 2).reshape(-1, 1)
        len_col = row[:, n_tab:n_tab + seq_dev].reshape(-1, 1)
        src_all = meta_all[:, n_tab + seq_dev:n_tab + seq_dev + n_move].reshape(1, -1)
        dst_all = meta_all[:, n_tab + seq_dev + n_move:].reshape(1, -1)
        n_all = n_dev * n_move
        n_arr = n_rows * n_move
        pos = jnp.stack([slot_base, lax.axis_index('kv')]).astype(I32)
        q_sel, cells, arr, info, w_sel, mig, w_info = pl.pallas_call(
            functools.partial(_prep_kernel, n_pages, page, n_cols, n_slots),
            in_specs=[vmem] * 7 + [pl.BlockSpec(memory_space=pltpu.SMEM)],
            out_specs=[vmem] * 7,
            out_shape=[
                jax.ShapeDtypeStruct((n_seq, LANES), BF16),
                jax.ShapeDtypeStruct((n_pages * n_seq, LANES), BF16),
                jax.ShapeDtypeStruct((n_arr, LANES), BF16),
                jax.ShapeDtypeStruct((8, LANES), F32),
                jax.ShapeDtypeStruct((n_seq, n_slots), BF16),
                jax.ShapeDtypeStruct((n_all, n_slots), BF16),
                jax.ShapeDtypeStruct((8, n_slots), F32),
            ],
            name='prep_tables',
        )(old_col, src_all, dst_all, dst_all.reshape(-1, 1), len_col, src_slot.reshape(1, -1), src_slot.reshape(-1, 1), pos)

        def attend(layer, q_all, pages):
            blk = pool_blk(layer)
            ml_rows = 2 * LANES // 4
            return pl.pallas_call(
                functools.partial(_attn_kernel, steps, group, pair),
                grid=(n_grid,),
                in_specs=[
                    pl.BlockSpec((n_cols, steps, seq_dev, q_w), lambda i: (0, 0, 0, i)),
                    blk, blk,
                    pl.BlockSpec((n_rows, 1, n_move, m_w), lambda i: (0, 0, 0, i)),
                    pl.BlockSpec((n_rows, 1, n_move, m_w), lambda i: (0, 1, 0, i)),
                    fixed(q_sel.shape), fixed(cells.shape), fixed(arr.shape), fixed(info.shape),
                ],
                out_specs=[
                    pl.BlockSpec((2, n_x, steps, seq_dev, q_w), lambda i: (0, 0, 0, 0, i)),
                    pl.BlockSpec((2, n_x, steps, seq_dev, ml_rows), lambda i: (0, 0, 0, 0, 0)),
                ],
                out_shape=[
                    jax.ShapeDtypeStruct((2, n_x, steps, seq_dev, heads * dim), F32),
                    jax.ShapeDtypeStruct((2, n_x, steps, seq_dev, ml_rows), F32),
                ],
                scratch_shapes=[
                    pltpu.VMEM((steps, q_w, LANES), F32),
                    pltpu.VMEM((page, dim, LANES), F32),
                    pltpu.VMEM((page, dim, LANES), F32),
                    pltpu.VMEM((n_rt, page, LANES), F32),
                    pltpu.VMEM((n_rt * dim, LANES), F32),
                    pltpu.VMEM((2 * n_rt, LANES), F32),
                    pltpu.VMEM((steps, ml_rows, n_seq), F32),
                ],
                compiler_params=pltpu.CompilerParams(vmem_limit_bytes=32 * 2**20),
                cost_estimate=pl.CostEstimate(flops=20 * 10**9, bytes_accessed=16 * 2**20, transcendentals=0),
                name='slot_attention',
            )(q_all.reshape(n_cols, steps, seq_dev, heads * dim), k_t, v_t, pages, pages, q_sel, cells, arr, info)

        def exchange(layer, o, ml, q, kv, pages):
            has = pages is not None
            half = (seq_dev, heads * dim)
            stat = (seq_dev, ml.shape[-1])
            out_shape = [jax.ShapeDtypeStruct((rows, heads * dim), BF16)] + ([pages_all_shape] if has else [])
            return pl.pallas_call(
                functools.partial(_exchange_kernel, n_cols, n_rows, heads, dim, has),
                in_specs=[vmem] * (5 if has else 4),
                out_specs=[vmem] * len(out_shape),
                out_shape=out_shape,
                scratch_shapes=[
                    pltpu.VMEM((4, steps) + half, F32), pltpu.VMEM((4, steps) + stat, F32),
                    pltpu.VMEM((5, steps) + half, F32), pltpu.VMEM((5, steps) + stat, F32),
                    pltpu.VMEM((2,) + half, F32), pltpu.VMEM((2,) + stat, F32),
                    pltpu.VMEM((2, steps) + half, F32), pltpu.VMEM((2, steps) + stat, F32),
                    pltpu.VMEM((heads, heads * dim), BF16), pltpu.VMEM((kv_w, q_w), BF16),
                    dma((2, 8)), dma((2, 12)), dma((2, 6)),
                ],
                compiler_params=pltpu.CompilerParams(collective_id=1 + layer, has_side_effects=True, vmem_limit_bytes=32 * 2**20),
                cost_estimate=pl.CostEstimate(flops=10**10, bytes_accessed=2**22, transcendentals=0),
                name='exchange_partials',
            )(o, ml, q, kv, *([pages] if has else []))

        def place(layer, kv_row, k_prev, v_prev):
            blk = pool_blk(layer)
            v_at = kv_heads * dim // kv_w
            in_specs = [
                pl.BlockSpec((n_cols, steps, seq_dev, kv_w), lambda i: (0, 0, 0, i)),
                pl.BlockSpec((n_cols, steps, seq_dev, kv_w), lambda i: (0, 0, 0, v_at + i)),
                blk, blk,
                pl.BlockSpec((n_dev, 1, n_move, m_w), lambda i: (0, 0, 0, i)),
                pl.BlockSpec((n_dev, 1, n_move, m_w), lambda i: (0, 1, 0, i)),
                fixed(w_sel.shape), fixed(mig.shape), fixed(w_info.shape),
            ]
            kv4 = kv_row.reshape(n_cols, steps, seq_dev, -1)
            args = [kv4, kv4, k_t, v_t, moved[layer], moved[layer], w_sel, mig, w_info]
            aliases = {}
            if k_prev is not None:
                in_specs += [pl.BlockSpec(memory_space=pl.ANY)] * 2
                aliases = {len(args): 0, len(args) + 1: 1}
                args += [k_prev, v_prev]
            return pl.pallas_call(
                functools.partial(_place_kernel, steps, pair, len(aliases)),
                grid=(n_grid,),
                in_specs=in_specs,
                out_specs=[blk, blk],
                out_shape=[jax.ShapeDtypeStruct(k_t.shape, BF16), jax.ShapeDtypeStruct(v_t.shape, BF16)],
                scratch_shapes=[pltpu.VMEM((2, steps, kv_w, n_slots), F32), pltpu.VMEM((page, dim, n_slots), F32)],
                input_output_aliases=aliases,
                compiler_params=pltpu.CompilerParams(vmem_limit_bytes=32 * 2**20),
                cost_estimate=pl.CostEstimate(flops=20 * 10**9, bytes_accessed=32 * 2**20, transcendentals=0),
                name='place_pages',
            )(*args)

        k_out = v_out = None
        kv_rows = []
        for layer in range(layers):
            if layer:
                q, kv = project(hidden, layer)
                [q_all] = pl.pallas_call(
                    functools.partial(_query_kernel, n_cols),
                    in_specs=[vmem],
                    out_specs=[vmem],
                    out_shape=[q_all_shape],
                    scratch_shapes=[dma((2, 13))],
                    compiler_params=pltpu.CompilerParams(collective_id=1 + layers + layer, has_side_effects=True, vmem_limit_bytes=16 * 2**20),
                    cost_estimate=pl.CostEstimate(flops=5 * 10**9, bytes_accessed=2**22, transcendentals=0),
                    name='query_gather',
                )(q)
            kv_rows.append(lax.all_gather(kv, 'kv'))
            o, ml = attend(layer, q_all, pages_y)
            nxt = packed[layer + 1] if layer + 1 < layers else None
            attn, *more = exchange(layer, o, ml, q, kv, nxt)
            pages_y = more[0] if more else None
            hidden = (hidden.astype(F32) + jnp.dot(attn, w_out[layer], preferred_element_type=F32)).astype(BF16)
            up_act = jax.nn.gelu(jnp.dot(hidden, w_up[layer], preferred_element_type=F32)).astype(BF16)
            hidden = (hidden.astype(F32) + jnp.dot(up_act, w_down[layer], preferred_element_type=F32)).astype(BF16)
        for layer in range(layers):
            k_out, v_out = place(layer, kv_rows[layer], k_out, v_out)
        y_out = hidden.reshape(steps, seq_dev, width)
        back = (4, 0, 1, 2, 3)
        return y_out, jnp.transpose(k_out, back), jnp.transpose(v_out, back)

    return jax.shard_map(per_device, mesh=mesh, in_specs=(seq_spec, full_spec, full_spec, full_spec, full_spec, full_spec, full_spec, pool_spec, pool_spec, table_spec, vec_spec, vec_spec, vec_spec), out_specs=(seq_spec, pool_spec, pool_spec), check_vma=False)
```

```python
import functools

import jax
import jax.numpy as jnp
from jax import lax
from jax.experimental import pallas as pl
from jax.experimental.pallas import tpu as pltpu
from jax.sharding import PartitionSpec as P

F32 = jnp.float32
BF16 = jnp.bfloat16
I32 = jnp.int32
NEG = -1e30
NN = (((1,), (0,)), ((), ()))
NT = (((1,), (1,)), ((), ()))
TN = (((0,), (0,)), ((), ()))
MESH = pl.DeviceIdType.MESH
LANES = 256
MIB = 2**20
I0, I1, I2, I3, I4, I5 = range(6)


def _cost(gflops, mib):
    return pl.CostEstimate(flops=gflops * 10**9, bytes_accessed=mib * MIB, transcendentals=0)


def _dot(a, b, dims):
    return lax.dot_general(a, b, dims, preferred_element_type=F32)


def _split(x):
    hi = x.astype(BF16)
    rest = x - hi.astype(F32)
    mid = rest.astype(BF16)
    low = (rest - mid.astype(F32)).astype(BF16)
    return hi, mid, low


def _pick_lhs(x, sel, dims):
    hi, mid, low = _split(x)
    return _dot(hi, sel, dims) + _dot(mid, sel, dims) + _dot(low, sel, dims)


def _pick_rhs(sel, x, dims):
    hi, mid, low = _split(x)
    return _dot(sel, hi, dims) + _dot(sel, mid, dims) + _dot(sel, low, dims)


def _columns(rows):
    full = jnp.concatenate([rows, jnp.zeros((LANES // 2 - rows.shape[0], rows.shape[1]), F32)], axis=0).T
    ids = lax.broadcasted_iota(I32, full.shape, 1)

    def column(i):
        return jnp.sum(jnp.where(ids == i, full, 0.0), axis=1, keepdims=True).astype(I32)

    return column


def _tables(dims, meta_all, mysrc_ref, mysrcc_ref, qsel_ref, cell_ref, arr_ref, info_ref, wsel_ref, mig_ref, winfo_ref):
    n_rows, n_cols, n_slots, n_pages, page, seq_dev = dims
    y, my_col = lax.axis_index('kv2'), lax.axis_index('kv')
    base = (y * n_cols + my_col) * n_slots
    n_seq = n_cols * seq_dev
    n_move = mysrc_ref.shape[1]
    n_arr = arr_ref.shape[0]
    spare = LANES - n_slots
    src = jnp.sum(meta_all[:, 8:16, :], axis=0)
    dst = jnp.sum(meta_all[:, 16:24, :], axis=0)
    tab = jnp.concatenate([meta_all[y * n_cols + i, 0:1, :] for i in range(n_cols)], axis=0).astype(F32)
    column = _columns(tab)
    tabs = [column(i) for i in range(n_cols)]
    old = jnp.concatenate([c[j * seq_dev:(j + 1) * seq_dev] for j in range(n_pages) for c in tabs], axis=0)
    lens = jnp.concatenate([c[n_pages * seq_dev:] for c in tabs], axis=0)
    per_row = n_cols * n_move
    ids = lax.broadcasted_iota(I32, (1, per_row), 1)
    entry = jnp.zeros(old.shape, F32)
    to = jnp.zeros(old.shape, F32)
    for r in range(n_rows):
        hit = old == src[r:r + 1]
        entry = entry + jnp.sum(jnp.where(hit, ids + (r * per_row + 1), 0).astype(F32), axis=1, keepdims=True)
        to = to + jnp.sum(jnp.where(hit, dst[r:r + 1] + 1, 0).astype(F32), axis=1, keepdims=True)
    entry = entry.astype(I32) - 1
    to = to.astype(I32) - 1
    is_moved = entry >= 0
    dev = entry // n_move
    nth = entry - dev * n_move
    arrival = (dev // n_cols) * n_move + nth
    free = jnp.sum(jnp.where(nth == lax.broadcasted_iota(I32, (1, n_move), 1), mysrc_ref[...] - base, 0).astype(F32), axis=1, keepdims=True).astype(I32)
    arr_lane = jnp.where(arrival < spare, n_slots + arrival, free)
    here = old - base
    here = jnp.where((here >= 0) & (here < n_slots), here, -1)
    lane = jnp.where(is_moved, jnp.where(dev % n_cols == my_col, arr_lane, -1), here)
    final = jnp.where(is_moved, to, old) - base
    lane_ids = lax.broadcasted_iota(I32, (1, LANES), 1)
    slot_ids = lax.broadcasted_iota(I32, (1, n_slots), 1)
    last = lens // page
    q_sel = jnp.zeros((n_seq, LANES), F32)
    w_sel = jnp.zeros((n_seq, n_slots), F32)
    first = jnp.zeros((1, LANES), F32)
    for j in range(n_pages):
        eq = (lane[j * n_seq:(j + 1) * n_seq] == lane_ids).astype(F32)
        cell_ref[j * n_seq:(j + 1) * n_seq, :] = eq.astype(BF16)
        q_sel = q_sel + eq
        first = first + jnp.sum(eq, axis=0, keepdims=True) * float(j * page)
        w_sel = w_sel + jnp.where((final[j * n_seq:(j + 1) * n_seq] == slot_ids) & (last == j), 1.0, 0.0)
    qsel_ref[...] = q_sel.astype(BF16)
    wsel_ref[...] = w_sel.astype(BF16)
    used = jnp.sum(q_sel, axis=0, keepdims=True)
    slot_len = jnp.sum(q_sel * lens.astype(F32), axis=0, keepdims=True)
    arr_ids = lax.broadcasted_iota(I32, (n_arr, LANES), 0)
    arr_ref[...] = jnp.where(lane_ids == n_slots + arr_ids, 1.0, 0.0).astype(BF16)
    mine = mysrcc_ref[...] - base
    arr_ref[spare:n_arr, :] = jnp.where(lane_ids == mine, 1.0, 0.0).astype(BF16)
    out_lanes = jnp.sum(jnp.where(mine == lane_ids, 1.0, 0.0), axis=0, keepdims=True)
    info_ref[...] = jnp.zeros_like(info_ref)
    info_ref[0:1, :] = used
    info_ref[1:2, :] = jnp.where(used > 0, slot_len - first - 1.0, -100.0)
    info_ref[2:3, :] = jnp.where(lane_ids >= n_slots, 1.0, out_lanes)
    written = jnp.sum(w_sel, axis=0, keepdims=True)
    w_off = jnp.sum(w_sel * (lens - last * page).astype(F32), axis=0, keepdims=True)
    to_col = _columns(dst.astype(F32))
    dst_col = jnp.concatenate([to_col(r) for r in range(n_rows)], axis=0)
    mig = jnp.where(dst_col - base == slot_ids, 1.0, 0.0)
    mig_ref[...] = mig.astype(BF16)
    winfo_ref[...] = jnp.zeros_like(winfo_ref)
    winfo_ref[0:1, :] = jnp.sum(mig, axis=0, keepdims=True)
    winfo_ref[1:2, :] = jnp.where(written > 0, w_off, -100.0)


def _pack_kernel(heads, onehot_ref, k_ref, v_ref, out_ref):
    page, _, dim, n_slots = k_ref.shape[1:]
    width = page * dim
    for h in range(heads):
        for which, src in enumerate((k_ref, v_ref)):
            rows = src[0, :, h].reshape(width, n_slots)
            out_ref[0, which, :, h * width:(h + 1) * width] = _dot(onehot_ref[...], rows, NT).astype(BF16)


def _copy(src, dst, sems, k, dev):
    return pltpu.make_async_remote_copy(src_ref=src, dst_ref=dst, send_sem=sems.at[0, k], recv_sem=sems.at[1, k], device_id=dev, device_id_type=MESH)


def _rows_on_y(own, out, sems, halves):
    n = out.shape[I0]
    y = lax.axis_index('kv2')
    up, dn, far = (y + I1) % n, (y + n - I1) % n, (y + I2) % n
    to_up, to_dn = {'kv2': up}, {'kv2': dn}
    first = [
        _copy(halves(own, I0), halves(out.at[y], I0), sems, I0, to_up),
        _copy(halves(own, I1), halves(out.at[y], I1), sems, I1, to_up),
        _copy(halves(own, I1), halves(out.at[y], I1), sems, I2, to_dn),
        _copy(halves(own, I0), halves(out.at[y], I0), sems, I3, to_dn),
    ]
    relay = [
        _copy(halves(out.at[dn], I0), halves(out.at[dn], I0), sems, I4, to_up),
        _copy(halves(out.at[up], I1), halves(out.at[up], I1), sems, I5, to_dn),
    ]
    lands = [(dn, I0), (dn, I1), (up, I1), (up, I0), (far, I0), (far, I1)]

    def got(k):
        at, h = lands[k]
        _copy(halves(out.at[at], h), halves(out.at[at], h), sems, k, to_up).wait_recv()

    def start():
        for k in (I0, I2, I1, I3):
            first[k].start()

    def forward():
        got(I0)
        relay[I0].start()
        got(I2)
        relay[I1].start()

    def finish():
        for k in (I1, I3, I4, I5):
            got(k)
        for c in first + relay:
            c.wait_send()

    return start, forward, finish


def _signal_all(devs):
    barrier = pltpu.get_barrier_semaphore()
    for dev in devs:
        pl.semaphore_signal(barrier, inc=1, device_id=dev, device_id_type=MESH)
    pl.semaphore_wait(barrier, len(devs))


def _q_gather(n_cols, q_ref, q_all, x_sem):
    n_x = n_cols // I2
    at = lax.axis_index('kv')
    x, core = at // I2, at % I2
    up, dn, far = (x + I1) % n_x, (x + n_x - I1) % n_x, (x + I2) % n_x
    to_up, to_dn, to_pal = {'kv': up * I2 + core}, {'kv': dn * I2 + core}, {'kv': x * I2 + I1 - core}
    n_half = q_ref.shape[I0] // I2

    def half(ref, h):
        return ref.at[pl.ds(h * n_half, n_half)]

    def slot(pos, c):
        return q_all.at[pos * I2 + c]

    first = [
        _copy(half(q_ref, I0), half(slot(x, core), I0), x_sem, I0, to_up),
        _copy(half(q_ref, I1), half(slot(x, core), I1), x_sem, I1, to_up),
        _copy(half(q_ref, I1), half(slot(x, core), I1), x_sem, I2, to_dn),
        _copy(half(q_ref, I0), half(slot(x, core), I0), x_sem, I3, to_dn),
    ]
    relay = [
        _copy(half(slot(dn, core), I0), half(slot(dn, core), I0), x_sem, I4, to_up),
        _copy(half(slot(up, core), I1), half(slot(up, core), I1), x_sem, I5, to_dn),
    ]
    lands = [(dn, I0), (dn, I1), (up, I1), (up, I0), (far, I0), (far, I1)]
    pal = [_copy(half(slot(p, core), h), half(slot(p, core), h), x_sem, 6 + k, to_pal) for k, (p, h) in enumerate(lands)]
    own = _copy(q_ref, slot(x, core), x_sem, 12, to_pal)

    def got(k):
        p, h = lands[k]
        _copy(half(slot(p, core), h), half(slot(p, core), h), x_sem, k, to_up).wait_recv()

    for k in (I0, I2, I1, I3):
        first[k].start()
    own.start()
    q_all[at] = q_ref[...]
    yield
    got(I0)
    relay[I0].start()
    pal[I0].start()
    got(I2)
    relay[I1].start()
    pal[I2].start()
    yield
    for k in (I1, I3, I4, I5):
        got(k)
        pal[k].start()
    yield
    _copy(q_ref, slot(x, I1 - core), x_sem, 12, to_pal).wait_recv()
    for k, (p, h) in enumerate(lands):
        _copy(half(slot(p, I1 - core), h), half(slot(p, I1 - core), h), x_sem, 6 + k, to_pal).wait_recv()
    for c in first + relay + pal + [own]:
        c.wait_send()


def _x_peers(n_cols):
    n_x = n_cols // I2
    at = lax.axis_index('kv')
    x, core = at // I2, at % I2
    return [{'kv': ((x + I1) % n_x) * I2 + core}, {'kv': ((x + n_x - I1) % n_x) * I2 + core}, {'kv': x * I2 + I1 - core}]


def _y_peers(n_rows):
    y = lax.axis_index('kv2')
    return [{'kv2': (y + I1) % n_rows}, {'kv2': (y + n_rows - I1) % n_rows}]


def _half0(ref, h):
    return ref.at[h]


def _head_kernel(dims, meta_ref, pages_ref, q_ref, mysrc_ref, mysrcc_ref, pages_all, q_all, *refs):
    tables, (meta_all, m_sem, y_sem, x_sem) = refs[:7], refs[7:]
    n_rows, n_cols = dims[:2]
    pages_ref = pages_ref.at[0]
    y, at = lax.axis_index('kv2'), lax.axis_index('kv')
    offsets = [(a, b) for a in range(n_rows) for b in range(n_cols) if (a, b) != (0, 0)]
    peers = [{'kv2': (y + a) % n_rows, 'kv': (at + b) % n_cols} for a, b in offsets]
    _signal_all(peers)
    me = y * n_cols + at
    metas = [_copy(meta_ref, meta_all.at[me], m_sem, k, peers[k]) for k in range(len(peers))]
    for c in metas:
        c.start()
    start, forward, finish = _rows_on_y(pages_ref, pages_all, y_sem, _half0)
    start()
    steps = _q_gather(n_cols, q_ref, q_all, x_sem)
    next(steps)
    meta_all[me] = meta_ref[...]
    pages_all[y] = pages_ref[...]
    next(steps)
    forward()
    for k, (a, b) in enumerate(offsets):
        frm = ((y + n_rows - a) % n_rows) * n_cols + (at + n_cols - b) % n_cols
        _copy(meta_ref, meta_all.at[frm], m_sem, k, peers[k]).wait_recv()
    _tables(dims, meta_all, mysrc_ref, mysrcc_ref, *tables)
    next(steps)
    finish()
    for _ in steps:
        pass
    for c in metas:
        c.wait_send()


def _query_kernel(n_cols, q_ref, q_all, x_sem):
    _signal_all(_x_peers(n_cols))
    for _ in _q_gather(n_cols, q_ref, q_all, x_sem):
        pass


def _attn_kernel(steps, group, heads, q_ref, k_ref, v_ref, mk_ref, mv_ref, qsel_ref, cell_ref, arr_ref, info_ref, o_ref, ml_ref, q_s, mk_s, mv_s, s_s, os_s, ml_s, ml_all):
    page, _, dim, n_slots = k_ref.shape[1:]
    n_seq = qsel_ref.shape[0]
    n_core, n_x, _, home = o_ref.shape[:4]
    n_arr = arr_ref.shape[0]
    pid = pl.program_id(0)
    n_rt = steps * group
    width = page * dim
    used = info_ref[0:1, :]
    limit = info_ref[1:2, :]
    freed = info_ref[2:3, 0:n_slots] > 0
    cells = cell_ref[...]
    owned = _dot(jnp.ones((8, LANES), BF16), cells, NT)[0:1] > 0
    scale = dim ** -0.5
    q_sel = qsel_ref[...]

    @pl.when(pid == 0)
    def _():
        ml_all[...] = jnp.zeros_like(ml_all)

    for t in range(steps):
        q_s[t] = _dot(q_ref[:, t].reshape(n_seq, heads * group * dim), q_sel, TN)
    tops, sums = [[] for _ in range(steps)], [[] for _ in range(steps)]
    for h in range(heads):
        for pages, full in ((mk_ref, mk_s), (mv_ref, mv_s)):
            full[...] = _dot(pages[:, 0, :, h * width:(h + 1) * width].reshape(n_arr, width), arr_ref[...], TN).reshape(page, dim, LANES)

        def join(tok, _, h=h):
            for pool, full in ((k_ref, mk_s), (v_ref, mv_s)):
                full[tok, :, 0:n_slots] = jnp.where(freed, full[tok, :, 0:n_slots], pool[0, tok, h].astype(F32))
            return 0

        lax.fori_loop(0, page, join, 0)

        def score(pair, _, h=h):
            toks = [pair * 2, pair * 2 + 1]
            keys = [mk_s[tok] for tok in toks]
            for t in range(steps):
                for r in range(group):
                    q_row = q_s[t, (h * group + r) * dim:(h * group + r + 1) * dim, :]
                    for tok, key in zip(toks, keys):
                        s_s[t * group + r, pl.ds(tok, 1), :] = jnp.sum(key * q_row, axis=0, keepdims=True)
            return 0

        lax.fori_loop(0, page // 2, score, 0)
        visible = lax.broadcasted_iota(I32, (page, LANES), 0).astype(F32) <= limit
        for rt in range(n_rt):
            sc = jnp.where(visible, s_s[rt] * scale, NEG)
            top = jnp.max(sc, axis=0, keepdims=True)
            ex = jnp.where(visible, jnp.exp(sc - top), 0.0)
            s_s[rt] = ex
            ml_s[rt:rt + 1, :] = top
            ml_s[n_rt + rt:n_rt + rt + 1, :] = jnp.sum(ex, axis=0, keepdims=True)
        live = (used > 0) & (limit >= 0)
        m_slot = ml_s[0:n_rt]
        l_slot = ml_s[n_rt:2 * n_rt]
        m_cell = jnp.where(owned, _pick_lhs(m_slot, cells, NT), NEG)
        m_seq = m_cell[:, 0:n_seq]
        for j in range(1, cells.shape[0] // n_seq):
            m_seq = jnp.maximum(m_seq, m_cell[:, j * n_seq:(j + 1) * n_seq])
        m_back = _pick_lhs(m_seq, q_sel, NN)
        w_slot = jnp.where(live, jnp.exp(jnp.minimum(m_slot - m_back, 0.0)), 0.0)
        l_seq = _pick_lhs(l_slot * w_slot, q_sel, NT)
        for t in range(steps):
            tops[t].append(m_seq[t * group:(t + 1) * group])
            sums[t].append(l_seq[t * group:(t + 1) * group])
        for rt in range(n_rt):
            s_s[rt] = s_s[rt] * w_slot[rt:rt + 1]

        def weigh(c, _):
            row = pl.multiple_of(c * 8, 8)
            acc = [jnp.zeros((8, LANES), F32) for _ in range(n_rt)]
            for tok in range(page):
                vals = mv_s[tok, pl.ds(row, 8), :]
                for rt in range(n_rt):
                    acc[rt] = acc[rt] + s_s[rt, tok:tok + 1, :] * vals
            for rt in range(n_rt):
                os_s[pl.ds(rt * dim + row, 8), :] = acc[rt]
            return 0

        lax.fori_loop(0, dim // 8, weigh, 0)
        for t in range(steps):
            part = _pick_rhs(q_sel, os_s[t * group * dim:(t + 1) * group * dim, :], NT).reshape(n_x, n_core, home, group * dim)
            for c in range(n_core):
                o_ref[c, :, t, :, h * group * dim:(h + 1) * group * dim] = part[:, c]

    n_row = heads * group
    for t in range(steps):
        ml_all[t, pl.ds(pl.multiple_of(pid * n_row, n_row), n_row), :] = jnp.concatenate(tops[t], axis=0)
        ml_all[t, pl.ds(pl.multiple_of((pl.num_programs(0) + pid) * n_row, n_row), n_row), :] = jnp.concatenate(sums[t], axis=0)

    @pl.when(pid == pl.num_programs(0) - 1)
    def _():
        for t in range(steps):
            flat = ml_all[t].T.reshape(n_x, n_core, home, ml_all.shape[1])
            for c in range(n_core):
                ml_ref[c, :, t] = flat[:, c]


def _exchange_kernel(n_cols, n_rows, heads, dim, has_pages, *refs):
    o_ref, ml_ref, q_ref, kv_ref = refs[:I4]
    n_in = I5 if has_pages else I4
    n_out = I2 if has_pages else I1
    out_ref = refs[n_in]
    rp_o, rp_ml, cur_o, cur_ml, rel_o, rel_ml, fin_o, fin_ml, spread, expand, p_sem, r_sem, y_sem = refs[n_in + n_out:]
    n_x = n_cols // I2
    home = q_ref.shape[I0] // I2
    width = heads * dim
    at = lax.axis_index('kv')
    x, core = at // I2, at % I2
    up, dn, far = (x + I1) % n_x, (x + n_x - I1) % n_x, (x + I2) % n_x
    to_up, to_dn, to_pal = {'kv': up * I2 + core}, {'kv': dn * I2 + core}, {'kv': x * I2 + I1 - core}
    _signal_all(_x_peers(n_cols) + (_y_peers(n_rows) if has_pages else []))
    order = [far, up, dn, x]
    pals = []
    for i, pos in enumerate(order):
        pals.append(_copy(o_ref.at[I1 - core, pos], rp_o.at[i], p_sem, i, to_pal))
        pals.append(_copy(ml_ref.at[I1 - core, pos], rp_ml.at[i], p_sem, I4 + i, to_pal))
    for c in pals:
        c.start()
    if has_pages:
        pages_ref, pages_all = refs[I4].at[I1], refs[n_in + I1]
        y_start, y_forward, y_finish = _rows_on_y(pages_ref, pages_all, y_sem, _half0)
        y_start()
        pages_all[lax.axis_index('kv2')] = pages_ref[...]

    n_chunk = I4
    cw = width // n_chunk
    kv_w = kv_ref.shape[I1] // I2
    kw = kv_w // n_chunk
    spread[...] = (lax.broadcasted_iota(I32, spread.shape, I1) // dim == lax.broadcasted_iota(I32, spread.shape, I0)).astype(F32).astype(BF16)
    lane = lax.broadcasted_iota(I32, expand.shape, I1)
    row = lax.broadcasted_iota(I32, expand.shape, I0)
    group = cw // kw
    expand[...] = ((lane // (dim * group) == row // dim) & (lane % dim == row % dim)).astype(F32).astype(BF16)

    def widen(w, c):
        return _pick_lhs(w, spread[:, c * cw:(c + I1) * cw], NN)

    s = jnp.zeros((I3 * home, heads), F32)
    for c in range(n_chunk):
        q_c = q_ref[:, c * cw:(c + I1) * cw].astype(F32)
        k_c = _dot(kv_ref[:, c * kw:(c + I1) * kw], expand[...], NN)
        prod = jnp.concatenate([q_c[I0:home] * k_c[I0:home], q_c[home:] * k_c[I0:home], q_c[home:] * k_c[home:]], axis=I0)
        s = s + _pick_lhs(prod, spread[:, c * cw:(c + I1) * cw], NT)
    s = s * dim ** -0.5
    s00, s10, s11 = s[I0:home], s[home:I2 * home], s[I2 * home:]
    m1 = jnp.maximum(s10, s11)
    e10, e11 = jnp.exp(s10 - m1), jnp.exp(s11 - m1)
    self_m = [s00, m1]
    self_l = [jnp.ones_like(s00), e10 + e11]
    self_w = [[(I0, None)], [(I0, e10), (I1, e11)]]

    def stats(ref):
        return ref[:, I0:heads], ref[:, heads:I2 * heads]

    def fold(a_o, a_ml, b_o, b_ml, out_o, out_ml):
        am, al = stats(a_ml)
        bm, bl = stats(b_ml)
        top = jnp.maximum(am, bm)
        aw, bw = jnp.exp(am - top), jnp.exp(bm - top)
        out_ml[:, I0:heads] = top
        out_ml[:, heads:I2 * heads] = aw * al + bw * bl
        w = jnp.concatenate([aw, bw], axis=I0)
        for c in range(n_chunk):
            wx = widen(w, c)
            sl = slice(c * cw, (c + I1) * cw)
            out_o[:, sl] = a_o[:, sl] * wx[I0:home] + b_o[:, sl] * wx[home:]

    cur_ml[...] = jnp.zeros_like(cur_ml)

    def fold_pal(i):
        _copy(o_ref.at[I1 - core, order[i]], rp_o.at[i], p_sem, i, to_pal).wait_recv()
        _copy(ml_ref.at[I1 - core, order[i]], rp_ml.at[i], p_sem, I4 + i, to_pal).wait_recv()
        for t in range(I2):
            fold(o_ref.at[core, order[i], t], ml_ref.at[core, order[i], t], rp_o.at[i, t], rp_ml.at[i, t], cur_o.at[i, t], cur_ml.at[i, t])

    sends = []

    def send(i, t, dst_o, dst_ml, k, dev):
        a = _copy(cur_o.at[i, t], dst_o, r_sem, I2 * k, dev)
        b = _copy(cur_ml.at[i, t], dst_ml, r_sem, I2 * k + I1, dev)
        a.start()
        b.start()
        sends.extend([a, b])

    def got(dst_o, dst_ml, k):
        _copy(dst_o, dst_o, r_sem, I2 * k, to_up).wait_recv()
        _copy(dst_ml, dst_ml, r_sem, I2 * k + I1, to_up).wait_recv()

    fold_pal(I0)
    send(I0, I0, rel_o.at[I0], rel_ml.at[I0], I0, to_up)
    send(I0, I1, rel_o.at[I1], rel_ml.at[I1], I1, to_dn)
    fold_pal(I1)
    send(I1, I1, fin_o.at[I0, I1], fin_ml.at[I0, I1], I2, to_up)
    fold_pal(I2)
    send(I2, I0, fin_o.at[I1, I0], fin_ml.at[I1, I0], I3, to_dn)
    got(rel_o.at[I0], rel_ml.at[I0], I0)
    fold(cur_o.at[I1, I0], cur_ml.at[I1, I0], rel_o.at[I0], rel_ml.at[I0], cur_o.at[I4, I0], cur_ml.at[I4, I0])
    send(I4, I0, fin_o.at[I0, I0], fin_ml.at[I0, I0], I4, to_up)
    got(rel_o.at[I1], rel_ml.at[I1], I1)
    fold(cur_o.at[I2, I1], cur_ml.at[I2, I1], rel_o.at[I1], rel_ml.at[I1], cur_o.at[I4, I1], cur_ml.at[I4, I1])
    send(I4, I1, fin_o.at[I1, I1], fin_ml.at[I1, I1], I5, to_dn)
    fold_pal(I3)
    if has_pages:
        y_forward()
    for side, t, k in ((I0, I1, I2), (I1, I0, I3), (I0, I0, I4), (I1, I1, I5)):
        got(fin_o.at[side, t], fin_ml.at[side, t], k)
    for t in range(I2):
        parts = [(cur_o.at[I3, t], cur_ml.at[I3, t]), (fin_o.at[I0, t], fin_ml.at[I0, t]), (fin_o.at[I1, t], fin_ml.at[I1, t])]
        ms = [stats(ml)[I0] for _, ml in parts] + [self_m[t]]
        ls = [stats(ml)[I1] for _, ml in parts] + [self_l[t]]
        top = functools.reduce(jnp.maximum, ms)
        ws = [jnp.exp(m - top) for m in ms]
        total = functools.reduce(jnp.add, [w * l for w, l in zip(ws, ls)])
        ws = [w / total for w in ws]
        own = ws.pop()
        ws += [own if e is None else own * e for _, e in self_w[t]]
        w = jnp.concatenate(ws, axis=I0)
        for c in range(n_chunk):
            wx = widen(w, c)
            sl = slice(c * cw, (c + I1) * cw)
            v_c = _dot(kv_ref[:, kv_w + c * kw:kv_w + (c + I1) * kw], expand[...], NN)
            acc = jnp.zeros((home, cw), F32)
            for i, (o, _) in enumerate(parts):
                acc = acc + o[:, sl] * wx[i * home:(i + I1) * home]
            for i, (step, _) in enumerate(self_w[t]):
                acc = acc + v_c[step * home:(step + I1) * home] * wx[(I3 + i) * home:(I4 + i) * home]
            out_ref[t * home:(t + I1) * home, sl] = acc.astype(BF16)
    if has_pages:
        y_finish()
    for c in pals + sends:
        c.wait_send()


def _place_kernel(steps, heads, kn_ref, vn_ref, k_ref, v_ref, mk_ref, mv_ref, wsel_ref, mig_ref, info_ref, ko_ref, vo_ref, kv_s, full):
    page, _, dim, n_slots = k_ref.shape[1:]
    n_seq = wsel_ref.shape[0]
    width = page * dim
    n_all = mig_ref.shape[0]
    moved = info_ref[0:1, :]
    w_off = info_ref[1:2, :]
    for t in range(steps):
        for which, ref in enumerate((kn_ref, vn_ref)):
            kv_s[which, t] = _dot(ref[:, 0, t].reshape(n_seq, heads * dim), wsel_ref[...], TN).astype(BF16)
    for h in range(heads):
        for which, (pool, pages, out) in enumerate(((k_ref, mk_ref, ko_ref), (v_ref, mv_ref, vo_ref))):
            full[...] = _dot(pages[:, 0, 0, :, h * width:(h + 1) * width].reshape(n_all, width), mig_ref[...], TN).astype(BF16).reshape(page, dim, n_slots)

            def fill(tok, _, which=which, pool=pool, out=out, h=h):
                at = w_off - tok.astype(F32)
                new = [jnp.where(at == -float(t), 1.0, 0.0) for t in range(steps)]
                kept = 1.0 - functools.reduce(jnp.add, new)
                val = full[tok] * kept.astype(BF16) + pool[0, tok, h] * (kept * (1.0 - moved)).astype(BF16)
                for t in range(steps):
                    val = val + kv_s[which, t, h * dim:(h + 1) * dim, :] * new[t].astype(BF16)
                out[0, tok, h] = val
                return 0

            lax.fori_loop(0, page, fill, 0, unroll=2)


def solution(mesh):
    n_rows, n_cols = mesh.shape['kv2'], mesh.shape['kv']
    dev_axes = ('rep', 'kv2', 'kv')
    group_axes = ('kv2', 'kv')
    seq_spec = P(None, dev_axes, None)
    pool_spec = P(dev_axes, None, None, None, None)
    table_spec = P(dev_axes, None)
    vec_spec = P(dev_axes)
    full_spec = P()
    pair = 2
    vmem = pl.BlockSpec(memory_space=pltpu.VMEM)
    dma = pltpu.SemaphoreType.DMA

    def per_device(x_embed, w_query, w_key, w_value, w_out, w_up, w_down, k_pool, v_pool, old_table, seq_len, src_slot, dst_slot):
        n_slots, layers, page, kv_heads, dim = k_pool.shape
        steps, seq_dev, width = x_embed.shape
        heads = w_query.shape[2] // dim
        group = heads // kv_heads
        n_pages = old_table.shape[1]
        n_seq = seq_dev * n_cols
        n_move = src_slot.shape[0]
        n_rt = steps * group
        n_grid = kv_heads // pair
        page_w = page * dim
        n_x = n_cols // 2
        n_dev = n_rows * n_cols
        rows = steps * seq_dev
        me = lax.axis_index('kv2') * n_cols + lax.axis_index('kv')
        slot_base = me * n_slots
        k_t, v_t = (pltpu.with_memory_space_constraint(jnp.transpose(a, (1, 2, 3, 4, 0)), pltpu.HBM) for a in (k_pool, v_pool))
        q_w, kv_w, m_w = pair * group * dim, pair * dim, pair * page_w

        def fixed(shape):
            return pl.BlockSpec(shape, lambda i: (0,) * len(shape), pipeline_mode=pl.Buffered(1))

        src_hot = ((src_slot - slot_base)[:, None] == jnp.arange(n_slots, dtype=I32)[None, :]).astype(BF16)
        page_shape = (2, n_move, kv_heads * page_w)

        def pool_blk(layer):
            return pl.BlockSpec((1, page, pair, dim, n_slots), lambda i: (layer, 0, i, 0, 0))

        both = pl.BlockSpec((1, page, pair, dim, n_slots), lambda l, i: (l, 0, i, 0, 0))
        packed = pl.pallas_call(
            functools.partial(_pack_kernel, pair),
            grid=(layers, n_grid),
            in_specs=[pl.BlockSpec((n_move, n_slots), lambda l, i: (0, 0)), both, both],
            out_specs=pl.BlockSpec((1, 2, n_move, m_w), lambda l, i: (l, 0, 0, i)),
            out_shape=jax.ShapeDtypeStruct((layers,) + page_shape, BF16),
            cost_estimate=_cost(8, 16),
            name='pack_pages',
        )(src_hot, k_t, v_t)
        moved = lax.all_gather(packed, group_axes)

        def project(hidden, layer):
            q = jnp.dot(hidden, w_query[layer], preferred_element_type=F32).astype(BF16)
            kv = jnp.concatenate([jnp.dot(hidden, w[layer], preferred_element_type=F32).astype(BF16) for w in (w_key, w_value)], axis=1)
            return q, kv

        hidden = x_embed.reshape(rows, width)
        q, kv = project(hidden, 0)
        y, at = lax.axis_index('kv2'), lax.axis_index('kv')
        n_all = n_dev * n_move
        n_arr = n_rows * n_move

        def own_place(v):
            wide = jnp.tile(v, n_cols)[None, :]
            lane = jnp.arange(n_cols * n_move, dtype=I32)[None, :] // n_move
            return jnp.where((lane == at) & (jnp.arange(8, dtype=I32)[:, None] == y), wide, 0)

        tab = jnp.concatenate([old_table.T.reshape(-1), seq_len])[None, :]
        meta = jnp.concatenate([jnp.where(jnp.arange(8, dtype=I32)[:, None] == 0, tab, 0), own_place(src_slot), own_place(dst_slot)], axis=0)
        pages_all_shape = jax.ShapeDtypeStruct((n_rows,) + page_shape, BF16)
        q_all_shape = jax.ShapeDtypeStruct((n_cols, rows, heads * dim), BF16)
        dims = (n_rows, n_cols, n_slots, n_pages, page, seq_dev)
        pages_y, q_all, q_sel, cells, arr, info, w_sel, mig, w_info = pl.pallas_call(
            functools.partial(_head_kernel, dims),
            in_specs=[vmem] * 5,
            out_specs=[vmem] * 9,
            out_shape=[
                pages_all_shape,
                q_all_shape,
                jax.ShapeDtypeStruct((n_seq, LANES), BF16),
                jax.ShapeDtypeStruct((n_pages * n_seq, LANES), BF16),
                jax.ShapeDtypeStruct((n_arr, LANES), BF16),
                jax.ShapeDtypeStruct((8, LANES), F32),
                jax.ShapeDtypeStruct((n_seq, n_slots), BF16),
                jax.ShapeDtypeStruct((n_all, n_slots), BF16),
                jax.ShapeDtypeStruct((8, n_slots), F32),
            ],
            scratch_shapes=[pltpu.VMEM((n_dev,) + meta.shape, I32), dma((2, n_dev - 1)), dma((2, 6)), dma((2, 13))],
            compiler_params=pltpu.CompilerParams(collective_id=0, has_side_effects=True, vmem_limit_bytes=24 * MIB),
            cost_estimate=_cost(10, 4),
            name='head_gather',
        )(meta, packed, q, src_slot.reshape(1, -1), src_slot.reshape(-1, 1))

        def attend(layer, q_all, pages):
            blk = pool_blk(layer)
            ml_rows = 2 * LANES // 4
            return pl.pallas_call(
                functools.partial(_attn_kernel, steps, group, pair),
                grid=(n_grid,),
                in_specs=[
                    pl.BlockSpec((n_cols, steps, seq_dev, q_w), lambda i: (0, 0, 0, i)),
                    blk, blk,
                    pl.BlockSpec((n_rows, 1, n_move, m_w), lambda i: (0, 0, 0, i)),
                    pl.BlockSpec((n_rows, 1, n_move, m_w), lambda i: (0, 1, 0, i)),
                    fixed(q_sel.shape), fixed(cells.shape), fixed(arr.shape), fixed(info.shape),
                ],
                out_specs=[
                    pl.BlockSpec((2, n_x, steps, seq_dev, q_w), lambda i: (0, 0, 0, 0, i)),
                    pl.BlockSpec((2, n_x, steps, seq_dev, ml_rows), lambda i: (0, 0, 0, 0, 0)),
                ],
                out_shape=[
                    jax.ShapeDtypeStruct((2, n_x, steps, seq_dev, heads * dim), F32),
                    jax.ShapeDtypeStruct((2, n_x, steps, seq_dev, ml_rows), F32),
                ],
                scratch_shapes=[
                    pltpu.VMEM((steps, q_w, LANES), F32),
                    pltpu.VMEM((page, dim, LANES), F32),
                    pltpu.VMEM((page, dim, LANES), F32),
                    pltpu.VMEM((n_rt, page, LANES), F32),
                    pltpu.VMEM((n_rt * dim, LANES), F32),
                    pltpu.VMEM((2 * n_rt, LANES), F32),
                    pltpu.VMEM((steps, ml_rows, n_seq), F32),
                ],
                compiler_params=pltpu.CompilerParams(vmem_limit_bytes=32 * MIB),
                cost_estimate=_cost(20, 16),
                name='slot_attention',
            )(q_all.reshape(n_cols, steps, seq_dev, heads * dim), k_t, v_t, pages, pages, q_sel, cells, arr, info)

        def exchange(layer, o, ml, q, kv, pages):
            has = pages is not None
            half = (seq_dev, heads * dim)
            stat = (seq_dev, ml.shape[-1])
            out_shape = [jax.ShapeDtypeStruct((rows, heads * dim), BF16)] + ([pages_all_shape] if has else [])
            return pl.pallas_call(
                functools.partial(_exchange_kernel, n_cols, n_rows, heads, dim, has),
                in_specs=[vmem] * (5 if has else 4),
                out_specs=[vmem] * len(out_shape),
                out_shape=out_shape,
                scratch_shapes=[
                    pltpu.VMEM((4, steps) + half, F32), pltpu.VMEM((4, steps) + stat, F32),
                    pltpu.VMEM((5, steps) + half, F32), pltpu.VMEM((5, steps) + stat, F32),
                    pltpu.VMEM((2,) + half, F32), pltpu.VMEM((2,) + stat, F32),
                    pltpu.VMEM((2, steps) + half, F32), pltpu.VMEM((2, steps) + stat, F32),
                    pltpu.VMEM((heads, heads * dim), BF16), pltpu.VMEM((kv_w, q_w), BF16),
                    dma((2, 8)), dma((2, 12)), dma((2, 6)),
                ],
                compiler_params=pltpu.CompilerParams(collective_id=1 + layer, has_side_effects=True, vmem_limit_bytes=32 * MIB),
                cost_estimate=_cost(10, 4),
                name='exchange_partials',
            )(o, ml, q, kv, *([pages] if has else []))

        kv_all = []
        for layer in range(layers):
            if layer:
                q, kv = project(hidden, layer)
                [q_all] = pl.pallas_call(
                    functools.partial(_query_kernel, n_cols),
                    in_specs=[vmem],
                    out_specs=[vmem],
                    out_shape=[q_all_shape],
                    scratch_shapes=[dma((2, 13))],
                    compiler_params=pltpu.CompilerParams(collective_id=1 + layers + layer, has_side_effects=True, vmem_limit_bytes=16 * MIB),
                    cost_estimate=_cost(5, 4),
                    name='query_gather',
                )(q)
            kv_all.append(kv)
            o, ml = attend(layer, q_all, pages_y)
            nxt = packed if layer + 1 < layers else None
            attn, *more = exchange(layer, o, ml, q, kv, nxt)
            pages_y = more[0] if more else None
            hidden = (hidden.astype(F32) + jnp.dot(attn, w_out[layer], preferred_element_type=F32)).astype(BF16)
            up_act = jax.nn.gelu(jnp.dot(hidden, w_up[layer], preferred_element_type=F32)).astype(BF16)
            hidden = (hidden.astype(F32) + jnp.dot(up_act, w_down[layer], preferred_element_type=F32)).astype(BF16)
        kv_rows = lax.all_gather(jnp.stack(kv_all), 'kv').reshape(n_cols, layers, steps, seq_dev, -1)
        v_at = kv_heads * dim // kv_w

        def held(arr):
            return pl.BlockSpec(arr.shape, lambda l, i: (0,) * arr.ndim, pipeline_mode=pl.Buffered(1))

        k_out, v_out = pl.pallas_call(
            functools.partial(_place_kernel, steps, pair),
            grid=(layers, n_grid),
            in_specs=[
                pl.BlockSpec((n_cols, 1, steps, seq_dev, kv_w), lambda l, i: (0, l, 0, 0, i)),
                pl.BlockSpec((n_cols, 1, steps, seq_dev, kv_w), lambda l, i: (0, l, 0, 0, v_at + i)),
                both, both,
                pl.BlockSpec((n_dev, 1, 1, n_move, m_w), lambda l, i: (0, l, 0, 0, i)),
                pl.BlockSpec((n_dev, 1, 1, n_move, m_w), lambda l, i: (0, l, 1, 0, i)),
                held(w_sel), held(mig), held(w_info),
            ],
            out_specs=[both, both],
            out_shape=[jax.ShapeDtypeStruct(k_t.shape, BF16), jax.ShapeDtypeStruct(v_t.shape, BF16)],
            scratch_shapes=[pltpu.VMEM((2, steps, kv_w, n_slots), BF16), pltpu.VMEM((page, dim, n_slots), BF16)],
            compiler_params=pltpu.CompilerParams(vmem_limit_bytes=32 * MIB),
            cost_estimate=_cost(40, 64),
            name='place_pages',
        )(kv_rows, kv_rows, k_t, v_t, moved, moved, w_sel, mig, w_info)
        y_out = hidden.reshape(steps, seq_dev, width)
        back = (4, 0, 1, 2, 3)
        return y_out, jnp.transpose(k_out, back), jnp.transpose(v_out, back)

    return jax.shard_map(per_device, mesh=mesh, in_specs=(seq_spec, full_spec, full_spec, full_spec, full_spec, full_spec, full_spec, pool_spec, pool_spec, table_spec, vec_spec, vec_spec, vec_spec), out_specs=(seq_spec, pool_spec, pool_spec), check_vma=False)
```

```python
import functools

import jax
import jax.numpy as jnp
from jax import lax
from jax.experimental import pallas as pl
from jax.experimental.pallas import tpu as pltpu
from jax.sharding import PartitionSpec as P


F32 = jnp.float32
BF16 = jnp.bfloat16
I32 = jnp.int32
NEG = -1e30
NN = (((1,), (0,)), ((), ()))
NT = (((1,), (1,)), ((), ()))
TN = (((0,), (0,)), ((), ()))
MESH = pl.DeviceIdType.MESH
LANES = 256
MIB = 2**20
I0, I1, I2, I3, I4, I5 = range(6)


def _cost(gflops, mib):
    return pl.CostEstimate(flops=gflops * 10**9, bytes_accessed=mib * MIB, transcendentals=0)


def _dot(a, b, dims):
    return lax.dot_general(a, b, dims, preferred_element_type=F32)


def _split(x):
    hi = x.astype(BF16)
    rest = x - hi.astype(F32)
    mid = rest.astype(BF16)
    low = (rest - mid.astype(F32)).astype(BF16)
    return hi, mid, low


def _pick_lhs(x, sel, dims):
    hi, mid, low = _split(x)
    return _dot(hi, sel, dims) + _dot(mid, sel, dims) + _dot(low, sel, dims)


def _pick_rhs(sel, x, dims):
    hi, mid, low = _split(x)
    return _dot(sel, hi, dims) + _dot(sel, mid, dims) + _dot(sel, low, dims)


def _columns(rows):
    full = jnp.concatenate([rows, jnp.zeros((LANES // 2 - rows.shape[0], rows.shape[1]), F32)], axis=0).T
    ids = lax.broadcasted_iota(I32, full.shape, 1)

    def column(i):
        return jnp.sum(jnp.where(ids == i, full, 0.0), axis=1, keepdims=True).astype(I32)

    return column


def _tables(dims, meta_all, mysrc_ref, mysrcc_ref, qsel_ref, cell_ref, arr_ref, info_ref, wsel_ref, mig_ref, winfo_ref):
    n_rows, n_cols, n_slots, n_pages, page, seq_dev = dims
    y, my_col = lax.axis_index('kv2'), lax.axis_index('kv')
    base = (y * n_cols + my_col) * n_slots
    n_seq = n_cols * seq_dev
    n_move = mysrc_ref.shape[1]
    n_arr = arr_ref.shape[0]
    spare = LANES - n_slots
    src = jnp.sum(meta_all[:, 8:16, :], axis=0)
    dst = jnp.sum(meta_all[:, 16:24, :], axis=0)
    tab = jnp.concatenate([meta_all[y * n_cols + i, 0:1, :] for i in range(n_cols)], axis=0).astype(F32)
    column = _columns(tab)
    tabs = [column(i) for i in range(n_cols)]
    old = jnp.concatenate([c[j * seq_dev:(j + 1) * seq_dev] for j in range(n_pages) for c in tabs], axis=0)
    lens = jnp.concatenate([c[n_pages * seq_dev:] for c in tabs], axis=0)
    per_row = n_cols * n_move
    ids = lax.broadcasted_iota(I32, (1, per_row), 1)
    entry = jnp.zeros(old.shape, F32)
    to = jnp.zeros(old.shape, F32)
    for r in range(n_rows):
        hit = old == src[r:r + 1]
        entry = entry + jnp.sum(jnp.where(hit, ids + (r * per_row + 1), 0).astype(F32), axis=1, keepdims=True)
        to = to + jnp.sum(jnp.where(hit, dst[r:r + 1] + 1, 0).astype(F32), axis=1, keepdims=True)
    entry = entry.astype(I32) - 1
    to = to.astype(I32) - 1
    is_moved = entry >= 0
    dev = entry // n_move
    nth = entry - dev * n_move
    arrival = (dev // n_cols) * n_move + nth
    free = jnp.sum(jnp.where(nth == lax.broadcasted_iota(I32, (1, n_move), 1), mysrc_ref[...] - base, 0).astype(F32), axis=1, keepdims=True).astype(I32)
    arr_lane = jnp.where(arrival < spare, n_slots + arrival, free)
    here = old - base
    here = jnp.where((here >= 0) & (here < n_slots), here, -1)
    lane = jnp.where(is_moved, jnp.where(dev % n_cols == my_col, arr_lane, -1), here)
    final = jnp.where(is_moved, to, old) - base
    lane_ids = lax.broadcasted_iota(I32, (1, LANES), 1)
    slot_ids = lax.broadcasted_iota(I32, (1, n_slots), 1)
    last = lens // page
    q_sel = jnp.zeros((n_seq, LANES), F32)
    w_sel = jnp.zeros((n_seq, n_slots), F32)
    first = jnp.zeros((1, LANES), F32)
    for j in range(n_pages):
        eq = (lane[j * n_seq:(j + 1) * n_seq] == lane_ids).astype(F32)
        cell_ref[j * n_seq:(j + 1) * n_seq, :] = eq.astype(BF16)
        q_sel = q_sel + eq
        first = first + jnp.sum(eq, axis=0, keepdims=True) * float(j * page)
        w_sel = w_sel + jnp.where((final[j * n_seq:(j + 1) * n_seq] == slot_ids) & (last == j), 1.0, 0.0)
    qsel_ref[...] = q_sel.astype(BF16)
    wsel_ref[...] = w_sel.astype(BF16)
    used = jnp.sum(q_sel, axis=0, keepdims=True)
    slot_len = jnp.sum(q_sel * lens.astype(F32), axis=0, keepdims=True)
    arr_ids = lax.broadcasted_iota(I32, (n_arr, LANES), 0)
    arr_ref[...] = jnp.where(lane_ids == n_slots + arr_ids, 1.0, 0.0).astype(BF16)
    mine = mysrcc_ref[...] - base
    arr_ref[spare:n_arr, :] = jnp.where(lane_ids == mine, 1.0, 0.0).astype(BF16)
    out_lanes = jnp.sum(jnp.where(mine == lane_ids, 1.0, 0.0), axis=0, keepdims=True)
    info_ref[...] = jnp.zeros_like(info_ref)
    info_ref[0:1, :] = used
    info_ref[1:2, :] = jnp.where(used > 0, slot_len - first - 1.0, -100.0)
    info_ref[2:3, :] = jnp.where(lane_ids >= n_slots, 1.0, out_lanes)
    written = jnp.sum(w_sel, axis=0, keepdims=True)
    w_off = jnp.sum(w_sel * (lens - last * page).astype(F32), axis=0, keepdims=True)
    to_col = _columns(dst.astype(F32))
    dst_col = jnp.concatenate([to_col(r) for r in range(n_rows)], axis=0)
    mig = jnp.where(dst_col - base == slot_ids, 1.0, 0.0)
    mig_ref[...] = mig.astype(BF16)
    winfo_ref[...] = jnp.zeros_like(winfo_ref)
    winfo_ref[0:1, :] = jnp.sum(mig, axis=0, keepdims=True)
    winfo_ref[1:2, :] = jnp.where(written > 0, w_off, -100.0)


def _pack_kernel(heads, onehot_ref, *refs):
    half = len(refs) // 2
    for src, out in zip(refs[:half], refs[half:]):
        page, _, dim, n_slots = src.shape[1:]
        width = page * dim
        for h in range(heads):
            rows = src[0, :, h].reshape(width, n_slots)
            out[:, h * width:(h + 1) * width] = _dot(onehot_ref[...], rows, NT).astype(BF16)


def _copy(src, dst, sems, k, dev):
    return pltpu.make_async_remote_copy(src_ref=src, dst_ref=dst, send_sem=sems.at[0, k], recv_sem=sems.at[1, k], device_id=dev, device_id_type=MESH)


def _rows_on_y(own, out, sems, halves):
    n = out.shape[I0]
    y = lax.axis_index('kv2')
    up, dn, far = (y + I1) % n, (y + n - I1) % n, (y + I2) % n
    to_up, to_dn = {'kv2': up}, {'kv2': dn}
    first = [
        _copy(halves(own, I0), halves(out.at[y], I0), sems, I0, to_up),
        _copy(halves(own, I1), halves(out.at[y], I1), sems, I1, to_up),
        _copy(halves(own, I1), halves(out.at[y], I1), sems, I2, to_dn),
        _copy(halves(own, I0), halves(out.at[y], I0), sems, I3, to_dn),
    ]
    relay = [
        _copy(halves(out.at[dn], I0), halves(out.at[dn], I0), sems, I4, to_up),
        _copy(halves(out.at[up], I1), halves(out.at[up], I1), sems, I5, to_dn),
    ]
    lands = [(dn, I0), (dn, I1), (up, I1), (up, I0), (far, I0), (far, I1)]

    def got(k):
        at, h = lands[k]
        _copy(halves(out.at[at], h), halves(out.at[at], h), sems, k, to_up).wait_recv()

    def start():
        for k in (I0, I2, I1, I3):
            first[k].start()

    def forward():
        got(I0)
        relay[I0].start()
        got(I2)
        relay[I1].start()

    def finish():
        for k in (I1, I3, I4, I5):
            got(k)
        for c in first + relay:
            c.wait_send()

    return start, forward, finish


def _signal_all(devs):
    barrier = pltpu.get_barrier_semaphore()
    for dev in devs:
        pl.semaphore_signal(barrier, inc=1, device_id=dev, device_id_type=MESH)
    pl.semaphore_wait(barrier, len(devs))


def _q_gather(n_cols, q_ref, q_all, x_sem):
    n_x = n_cols // I2
    at = lax.axis_index('kv')
    x, core = at // I2, at % I2
    up, dn, far = (x + I1) % n_x, (x + n_x - I1) % n_x, (x + I2) % n_x
    to_up, to_dn, to_pal = {'kv': up * I2 + core}, {'kv': dn * I2 + core}, {'kv': x * I2 + I1 - core}
    n_half = q_ref.shape[I0] // I2

    def half(ref, h):
        return ref.at[pl.ds(h * n_half, n_half)]

    def slot(pos, c):
        return q_all.at[pos * I2 + c]

    first = [
        _copy(half(q_ref, I0), half(slot(x, core), I0), x_sem, I0, to_up),
        _copy(half(q_ref, I1), half(slot(x, core), I1), x_sem, I1, to_up),
        _copy(half(q_ref, I1), half(slot(x, core), I1), x_sem, I2, to_dn),
        _copy(half(q_ref, I0), half(slot(x, core), I0), x_sem, I3, to_dn),
    ]
    relay = [
        _copy(half(slot(dn, core), I0), half(slot(dn, core), I0), x_sem, I4, to_up),
        _copy(half(slot(up, core), I1), half(slot(up, core), I1), x_sem, I5, to_dn),
    ]
    lands = [(dn, I0), (dn, I1), (up, I1), (up, I0), (far, I0), (far, I1)]
    pal = [_copy(half(slot(p, core), h), half(slot(p, core), h), x_sem, 6 + k, to_pal) for k, (p, h) in enumerate(lands)]
    own = _copy(q_ref, slot(x, core), x_sem, 12, to_pal)

    def got(k):
        p, h = lands[k]
        _copy(half(slot(p, core), h), half(slot(p, core), h), x_sem, k, to_up).wait_recv()

    for k in (I0, I2, I1, I3):
        first[k].start()
    own.start()
    q_all[at] = q_ref[...]
    yield
    got(I0)
    relay[I0].start()
    pal[I0].start()
    got(I2)
    relay[I1].start()
    pal[I2].start()
    yield
    for k in (I1, I3, I4, I5):
        got(k)
        pal[k].start()
    yield
    _copy(q_ref, slot(x, I1 - core), x_sem, 12, to_pal).wait_recv()
    for k, (p, h) in enumerate(lands):
        _copy(half(slot(p, I1 - core), h), half(slot(p, I1 - core), h), x_sem, 6 + k, to_pal).wait_recv()
    for c in first + relay + pal + [own]:
        c.wait_send()


def _x_peers(n_cols):
    n_x = n_cols // I2
    at = lax.axis_index('kv')
    x, core = at // I2, at % I2
    return [{'kv': ((x + I1) % n_x) * I2 + core}, {'kv': ((x + n_x - I1) % n_x) * I2 + core}, {'kv': x * I2 + I1 - core}]


def _y_peers(n_rows):
    y = lax.axis_index('kv2')
    return [{'kv2': (y + I1) % n_rows}, {'kv2': (y + n_rows - I1) % n_rows}]


def _half0(ref, h):
    return ref[h] if isinstance(ref, tuple) else ref.at[h]


def _head_kernel(dims, meta_ref, kp_ref, vp_ref, q_ref, mysrc_ref, mysrcc_ref, pages_all, q_all, *refs):
    tables, (meta_all, m_sem, y_sem, x_sem) = refs[:7], refs[7:]
    n_rows, n_cols = dims[:2]
    pages_ref = (kp_ref, vp_ref)
    y, at = lax.axis_index('kv2'), lax.axis_index('kv')
    offsets = [(a, b) for a in range(n_rows) for b in range(n_cols) if (a, b) != (0, 0)]
    peers = [{'kv2': (y + a) % n_rows, 'kv': (at + b) % n_cols} for a, b in offsets]
    _signal_all(peers)
    me = y * n_cols + at
    metas = [_copy(meta_ref, meta_all.at[me], m_sem, k, peers[k]) for k in range(len(peers))]
    for c in metas:
        c.start()
    start, forward, finish = _rows_on_y(pages_ref, pages_all, y_sem, _half0)
    start()
    steps = _q_gather(n_cols, q_ref, q_all, x_sem)
    next(steps)
    meta_all[me] = meta_ref[...]
    for h, ref in enumerate(pages_ref):
        pages_all[y, h] = ref[...]
    next(steps)
    forward()
    for k, (a, b) in enumerate(offsets):
        frm = ((y + n_rows - a) % n_rows) * n_cols + (at + n_cols - b) % n_cols
        _copy(meta_ref, meta_all.at[frm], m_sem, k, peers[k]).wait_recv()
    _tables(dims, meta_all, mysrc_ref, mysrcc_ref, *tables)
    next(steps)
    finish()
    for _ in steps:
        pass
    for c in metas:
        c.wait_send()


def _query_kernel(n_cols, q_ref, q_all, x_sem):
    _signal_all(_x_peers(n_cols))
    for _ in _q_gather(n_cols, q_ref, q_all, x_sem):
        pass


def _attn_kernel(steps, group, heads, q_ref, k_ref, v_ref, mk_ref, mv_ref, qsel_ref, cell_ref, arr_ref, info_ref, o_ref, ml_ref, q_s, mk_s, mv_s, s_s, os_s, ml_s, ml_all):
    page, _, dim, n_slots = k_ref.shape[1:]
    n_seq = qsel_ref.shape[0]
    n_core, n_x, _, home = o_ref.shape[:4]
    n_arr = arr_ref.shape[0]
    pid = pl.program_id(0)
    n_rt = steps * group
    width = page * dim
    used = info_ref[0:1, :]
    limit = info_ref[1:2, :]
    freed = info_ref[2:3, 0:n_slots] > 0
    cells = cell_ref[...]
    owned = _dot(jnp.ones((8, LANES), BF16), cells, NT)[0:1] > 0
    scale = dim ** -0.5
    q_sel = qsel_ref[...]

    @pl.when(pid == 0)
    def _():
        ml_all[...] = jnp.zeros_like(ml_all)

    for t in range(steps):
        q_s[t] = _dot(q_ref[:, t].reshape(n_seq, heads * group * dim), q_sel, TN)
    tops, sums = [[] for _ in range(steps)], [[] for _ in range(steps)]
    for h in range(heads):
        for pages, full in ((mk_ref, mk_s), (mv_ref, mv_s)):
            full[...] = _dot(pages[:, 0, :, h * width:(h + 1) * width].reshape(n_arr, width), arr_ref[...], TN).reshape(page, dim, LANES)

        def join(tok, _, h=h):
            for pool, full in ((k_ref, mk_s), (v_ref, mv_s)):
                full[tok, :, 0:n_slots] = jnp.where(freed, full[tok, :, 0:n_slots], pool[0, tok, h].astype(F32))
            return 0

        lax.fori_loop(0, page, join, 0)

        def score(pair, _, h=h):
            toks = [pair * 2, pair * 2 + 1]
            keys = [mk_s[tok] for tok in toks]
            for t in range(steps):
                for r in range(group):
                    q_row = q_s[t, (h * group + r) * dim:(h * group + r + 1) * dim, :]
                    for tok, key in zip(toks, keys):
                        s_s[t * group + r, pl.ds(tok, 1), :] = jnp.sum(key * q_row, axis=0, keepdims=True)
            return 0

        lax.fori_loop(0, page // 2, score, 0)
        visible = lax.broadcasted_iota(I32, (page, LANES), 0).astype(F32) <= limit
        for rt in range(n_rt):
            sc = jnp.where(visible, s_s[rt] * scale, NEG)
            top = jnp.max(sc, axis=0, keepdims=True)
            ex = jnp.where(visible, jnp.exp(sc - top), 0.0)
            s_s[rt] = ex
            ml_s[rt:rt + 1, :] = top
            ml_s[n_rt + rt:n_rt + rt + 1, :] = jnp.sum(ex, axis=0, keepdims=True)
        live = (used > 0) & (limit >= 0)
        m_slot = ml_s[0:n_rt]
        l_slot = ml_s[n_rt:2 * n_rt]
        m_cell = jnp.where(owned, _pick_lhs(m_slot, cells, NT), NEG)
        m_seq = m_cell[:, 0:n_seq]
        for j in range(1, cells.shape[0] // n_seq):
            m_seq = jnp.maximum(m_seq, m_cell[:, j * n_seq:(j + 1) * n_seq])
        m_back = _pick_lhs(m_seq, q_sel, NN)
        w_slot = jnp.where(live, jnp.exp(jnp.minimum(m_slot - m_back, 0.0)), 0.0)
        l_seq = _pick_lhs(l_slot * w_slot, q_sel, NT)
        for t in range(steps):
            tops[t].append(m_seq[t * group:(t + 1) * group])
            sums[t].append(l_seq[t * group:(t + 1) * group])
        for rt in range(n_rt):
            s_s[rt] = s_s[rt] * w_slot[rt:rt + 1]

        def weigh(c, _):
            row = pl.multiple_of(c * 8, 8)
            acc = [jnp.zeros((8, LANES), F32) for _ in range(n_rt)]
            for tok in range(page):
                vals = mv_s[tok, pl.ds(row, 8), :]
                for rt in range(n_rt):
                    acc[rt] = acc[rt] + s_s[rt, tok:tok + 1, :] * vals
            for rt in range(n_rt):
                os_s[pl.ds(rt * dim + row, 8), :] = acc[rt]
            return 0

        lax.fori_loop(0, dim // 8, weigh, 0)
        for t in range(steps):
            part = _pick_rhs(q_sel, os_s[t * group * dim:(t + 1) * group * dim, :], NT).reshape(n_x, n_core, home, group * dim)
            for c in range(n_core):
                o_ref[c, :, t, :, h * group * dim:(h + 1) * group * dim] = part[:, c]

    n_row = heads * group
    for t in range(steps):
        ml_all[t, pl.ds(pl.multiple_of(pid * n_row, n_row), n_row), :] = jnp.concatenate(tops[t], axis=0)
        ml_all[t, pl.ds(pl.multiple_of((pl.num_programs(0) + pid) * n_row, n_row), n_row), :] = jnp.concatenate(sums[t], axis=0)

    @pl.when(pid == pl.num_programs(0) - 1)
    def _():
        for t in range(steps):
            flat = ml_all[t].T.reshape(n_x, n_core, home, ml_all.shape[1])
            for c in range(n_core):
                ml_ref[c, :, t] = flat[:, c]


def _exchange_kernel(n_cols, n_rows, heads, dim, has_pages, *refs):
    o_ref, ml_ref, q_ref, kv_ref = refs[:I4]
    n_in = 6 if has_pages else I4
    n_out = I2 if has_pages else I1
    out_ref = refs[n_in]
    rp_o, rp_ml, cur_o, cur_ml, rel_o, rel_ml, fin_o, fin_ml, spread, expand, p_sem, r_sem, y_sem = refs[n_in + n_out:]
    n_x = n_cols // I2
    home = q_ref.shape[I0] // I2
    width = heads * dim
    at = lax.axis_index('kv')
    x, core = at // I2, at % I2
    up, dn, far = (x + I1) % n_x, (x + n_x - I1) % n_x, (x + I2) % n_x
    to_up, to_dn, to_pal = {'kv': up * I2 + core}, {'kv': dn * I2 + core}, {'kv': x * I2 + I1 - core}
    _signal_all(_x_peers(n_cols) + (_y_peers(n_rows) if has_pages else []))
    order = [far, up, dn, x]
    pals = []
    for i, pos in enumerate(order):
        pals.append(_copy(o_ref.at[I1 - core, pos], rp_o.at[i], p_sem, i, to_pal))
        pals.append(_copy(ml_ref.at[I1 - core, pos], rp_ml.at[i], p_sem, I4 + i, to_pal))
    for c in pals:
        c.start()
    if has_pages:
        pages_ref, pages_all = refs[I4:n_in], refs[n_in + I1]
        y_start, y_forward, y_finish = _rows_on_y(pages_ref, pages_all, y_sem, _half0)
        y_start()
        for h, ref in enumerate(pages_ref):
            pages_all[lax.axis_index('kv2'), h] = ref[...]

    n_chunk = I4
    cw = width // n_chunk
    kv_w = kv_ref.shape[I1] // I2
    kw = kv_w // n_chunk
    spread[...] = (lax.broadcasted_iota(I32, spread.shape, I1) // dim == lax.broadcasted_iota(I32, spread.shape, I0)).astype(F32).astype(BF16)
    lane = lax.broadcasted_iota(I32, expand.shape, I1)
    row = lax.broadcasted_iota(I32, expand.shape, I0)
    group = cw // kw
    expand[...] = ((lane // (dim * group) == row // dim) & (lane % dim == row % dim)).astype(F32).astype(BF16)

    def widen(w, c):
        return _pick_lhs(w, spread[:, c * cw:(c + I1) * cw], NN)

    s = jnp.zeros((I3 * home, heads), F32)
    for c in range(n_chunk):
        q_c = q_ref[:, c * cw:(c + I1) * cw].astype(F32)
        k_c = _dot(kv_ref[:, c * kw:(c + I1) * kw], expand[...], NN)
        prod = jnp.concatenate([q_c[I0:home] * k_c[I0:home], q_c[home:] * k_c[I0:home], q_c[home:] * k_c[home:]], axis=I0)
        s = s + _pick_lhs(prod, spread[:, c * cw:(c + I1) * cw], NT)
    s = s * dim ** -0.5
    s00, s10, s11 = s[I0:home], s[home:I2 * home], s[I2 * home:]
    m1 = jnp.maximum(s10, s11)
    e10, e11 = jnp.exp(s10 - m1), jnp.exp(s11 - m1)
    self_m = [s00, m1]
    self_l = [jnp.ones_like(s00), e10 + e11]
    self_w = [[(I0, None)], [(I0, e10), (I1, e11)]]

    def stats(ref):
        return ref[:, I0:heads], ref[:, heads:I2 * heads]

    def fold(a_o, a_ml, b_o, b_ml, out_o, out_ml):
        am, al = stats(a_ml)
        bm, bl = stats(b_ml)
        top = jnp.maximum(am, bm)
        aw, bw = jnp.exp(am - top), jnp.exp(bm - top)
        out_ml[:, I0:heads] = top
        out_ml[:, heads:I2 * heads] = aw * al + bw * bl
        w = jnp.concatenate([aw, bw], axis=I0)
        for c in range(n_chunk):
            wx = widen(w, c)
            sl = slice(c * cw, (c + I1) * cw)
            out_o[:, sl] = a_o[:, sl] * wx[I0:home] + b_o[:, sl] * wx[home:]

    cur_ml[...] = jnp.zeros_like(cur_ml)

    def fold_pal(i):
        _copy(o_ref.at[I1 - core, order[i]], rp_o.at[i], p_sem, i, to_pal).wait_recv()
        _copy(ml_ref.at[I1 - core, order[i]], rp_ml.at[i], p_sem, I4 + i, to_pal).wait_recv()
        for t in range(I2):
            fold(o_ref.at[core, order[i], t], ml_ref.at[core, order[i], t], rp_o.at[i, t], rp_ml.at[i, t], cur_o.at[i, t], cur_ml.at[i, t])

    sends = []

    def send(i, t, dst_o, dst_ml, k, dev):
        a = _copy(cur_o.at[i, t], dst_o, r_sem, I2 * k, dev)
        b = _copy(cur_ml.at[i, t], dst_ml, r_sem, I2 * k + I1, dev)
        a.start()
        b.start()
        sends.extend([a, b])

    def got(dst_o, dst_ml, k):
        _copy(dst_o, dst_o, r_sem, I2 * k, to_up).wait_recv()
        _copy(dst_ml, dst_ml, r_sem, I2 * k + I1, to_up).wait_recv()

    fold_pal(I0)
    send(I0, I0, rel_o.at[I0], rel_ml.at[I0], I0, to_up)
    send(I0, I1, rel_o.at[I1], rel_ml.at[I1], I1, to_dn)
    fold_pal(I1)
    send(I1, I1, fin_o.at[I0, I1], fin_ml.at[I0, I1], I2, to_up)
    fold_pal(I2)
    send(I2, I0, fin_o.at[I1, I0], fin_ml.at[I1, I0], I3, to_dn)
    got(rel_o.at[I0], rel_ml.at[I0], I0)
    fold(cur_o.at[I1, I0], cur_ml.at[I1, I0], rel_o.at[I0], rel_ml.at[I0], cur_o.at[I4, I0], cur_ml.at[I4, I0])
    send(I4, I0, fin_o.at[I0, I0], fin_ml.at[I0, I0], I4, to_up)
    got(rel_o.at[I1], rel_ml.at[I1], I1)
    fold(cur_o.at[I2, I1], cur_ml.at[I2, I1], rel_o.at[I1], rel_ml.at[I1], cur_o.at[I4, I1], cur_ml.at[I4, I1])
    send(I4, I1, fin_o.at[I1, I1], fin_ml.at[I1, I1], I5, to_dn)
    fold_pal(I3)
    if has_pages:
        y_forward()
    for side, t, k in ((I0, I1, I2), (I1, I0, I3), (I0, I0, I4), (I1, I1, I5)):
        got(fin_o.at[side, t], fin_ml.at[side, t], k)
    for t in range(I2):
        parts = [(cur_o.at[I3, t], cur_ml.at[I3, t]), (fin_o.at[I0, t], fin_ml.at[I0, t]), (fin_o.at[I1, t], fin_ml.at[I1, t])]
        ms = [stats(ml)[I0] for _, ml in parts] + [self_m[t]]
        ls = [stats(ml)[I1] for _, ml in parts] + [self_l[t]]
        top = functools.reduce(jnp.maximum, ms)
        ws = [jnp.exp(m - top) for m in ms]
        total = functools.reduce(jnp.add, [w * l for w, l in zip(ws, ls)])
        ws = [w / total for w in ws]
        own = ws.pop()
        ws += [own if e is None else own * e for _, e in self_w[t]]
        w = jnp.concatenate(ws, axis=I0)
        for c in range(n_chunk):
            wx = widen(w, c)
            sl = slice(c * cw, (c + I1) * cw)
            v_c = _dot(kv_ref[:, kv_w + c * kw:kv_w + (c + I1) * kw], expand[...], NN)
            acc = jnp.zeros((home, cw), F32)
            for i, (o, _) in enumerate(parts):
                acc = acc + o[:, sl] * wx[i * home:(i + I1) * home]
            for i, (step, _) in enumerate(self_w[t]):
                acc = acc + v_c[step * home:(step + I1) * home] * wx[(I3 + i) * home:(I4 + i) * home]
            out_ref[t * home:(t + I1) * home, sl] = acc.astype(BF16)
    if has_pages:
        y_finish()
    for c in pals + sends:
        c.wait_send()


def _place_kernel(steps, heads, n_alias, *refs):
    kn_ref, vn_ref, k_ref, v_ref, mk_ref, mv_ref, wsel_ref, mig_ref, info_ref = refs[:9]
    ko_ref, vo_ref, kv_s, full = refs[9 + n_alias:]
    page, _, dim, n_slots = k_ref.shape[1:]
    n_seq = wsel_ref.shape[0]
    width = page * dim
    n_all = mig_ref.shape[0]
    moved = info_ref[0:1, :]
    w_off = info_ref[1:2, :]
    for t in range(steps):
        for which, ref in enumerate((kn_ref, vn_ref)):
            kv_s[which, t] = _dot(ref[:, 0, t].reshape(n_seq, heads * dim), wsel_ref[...], TN).astype(BF16)
    for h in range(heads):
        for which, (pool, pages, out) in enumerate(((k_ref, mk_ref, ko_ref), (v_ref, mv_ref, vo_ref))):
            full[...] = _dot(pages[:, :, h * width:(h + 1) * width].reshape(n_all, width), mig_ref[...], TN).astype(BF16).reshape(page, dim, n_slots)

            def fill(tok, _, which=which, pool=pool, out=out, h=h):
                at = w_off - tok.astype(F32)
                new = [jnp.where(at == -float(t), 1.0, 0.0) for t in range(steps)]
                kept = 1.0 - functools.reduce(jnp.add, new)
                val = full[tok] * kept.astype(BF16) + pool[0, tok, h] * (kept * (1.0 - moved)).astype(BF16)
                for t in range(steps):
                    val = val + kv_s[which, t, h * dim:(h + 1) * dim, :] * new[t].astype(BF16)
                out[0, tok, h] = val
                return 0

            lax.fori_loop(0, page, fill, 0, unroll=2)


def solution(mesh):
    n_rows, n_cols = mesh.shape['kv2'], mesh.shape['kv']
    dev_axes = ('rep', 'kv2', 'kv')
    group_axes = ('kv2', 'kv')
    seq_spec = P(None, dev_axes, None)
    pool_spec = P(dev_axes, None, None, None, None)
    table_spec = P(dev_axes, None)
    vec_spec = P(dev_axes)
    full_spec = P()
    pair = 2
    vmem = pl.BlockSpec(memory_space=pltpu.VMEM)
    dma = pltpu.SemaphoreType.DMA

    def per_device(x_embed, w_query, w_key, w_value, w_out, w_up, w_down, k_pool, v_pool, old_table, seq_len, src_slot, dst_slot):
        n_slots, layers, page, kv_heads, dim = k_pool.shape
        steps, seq_dev, width = x_embed.shape
        heads = w_query.shape[2] // dim
        group = heads // kv_heads
        n_pages = old_table.shape[1]
        n_seq = seq_dev * n_cols
        n_move = src_slot.shape[0]
        n_rt = steps * group
        n_grid = kv_heads // pair
        page_w = page * dim
        n_x = n_cols // 2
        n_dev = n_rows * n_cols
        rows = steps * seq_dev
        me = lax.axis_index('kv2') * n_cols + lax.axis_index('kv')
        slot_base = me * n_slots
        k_t, v_t = (pltpu.with_memory_space_constraint(jnp.transpose(a, (1, 2, 3, 4, 0)), pltpu.HBM) for a in (k_pool, v_pool))
        q_w, kv_w, m_w = pair * group * dim, pair * dim, pair * page_w

        def fixed(shape):
            return pl.BlockSpec(shape, lambda i: (0,) * len(shape), pipeline_mode=pl.Buffered(1))

        src_hot = ((src_slot - slot_base)[:, None] == jnp.arange(n_slots, dtype=I32)[None, :]).astype(BF16)
        page_shape = (2, n_move, kv_heads * page_w)

        def pool_blk(layer):
            return pl.BlockSpec((1, page, pair, dim, n_slots), lambda i: (layer, 0, i, 0, 0))

        page_blk = pl.BlockSpec((n_move, m_w), lambda i: (0, i))
        flat = jax.ShapeDtypeStruct((n_move, kv_heads * page_w), BF16)
        packed = pl.pallas_call(
            functools.partial(_pack_kernel, pair),
            grid=(n_grid,),
            in_specs=[pl.BlockSpec((n_move, n_slots), lambda i: (0, 0))] + [pool_blk(l) for l in range(layers) for _ in (k_t, v_t)],
            out_specs=[page_blk] * (2 * layers),
            out_shape=[flat] * (2 * layers),
            cost_estimate=_cost(8, 16),
            name='pack_pages',
        )(src_hot, *[a for _ in range(layers) for a in (k_t, v_t)])

        def whole(i, after):
            return lax.all_gather(lax.optimization_barrier((packed[i], after))[0], group_axes)

        def project(hidden, layer):
            q = jnp.dot(hidden, w_query[layer], preferred_element_type=F32).astype(BF16)
            kv = jnp.concatenate([jnp.dot(hidden, w[layer], preferred_element_type=F32).astype(BF16) for w in (w_key, w_value)], axis=1)
            return q, kv

        hidden = x_embed.reshape(rows, width)
        q, kv = project(hidden, 0)
        y, at = lax.axis_index('kv2'), lax.axis_index('kv')
        n_all = n_dev * n_move
        n_arr = n_rows * n_move

        def own_place(v):
            wide = jnp.tile(v, n_cols)[None, :]
            lane = jnp.arange(n_cols * n_move, dtype=I32)[None, :] // n_move
            return jnp.where((lane == at) & (jnp.arange(8, dtype=I32)[:, None] == y), wide, 0)

        tab = jnp.concatenate([old_table.T.reshape(-1), seq_len])[None, :]
        meta = jnp.concatenate([jnp.where(jnp.arange(8, dtype=I32)[:, None] == 0, tab, 0), own_place(src_slot), own_place(dst_slot)], axis=0)
        pages_all_shape = jax.ShapeDtypeStruct((n_rows,) + page_shape, BF16)
        q_all_shape = jax.ShapeDtypeStruct((n_cols, rows, heads * dim), BF16)
        dims = (n_rows, n_cols, n_slots, n_pages, page, seq_dev)
        pages_y, q_all, q_sel, cells, arr, info, w_sel, mig, w_info = pl.pallas_call(
            functools.partial(_head_kernel, dims),
            in_specs=[vmem] * 6,
            out_specs=[vmem] * 9,
            out_shape=[
                pages_all_shape,
                q_all_shape,
                jax.ShapeDtypeStruct((n_seq, LANES), BF16),
                jax.ShapeDtypeStruct((n_pages * n_seq, LANES), BF16),
                jax.ShapeDtypeStruct((n_arr, LANES), BF16),
                jax.ShapeDtypeStruct((8, LANES), F32),
                jax.ShapeDtypeStruct((n_seq, n_slots), BF16),
                jax.ShapeDtypeStruct((n_all, n_slots), BF16),
                jax.ShapeDtypeStruct((8, n_slots), F32),
            ],
            scratch_shapes=[pltpu.VMEM((n_dev,) + meta.shape, I32), dma((2, n_dev - 1)), dma((2, 6)), dma((2, 13))],
            compiler_params=pltpu.CompilerParams(collective_id=0, has_side_effects=True, vmem_limit_bytes=24 * MIB),
            cost_estimate=_cost(10, 4),
            name='head_gather',
        )(meta, *packed[:2], q, src_slot.reshape(1, -1), src_slot.reshape(-1, 1))

        def attend(layer, q_all, pages):
            blk = pool_blk(layer)
            ml_rows = 2 * LANES // 4
            return pl.pallas_call(
                functools.partial(_attn_kernel, steps, group, pair),
                grid=(n_grid,),
                in_specs=[
                    pl.BlockSpec((n_cols, steps, seq_dev, q_w), lambda i: (0, 0, 0, i)),
                    blk, blk,
                    pl.BlockSpec((n_rows, 1, n_move, m_w), lambda i: (0, 0, 0, i)),
                    pl.BlockSpec((n_rows, 1, n_move, m_w), lambda i: (0, 1, 0, i)),
                    fixed(q_sel.shape), fixed(cells.shape), fixed(arr.shape), fixed(info.shape),
                ],
                out_specs=[
                    pl.BlockSpec((2, n_x, steps, seq_dev, q_w), lambda i: (0, 0, 0, 0, i)),
                    pl.BlockSpec((2, n_x, steps, seq_dev, ml_rows), lambda i: (0, 0, 0, 0, 0)),
                ],
                out_shape=[
                    jax.ShapeDtypeStruct((2, n_x, steps, seq_dev, heads * dim), F32),
                    jax.ShapeDtypeStruct((2, n_x, steps, seq_dev, ml_rows), F32),
                ],
                scratch_shapes=[
                    pltpu.VMEM((steps, q_w, LANES), F32),
                    pltpu.VMEM((page, dim, LANES), F32),
                    pltpu.VMEM((page, dim, LANES), F32),
                    pltpu.VMEM((n_rt, page, LANES), F32),
                    pltpu.VMEM((n_rt * dim, LANES), F32),
                    pltpu.VMEM((2 * n_rt, LANES), F32),
                    pltpu.VMEM((steps, ml_rows, n_seq), F32),
                ],
                compiler_params=pltpu.CompilerParams(vmem_limit_bytes=32 * MIB),
                cost_estimate=_cost(20, 16),
                name='slot_attention',
            )(q_all.reshape(n_cols, steps, seq_dev, heads * dim), k_t, v_t, pages, pages, q_sel, cells, arr, info)

        def exchange(layer, o, ml, q, kv, pages):
            has = pages is not None
            half = (seq_dev, heads * dim)
            stat = (seq_dev, ml.shape[-1])
            out_shape = [jax.ShapeDtypeStruct((rows, heads * dim), BF16)] + ([pages_all_shape] if has else [])
            return pl.pallas_call(
                functools.partial(_exchange_kernel, n_cols, n_rows, heads, dim, has),
                in_specs=[vmem] * (6 if has else 4),
                out_specs=[vmem] * len(out_shape),
                out_shape=out_shape,
                scratch_shapes=[
                    pltpu.VMEM((4, steps) + half, F32), pltpu.VMEM((4, steps) + stat, F32),
                    pltpu.VMEM((5, steps) + half, F32), pltpu.VMEM((5, steps) + stat, F32),
                    pltpu.VMEM((2,) + half, F32), pltpu.VMEM((2,) + stat, F32),
                    pltpu.VMEM((2, steps) + half, F32), pltpu.VMEM((2, steps) + stat, F32),
                    pltpu.VMEM((heads, heads * dim), BF16), pltpu.VMEM((kv_w, q_w), BF16),
                    dma((2, 8)), dma((2, 12)), dma((2, 6)),
                ],
                compiler_params=pltpu.CompilerParams(collective_id=1 + layer, has_side_effects=True, vmem_limit_bytes=32 * MIB),
                cost_estimate=_cost(10, 4),
                name='exchange_partials',
            )(o, ml, q, kv, *(pages if has else []))

        kv_all, moved = [], []
        for layer in range(layers):
            if layer:
                q, kv = project(hidden, layer)
                [q_all] = pl.pallas_call(
                    functools.partial(_query_kernel, n_cols),
                    in_specs=[vmem],
                    out_specs=[vmem],
                    out_shape=[q_all_shape],
                    scratch_shapes=[dma((2, 13))],
                    compiler_params=pltpu.CompilerParams(collective_id=1 + layers + layer, has_side_effects=True, vmem_limit_bytes=16 * MIB),
                    cost_estimate=_cost(5, 4),
                    name='query_gather',
                )(q)
            kv_all.append(kv)
            if layer + 1 == layers:
                kv_rows = lax.all_gather(jnp.stack(kv_all), 'kv')
                kv_rows = kv_rows.reshape(n_cols, layers, steps, seq_dev, -1)
            o, ml = attend(layer, q_all, pages_y)
            nxt = packed[2 * (layer + 1):2 * (layer + 2)] if layer + 1 < layers else None
            moved.append(whole(2 * layer, q_all))
            attn, *more = exchange(layer, o, ml, q, kv, nxt)
            pages_y = more[0] if more else None
            moved.append(whole(2 * layer + 1, attn))
            hidden = (hidden.astype(F32) + jnp.dot(attn, w_out[layer], preferred_element_type=F32)).astype(BF16)
            up_act = jax.nn.gelu(jnp.dot(hidden, w_up[layer], preferred_element_type=F32)).astype(BF16)
            hidden = (hidden.astype(F32) + jnp.dot(up_act, w_down[layer], preferred_element_type=F32)).astype(BF16)
        v_at = kv_heads * dim // kv_w
        outs = []
        for layer in range(layers):
            blk = pool_blk(layer)
            specs = [
                pl.BlockSpec((n_cols, 1, steps, seq_dev, kv_w), lambda i, layer=layer: (0, layer, 0, 0, i)),
                pl.BlockSpec((n_cols, 1, steps, seq_dev, kv_w), lambda i, layer=layer: (0, layer, 0, 0, v_at + i)),
                blk, blk,
            ] + [pl.BlockSpec((n_dev, n_move, m_w), lambda i: (0, 0, i))] * 2 + [fixed(a.shape) for a in (w_sel, mig, w_info)]
            outs = pl.pallas_call(
                functools.partial(_place_kernel, steps, pair, len(outs)),
                grid=(n_grid,),
                in_specs=specs + [pl.BlockSpec(memory_space=pl.ANY)] * len(outs),
                out_specs=[blk, blk],
                out_shape=[jax.ShapeDtypeStruct(a.shape, BF16) for a in (k_t, v_t)],
                scratch_shapes=[pltpu.VMEM((2, steps, kv_w, n_slots), BF16), pltpu.VMEM((page, dim, n_slots), BF16)],
                input_output_aliases={len(specs) + i: i for i in range(len(outs))},
                compiler_params=pltpu.CompilerParams(vmem_limit_bytes=32 * MIB),
                cost_estimate=_cost(20, 32),
                name='place_pages',
            )(kv_rows, kv_rows, k_t, v_t, moved[2 * layer], moved[2 * layer + 1], w_sel, mig, w_info, *outs)
        k_out, v_out = outs
        y_out = hidden.reshape(steps, seq_dev, width)
        back = (4, 0, 1, 2, 3)
        return y_out, jnp.transpose(k_out, back), jnp.transpose(v_out, back)

    return jax.shard_map(per_device, mesh=mesh, in_specs=(seq_spec, full_spec, full_spec, full_spec, full_spec, full_spec, full_spec, pool_spec, pool_spec, table_spec, vec_spec, vec_spec, vec_spec), out_specs=(seq_spec, pool_spec, pool_spec), check_vma=False)
```

```python
import functools

import jax
import jax.numpy as jnp
from jax import lax
from jax.experimental import pallas as pl
from jax.experimental.pallas import tpu as pltpu
from jax.sharding import PartitionSpec as P


F32 = jnp.float32
BF16 = jnp.bfloat16
I32 = jnp.int32
NEG = -1e30
NN = (((1,), (0,)), ((), ()))
NT = (((1,), (1,)), ((), ()))
TN = (((0,), (0,)), ((), ()))
MESH = pl.DeviceIdType.MESH
LANES = 256
MIB = 2**20
I0, I1, I2, I3, I4, I5 = range(6)


def _cost(gflops, mib):
    return pl.CostEstimate(flops=gflops * 10**9, bytes_accessed=mib * MIB, transcendentals=0)


def _dot(a, b, dims):
    return lax.dot_general(a, b, dims, preferred_element_type=F32)


def _split(x):
    hi = x.astype(BF16)
    rest = x - hi.astype(F32)
    mid = rest.astype(BF16)
    low = (rest - mid.astype(F32)).astype(BF16)
    return hi, mid, low


def _pick_lhs(x, sel, dims):
    hi, mid, low = _split(x)
    return _dot(hi, sel, dims) + _dot(mid, sel, dims) + _dot(low, sel, dims)


def _pick_rhs(sel, x, dims):
    hi, mid, low = _split(x)
    return _dot(sel, hi, dims) + _dot(sel, mid, dims) + _dot(sel, low, dims)


def _columns(rows):
    full = jnp.concatenate([rows, jnp.zeros((LANES // 2 - rows.shape[0], rows.shape[1]), F32)], axis=0).T
    ids = lax.broadcasted_iota(I32, full.shape, 1)

    def column(i):
        return jnp.sum(jnp.where(ids == i, full, 0.0), axis=1, keepdims=True).astype(I32)

    return column


def _tables(dims, meta_all, mysrc_ref, mysrcc_ref, qsel_ref, cell_ref, arr_ref, info_ref, wsel_ref, mig_ref, winfo_ref):
    n_rows, n_cols, n_slots, n_pages, page, seq_dev = dims
    y, my_col = lax.axis_index('kv2'), lax.axis_index('kv')
    base = (y * n_cols + my_col) * n_slots
    n_seq = n_cols * seq_dev
    n_move = mysrc_ref.shape[1]
    n_arr = arr_ref.shape[0]
    spare = LANES - n_slots
    src = jnp.sum(meta_all[:, 8:16, :], axis=0)
    dst = jnp.sum(meta_all[:, 16:24, :], axis=0)
    tab = jnp.concatenate([meta_all[y * n_cols + i, 0:1, :] for i in range(n_cols)], axis=0).astype(F32)
    column = _columns(tab)
    tabs = [column(i) for i in range(n_cols)]
    old = jnp.concatenate([c[j * seq_dev:(j + 1) * seq_dev] for j in range(n_pages) for c in tabs], axis=0)
    lens = jnp.concatenate([c[n_pages * seq_dev:] for c in tabs], axis=0)
    per_row = n_cols * n_move
    ids = lax.broadcasted_iota(I32, (1, per_row), 1)
    entry = jnp.zeros(old.shape, F32)
    to = jnp.zeros(old.shape, F32)
    for r in range(n_rows):
        hit = old == src[r:r + 1]
        entry = entry + jnp.sum(jnp.where(hit, ids + (r * per_row + 1), 0).astype(F32), axis=1, keepdims=True)
        to = to + jnp.sum(jnp.where(hit, dst[r:r + 1] + 1, 0).astype(F32), axis=1, keepdims=True)
    entry = entry.astype(I32) - 1
    to = to.astype(I32) - 1
    is_moved = entry >= 0
    dev = entry // n_move
    nth = entry - dev * n_move
    arrival = (dev // n_cols) * n_move + nth
    free = jnp.sum(jnp.where(nth == lax.broadcasted_iota(I32, (1, n_move), 1), mysrc_ref[...] - base, 0).astype(F32), axis=1, keepdims=True).astype(I32)
    arr_lane = jnp.where(arrival < spare, n_slots + arrival, free)
    here = old - base
    here = jnp.where((here >= 0) & (here < n_slots), here, -1)
    lane = jnp.where(is_moved, jnp.where(dev % n_cols == my_col, arr_lane, -1), here)
    final = jnp.where(is_moved, to, old) - base
    lane_ids = lax.broadcasted_iota(I32, (1, LANES), 1)
    slot_ids = lax.broadcasted_iota(I32, (1, n_slots), 1)
    last = lens // page
    q_sel = jnp.zeros((n_seq, LANES), F32)
    w_sel = jnp.zeros((n_seq, n_slots), F32)
    first = jnp.zeros((1, LANES), F32)
    for j in range(n_pages):
        eq = (lane[j * n_seq:(j + 1) * n_seq] == lane_ids).astype(F32)
        cell_ref[j * n_seq:(j + 1) * n_seq, :] = eq.astype(BF16)
        q_sel = q_sel + eq
        first = first + jnp.sum(eq, axis=0, keepdims=True) * float(j * page)
        w_sel = w_sel + jnp.where((final[j * n_seq:(j + 1) * n_seq] == slot_ids) & (last == j), 1.0, 0.0)
    qsel_ref[...] = q_sel.astype(BF16)
    wsel_ref[...] = w_sel.astype(BF16)
    used = jnp.sum(q_sel, axis=0, keepdims=True)
    slot_len = jnp.sum(q_sel * lens.astype(F32), axis=0, keepdims=True)
    arr_ids = lax.broadcasted_iota(I32, (n_arr, LANES), 0)
    arr_ref[...] = jnp.where(lane_ids == n_slots + arr_ids, 1.0, 0.0).astype(BF16)
    mine = mysrcc_ref[...] - base
    arr_ref[spare:n_arr, :] = jnp.where(lane_ids == mine, 1.0, 0.0).astype(BF16)
    out_lanes = jnp.sum(jnp.where(mine == lane_ids, 1.0, 0.0), axis=0, keepdims=True)
    info_ref[...] = jnp.zeros_like(info_ref)
    info_ref[0:1, :] = used
    info_ref[1:2, :] = jnp.where(used > 0, slot_len - first - 1.0, -100.0)
    info_ref[2:3, :] = jnp.where(lane_ids >= n_slots, 1.0, out_lanes)
    written = jnp.sum(w_sel, axis=0, keepdims=True)
    w_off = jnp.sum(w_sel * (lens - last * page).astype(F32), axis=0, keepdims=True)
    to_col = _columns(dst.astype(F32))
    dst_col = jnp.concatenate([to_col(r) for r in range(n_rows)], axis=0)
    mig = jnp.where(dst_col - base == slot_ids, 1.0, 0.0)
    mig_ref[...] = mig.astype(BF16)
    winfo_ref[...] = jnp.zeros_like(winfo_ref)
    winfo_ref[0:1, :] = jnp.sum(mig, axis=0, keepdims=True)
    winfo_ref[1:2, :] = jnp.where(written > 0, w_off, -100.0)


def _pack_kernel(heads, onehot_ref, *refs):
    half = len(refs) // 2
    for src, out in zip(refs[:half], refs[half:]):
        page, _, dim, n_slots = src.shape[1:]
        width = page * dim
        for h in range(heads):
            rows = src[0, :, h].reshape(width, n_slots)
            out[:, h * width:(h + 1) * width] = _dot(onehot_ref[...], rows, NT).astype(BF16)


def _copy(src, dst, sems, k, dev):
    return pltpu.make_async_remote_copy(src_ref=src, dst_ref=dst, send_sem=sems.at[0, k], recv_sem=sems.at[1, k], device_id=dev, device_id_type=MESH)


def _rows_on_y(own, out, sems, halves):
    n = out.shape[I0]
    y = lax.axis_index('kv2')
    up, dn, far = (y + I1) % n, (y + n - I1) % n, (y + I2) % n
    to_up, to_dn = {'kv2': up}, {'kv2': dn}
    first = [
        _copy(halves(own, I0), halves(out.at[y], I0), sems, I0, to_up),
        _copy(halves(own, I1), halves(out.at[y], I1), sems, I1, to_up),
        _copy(halves(own, I1), halves(out.at[y], I1), sems, I2, to_dn),
        _copy(halves(own, I0), halves(out.at[y], I0), sems, I3, to_dn),
    ]
    relay = [
        _copy(halves(out.at[dn], I0), halves(out.at[dn], I0), sems, I4, to_up),
        _copy(halves(out.at[up], I1), halves(out.at[up], I1), sems, I5, to_dn),
    ]
    lands = [(dn, I0), (dn, I1), (up, I1), (up, I0), (far, I0), (far, I1)]

    def got(k):
        at, h = lands[k]
        _copy(halves(out.at[at], h), halves(out.at[at], h), sems, k, to_up).wait_recv()

    def start():
        for k in (I0, I2, I1, I3):
            first[k].start()

    def forward():
        got(I0)
        relay[I0].start()
        got(I2)
        relay[I1].start()

    def finish():
        for k in (I1, I3, I4, I5):
            got(k)
        for c in first + relay:
            c.wait_send()

    return start, forward, finish


def _signal_all(devs):
    barrier = pltpu.get_barrier_semaphore()
    for dev in devs:
        pl.semaphore_signal(barrier, inc=1, device_id=dev, device_id_type=MESH)
    pl.semaphore_wait(barrier, len(devs))


def _q_gather(n_cols, q_ref, q_all, x_sem):
    n_x = n_cols // I2
    at = lax.axis_index('kv')
    x, core = at // I2, at % I2
    up, dn, far = (x + I1) % n_x, (x + n_x - I1) % n_x, (x + I2) % n_x
    to_up, to_dn, to_pal = {'kv': up * I2 + core}, {'kv': dn * I2 + core}, {'kv': x * I2 + I1 - core}
    n_half = q_ref.shape[I0] // I2

    def half(ref, h):
        return ref.at[pl.ds(h * n_half, n_half)]

    def slot(pos, c):
        return q_all.at[pos * I2 + c]

    first = [
        _copy(half(q_ref, I0), half(slot(x, core), I0), x_sem, I0, to_up),
        _copy(half(q_ref, I1), half(slot(x, core), I1), x_sem, I1, to_up),
        _copy(half(q_ref, I1), half(slot(x, core), I1), x_sem, I2, to_dn),
        _copy(half(q_ref, I0), half(slot(x, core), I0), x_sem, I3, to_dn),
    ]
    relay = [
        _copy(half(slot(dn, core), I0), half(slot(dn, core), I0), x_sem, I4, to_up),
        _copy(half(slot(up, core), I1), half(slot(up, core), I1), x_sem, I5, to_dn),
    ]
    lands = [(dn, I0), (dn, I1), (up, I1), (up, I0), (far, I0), (far, I1)]
    pal = [_copy(half(slot(p, core), h), half(slot(p, core), h), x_sem, 6 + k, to_pal) for k, (p, h) in enumerate(lands)]
    own = _copy(q_ref, slot(x, core), x_sem, 12, to_pal)

    def got(k):
        p, h = lands[k]
        _copy(half(slot(p, core), h), half(slot(p, core), h), x_sem, k, to_up).wait_recv()

    for k in (I0, I2, I1, I3):
        first[k].start()
    own.start()
    q_all[at] = q_ref[...]
    yield
    got(I0)
    relay[I0].start()
    pal[I0].start()
    got(I2)
    relay[I1].start()
    pal[I2].start()
    yield
    for k in (I1, I3, I4, I5):
        got(k)
        pal[k].start()
    yield
    _copy(q_ref, slot(x, I1 - core), x_sem, 12, to_pal).wait_recv()
    for k, (p, h) in enumerate(lands):
        _copy(half(slot(p, I1 - core), h), half(slot(p, I1 - core), h), x_sem, 6 + k, to_pal).wait_recv()
    for c in first + relay + pal + [own]:
        c.wait_send()


def _x_peers(n_cols):
    n_x = n_cols // I2
    at = lax.axis_index('kv')
    x, core = at // I2, at % I2
    return [{'kv': ((x + I1) % n_x) * I2 + core}, {'kv': ((x + n_x - I1) % n_x) * I2 + core}, {'kv': x * I2 + I1 - core}]


def _y_peers(n_rows):
    y = lax.axis_index('kv2')
    return [{'kv2': (y + I1) % n_rows}, {'kv2': (y + n_rows - I1) % n_rows}]


def _half0(ref, h):
    return ref[h] if isinstance(ref, tuple) else ref.at[h]


def _head_kernel(dims, meta_ref, kp_ref, vp_ref, q_ref, mysrc_ref, mysrcc_ref, pages_all, q_all, *refs):
    tables, (meta_all, m_sem, y_sem, x_sem) = refs[:7], refs[7:]
    n_rows, n_cols = dims[:2]
    pages_ref = (kp_ref, vp_ref)
    y, at = lax.axis_index('kv2'), lax.axis_index('kv')
    offsets = [(a, b) for a in range(n_rows) for b in range(n_cols) if (a, b) != (0, 0)]
    peers = [{'kv2': (y + a) % n_rows, 'kv': (at + b) % n_cols} for a, b in offsets]
    _signal_all(peers)
    me = y * n_cols + at
    metas = [_copy(meta_ref, meta_all.at[me], m_sem, k, peers[k]) for k in range(len(peers))]
    for c in metas:
        c.start()
    start, forward, finish = _rows_on_y(pages_ref, pages_all, y_sem, _half0)
    start()
    steps = _q_gather(n_cols, q_ref, q_all, x_sem)
    next(steps)
    meta_all[me] = meta_ref[...]
    for h, ref in enumerate(pages_ref):
        pages_all[y, h] = ref[...]
    next(steps)
    forward()
    for k, (a, b) in enumerate(offsets):
        frm = ((y + n_rows - a) % n_rows) * n_cols + (at + n_cols - b) % n_cols
        _copy(meta_ref, meta_all.at[frm], m_sem, k, peers[k]).wait_recv()
    _tables(dims, meta_all, mysrc_ref, mysrcc_ref, *tables)
    next(steps)
    finish()
    for _ in steps:
        pass
    for c in metas:
        c.wait_send()


def _query_kernel(n_cols, q_ref, q_all, done_ref, x_sem):
    done_ref[...] = jnp.zeros_like(done_ref)
    _signal_all(_x_peers(n_cols))
    for _ in _q_gather(n_cols, q_ref, q_all, x_sem):
        pass


def _attn_kernel(steps, group, heads, q_ref, k_ref, v_ref, mk_ref, mv_ref, qsel_ref, cell_ref, arr_ref, info_ref, o_ref, ml_ref, q_s, mk_s, mv_s, s_s, os_s, ml_s, ml_all):
    page, _, dim, n_slots = k_ref.shape[1:]
    n_seq = qsel_ref.shape[0]
    n_core, n_x, _, home = o_ref.shape[:4]
    n_arr = arr_ref.shape[0]
    pid = pl.program_id(0)
    n_rt = steps * group
    width = page * dim
    used = info_ref[0:1, :]
    limit = info_ref[1:2, :]
    freed = info_ref[2:3, 0:n_slots] > 0
    cells = cell_ref[...]
    owned = _dot(jnp.ones((8, LANES), BF16), cells, NT)[0:1] > 0
    scale = dim ** -0.5
    q_sel = qsel_ref[...]

    @pl.when(pid == 0)
    def _():
        ml_all[...] = jnp.zeros_like(ml_all)

    for t in range(steps):
        q_s[t] = _dot(q_ref[:, t].reshape(n_seq, heads * group * dim), q_sel, TN)
    tops, sums = [[] for _ in range(steps)], [[] for _ in range(steps)]
    for h in range(heads):
        for pages, full in ((mk_ref, mk_s), (mv_ref, mv_s)):
            full[...] = _dot(pages[:, 0, :, h * width:(h + 1) * width].reshape(n_arr, width), arr_ref[...], TN).reshape(page, dim, LANES)

        def join(tok, _, h=h):
            for pool, full in ((k_ref, mk_s), (v_ref, mv_s)):
                full[tok, :, 0:n_slots] = jnp.where(freed, full[tok, :, 0:n_slots], pool[0, tok, h].astype(F32))
            return 0

        lax.fori_loop(0, page, join, 0)

        def score(pair, _, h=h):
            toks = [pair * 2, pair * 2 + 1]
            keys = [mk_s[tok] for tok in toks]
            for t in range(steps):
                for r in range(group):
                    q_row = q_s[t, (h * group + r) * dim:(h * group + r + 1) * dim, :]
                    for tok, key in zip(toks, keys):
                        s_s[t * group + r, pl.ds(tok, 1), :] = jnp.sum(key * q_row, axis=0, keepdims=True)
            return 0

        lax.fori_loop(0, page // 2, score, 0)
        visible = lax.broadcasted_iota(I32, (page, LANES), 0).astype(F32) <= limit
        for rt in range(n_rt):
            sc = jnp.where(visible, s_s[rt] * scale, NEG)
            top = jnp.max(sc, axis=0, keepdims=True)
            ex = jnp.where(visible, jnp.exp(sc - top), 0.0)
            s_s[rt] = ex
            ml_s[rt:rt + 1, :] = top
            ml_s[n_rt + rt:n_rt + rt + 1, :] = jnp.sum(ex, axis=0, keepdims=True)
        live = (used > 0) & (limit >= 0)
        m_slot = ml_s[0:n_rt]
        l_slot = ml_s[n_rt:2 * n_rt]
        m_cell = jnp.where(owned, _pick_lhs(m_slot, cells, NT), NEG)
        m_seq = m_cell[:, 0:n_seq]
        for j in range(1, cells.shape[0] // n_seq):
            m_seq = jnp.maximum(m_seq, m_cell[:, j * n_seq:(j + 1) * n_seq])
        m_back = _pick_lhs(m_seq, q_sel, NN)
        w_slot = jnp.where(live, jnp.exp(jnp.minimum(m_slot - m_back, 0.0)), 0.0)
        l_seq = _pick_lhs(l_slot * w_slot, q_sel, NT)
        for t in range(steps):
            tops[t].append(m_seq[t * group:(t + 1) * group])
            sums[t].append(l_seq[t * group:(t + 1) * group])
        for rt in range(n_rt):
            s_s[rt] = s_s[rt] * w_slot[rt:rt + 1]

        def weigh(c, _):
            row = pl.multiple_of(c * 8, 8)
            acc = [jnp.zeros((8, LANES), F32) for _ in range(n_rt)]
            for tok in range(page):
                vals = mv_s[tok, pl.ds(row, 8), :]
                for rt in range(n_rt):
                    acc[rt] = acc[rt] + s_s[rt, tok:tok + 1, :] * vals
            for rt in range(n_rt):
                os_s[pl.ds(rt * dim + row, 8), :] = acc[rt]
            return 0

        lax.fori_loop(0, dim // 8, weigh, 0)
        for t in range(steps):
            part = _pick_rhs(q_sel, os_s[t * group * dim:(t + 1) * group * dim, :], NT).reshape(n_x, n_core, home, group * dim)
            for c in range(n_core):
                o_ref[c, :, t, :, h * group * dim:(h + 1) * group * dim] = part[:, c]

    n_row = heads * group
    for t in range(steps):
        ml_all[t, pl.ds(pl.multiple_of(pid * n_row, n_row), n_row), :] = jnp.concatenate(tops[t], axis=0)
        ml_all[t, pl.ds(pl.multiple_of((pl.num_programs(0) + pid) * n_row, n_row), n_row), :] = jnp.concatenate(sums[t], axis=0)

    @pl.when(pid == pl.num_programs(0) - 1)
    def _():
        for t in range(steps):
            flat = ml_all[t].T.reshape(n_x, n_core, home, ml_all.shape[1])
            for c in range(n_core):
                ml_ref[c, :, t] = flat[:, c]


def _exchange_kernel(n_cols, n_rows, heads, dim, layer, has_pages, *refs):
    o_ref, ml_ref, q_ref, kv_ref, hid_ref, wo_ref, up_ref, down_ref = refs[:8]
    n_in = 10 if has_pages else 8
    n_out = I3 if has_pages else I2
    out_ref, done_ref = refs[n_in:n_in + I2]
    done_ref[...] = jnp.zeros_like(done_ref)
    rp_o, rp_ml, cur_o, cur_ml, rel_o, rel_ml, fin_o, fin_ml, spread, expand, p_sem, r_sem, y_sem = refs[n_in + n_out:n_in + n_out + 13]
    own_o, own_ml, attn_s, mid_s, acc_s, wo_buf, up_buf, down_buf, own_sem, w_sem = refs[n_in + n_out + 13:]
    n_x = n_cols // I2
    home = q_ref.shape[I0] // I2
    width = heads * dim
    n_buf, _, ff = up_buf.shape
    n_ff = up_ref.shape[I2] // ff

    def weights(c, slot):
        cols = pl.ds(pl.multiple_of(c * ff, ff), ff)
        return (
            pltpu.make_async_copy(up_ref.at[layer, :, cols], up_buf.at[slot], w_sem.at[I0, slot]),
            pltpu.make_async_copy(down_ref.at[layer, cols, :], down_buf.at[slot], w_sem.at[I1, slot]),
        )

    wo_copy = pltpu.make_async_copy(wo_ref.at[layer], wo_buf, own_sem.at[I0])
    at = lax.axis_index('kv')
    x, core = at // I2, at % I2
    up, dn, far = (x + I1) % n_x, (x + n_x - I1) % n_x, (x + I2) % n_x
    to_up, to_dn, to_pal = {'kv': up * I2 + core}, {'kv': dn * I2 + core}, {'kv': x * I2 + I1 - core}
    _signal_all(_x_peers(n_cols) + (_y_peers(n_rows) if has_pages else []))
    order = [far, up, dn, x]
    pals = []
    for i, pos in enumerate(order):
        pals.append(_copy(o_ref.at[I1 - core, pos], rp_o.at[i], p_sem, i, to_pal))
        pals.append(_copy(ml_ref.at[I1 - core, pos], rp_ml.at[i], p_sem, I4 + i, to_pal))
    for c in pals:
        c.start()
    owns = []
    for i, pos in enumerate(order):
        owns.append(pltpu.make_async_copy(o_ref.at[core, pos], own_o.at[i], own_sem.at[I1 + i]))
        owns.append(pltpu.make_async_copy(ml_ref.at[core, pos], own_ml.at[i], own_sem.at[I5 + i]))
    for c in owns:
        c.start()
    wo_copy.start()
    for b in range(n_buf):
        for c in weights(b, b):
            c.start()
    if has_pages:
        pages_ref, pages_all = refs[8:n_in], refs[n_in + I2]
        y_start, y_forward, y_finish = _rows_on_y(pages_ref, pages_all, y_sem, _half0)
        y_start()
        for h, ref in enumerate(pages_ref):
            pages_all[lax.axis_index('kv2'), h] = ref[...]

    n_chunk = I4
    cw = width // n_chunk
    kv_w = kv_ref.shape[I1] // I2
    kw = kv_w // n_chunk
    spread[...] = (lax.broadcasted_iota(I32, spread.shape, I1) // dim == lax.broadcasted_iota(I32, spread.shape, I0)).astype(F32).astype(BF16)
    lane = lax.broadcasted_iota(I32, expand.shape, I1)
    row = lax.broadcasted_iota(I32, expand.shape, I0)
    group = cw // kw
    expand[...] = ((lane // (dim * group) == row // dim) & (lane % dim == row % dim)).astype(F32).astype(BF16)

    def widen(w, c):
        return _pick_lhs(w, spread[:, c * cw:(c + I1) * cw], NN)

    s = jnp.zeros((I3 * home, heads), F32)
    for c in range(n_chunk):
        q_c = q_ref[:, c * cw:(c + I1) * cw].astype(F32)
        k_c = _dot(kv_ref[:, c * kw:(c + I1) * kw], expand[...], NN)
        prod = jnp.concatenate([q_c[I0:home] * k_c[I0:home], q_c[home:] * k_c[I0:home], q_c[home:] * k_c[home:]], axis=I0)
        s = s + _pick_lhs(prod, spread[:, c * cw:(c + I1) * cw], NT)
    s = s * dim ** -0.5
    s00, s10, s11 = s[I0:home], s[home:I2 * home], s[I2 * home:]
    m1 = jnp.maximum(s10, s11)
    e10, e11 = jnp.exp(s10 - m1), jnp.exp(s11 - m1)
    self_m = [s00, m1]
    self_l = [jnp.ones_like(s00), e10 + e11]
    self_w = [[(I0, None)], [(I0, e10), (I1, e11)]]

    def stats(ref):
        return ref[:, I0:heads], ref[:, heads:I2 * heads]

    def fold(a_o, a_ml, b_o, b_ml, out_o, out_ml):
        am, al = stats(a_ml)
        bm, bl = stats(b_ml)
        top = jnp.maximum(am, bm)
        aw, bw = jnp.exp(am - top), jnp.exp(bm - top)
        out_ml[:, I0:heads] = top
        out_ml[:, heads:I2 * heads] = aw * al + bw * bl
        w = jnp.concatenate([aw, bw], axis=I0)

        def chunk(c, _):
            sl = pl.ds(pl.multiple_of(c * cw, cw), cw)
            wx = _pick_lhs(w, spread[:, sl], NN)
            out_o[:, sl] = a_o[:, sl] * wx[I0:home] + b_o[:, sl] * wx[home:]
            return c

        lax.fori_loop(I0, n_chunk, chunk, I0)

    cur_ml[...] = jnp.zeros_like(cur_ml)

    def fold_pal(i):
        _copy(o_ref.at[I1 - core, order[i]], rp_o.at[i], p_sem, i, to_pal).wait_recv()
        _copy(ml_ref.at[I1 - core, order[i]], rp_ml.at[i], p_sem, I4 + i, to_pal).wait_recv()
        owns[I2 * i].wait()
        owns[I2 * i + I1].wait()
        for t in range(I2):
            fold(own_o.at[i, t], own_ml.at[i, t], rp_o.at[i, t], rp_ml.at[i, t], cur_o.at[i, t], cur_ml.at[i, t])

    sends = []

    def send(i, t, dst_o, dst_ml, k, dev):
        a = _copy(cur_o.at[i, t], dst_o, r_sem, I2 * k, dev)
        b = _copy(cur_ml.at[i, t], dst_ml, r_sem, I2 * k + I1, dev)
        a.start()
        b.start()
        sends.extend([a, b])

    def got(dst_o, dst_ml, k):
        _copy(dst_o, dst_o, r_sem, I2 * k, to_up).wait_recv()
        _copy(dst_ml, dst_ml, r_sem, I2 * k + I1, to_up).wait_recv()

    fold_pal(I0)
    send(I0, I0, rel_o.at[I0], rel_ml.at[I0], I0, to_up)
    send(I0, I1, rel_o.at[I1], rel_ml.at[I1], I1, to_dn)
    fold_pal(I1)
    send(I1, I1, fin_o.at[I0, I1], fin_ml.at[I0, I1], I2, to_up)
    fold_pal(I2)
    send(I2, I0, fin_o.at[I1, I0], fin_ml.at[I1, I0], I3, to_dn)
    got(rel_o.at[I0], rel_ml.at[I0], I0)
    fold(cur_o.at[I1, I0], cur_ml.at[I1, I0], rel_o.at[I0], rel_ml.at[I0], cur_o.at[I4, I0], cur_ml.at[I4, I0])
    send(I4, I0, fin_o.at[I0, I0], fin_ml.at[I0, I0], I4, to_up)
    got(rel_o.at[I1], rel_ml.at[I1], I1)
    fold(cur_o.at[I2, I1], cur_ml.at[I2, I1], rel_o.at[I1], rel_ml.at[I1], cur_o.at[I4, I1], cur_ml.at[I4, I1])
    send(I4, I1, fin_o.at[I1, I1], fin_ml.at[I1, I1], I5, to_dn)
    fold_pal(I3)
    if has_pages:
        y_forward()
    for side, t, k in ((I0, I1, I2), (I1, I0, I3), (I0, I0, I4), (I1, I1, I5)):
        got(fin_o.at[side, t], fin_ml.at[side, t], k)
    for t in range(I2):
        parts = [(cur_o.at[I3, t], cur_ml.at[I3, t]), (fin_o.at[I0, t], fin_ml.at[I0, t]), (fin_o.at[I1, t], fin_ml.at[I1, t])]
        ms = [stats(ml)[I0] for _, ml in parts] + [self_m[t]]
        ls = [stats(ml)[I1] for _, ml in parts] + [self_l[t]]
        top = functools.reduce(jnp.maximum, ms)
        ws = [jnp.exp(m - top) for m in ms]
        total = functools.reduce(jnp.add, [w * l for w, l in zip(ws, ls)])
        ws = [w / total for w in ws]
        own = ws.pop()
        ws += [own if e is None else own * e for _, e in self_w[t]]
        w = jnp.concatenate(ws, axis=I0)
        for c in range(n_chunk):
            wx = widen(w, c)
            sl = slice(c * cw, (c + I1) * cw)
            v_c = _dot(kv_ref[:, kv_w + c * kw:kv_w + (c + I1) * kw], expand[...], NN)
            acc = jnp.zeros((home, cw), F32)
            for i, (o, _) in enumerate(parts):
                acc = acc + o[:, sl] * wx[i * home:(i + I1) * home]
            for i, (step, _) in enumerate(self_w[t]):
                acc = acc + v_c[step * home:(step + I1) * home] * wx[(I3 + i) * home:(I4 + i) * home]
            attn_s[t * home:(t + I1) * home, sl] = acc.astype(BF16)
    if has_pages:
        y_finish()
    wo_copy.wait()

    def mix(c, _):
        sl = pl.ds(pl.multiple_of(c * cw, cw), cw)
        mid_s[:, sl] = (hid_ref[:, sl].astype(F32) + _dot(attn_s[...], wo_buf[:, sl], NN)).astype(BF16)
        acc_s[:, sl] = jnp.zeros((I2 * home, cw), F32)
        return c

    lax.fori_loop(I0, n_chunk, mix, I0)

    def mlp(c, _):
        slot = c % n_buf
        up, down = weights(c, slot)
        up.wait()
        act = jax.nn.gelu(_dot(mid_s[...], up_buf[slot], NN)).astype(BF16)
        down.wait()
        acc_s[...] += _dot(act, down_buf[slot], NN)

        @pl.when(c + n_buf < n_ff)
        def _():
            for w in weights(c + n_buf, slot):
                w.start()

        return c

    lax.fori_loop(I0, n_ff, mlp, I0)
    out_ref[...] = (mid_s[...].astype(F32) + acc_s[...]).astype(BF16)
    for c in pals + sends:
        c.wait_send()


def _place_kernel(steps, heads, n_alias, *refs):
    kn_ref, vn_ref, k_ref, v_ref, mk_ref, mv_ref, wsel_ref, mig_ref, info_ref = refs[:9]
    ko_ref, vo_ref, kv_s, full = refs[11 + n_alias:]
    page, _, dim, n_slots = k_ref.shape[1:]
    n_seq = wsel_ref.shape[0]
    width = page * dim
    n_all = mig_ref.shape[0]
    moved = info_ref[0:1, :]
    w_off = info_ref[1:2, :]
    for t in range(steps):
        for which, ref in enumerate((kn_ref, vn_ref)):
            kv_s[which, t] = _dot(ref[:, 0, t].reshape(n_seq, heads * dim), wsel_ref[...], TN).astype(BF16)

    def head(h, _):
        lanes = pl.ds(pl.multiple_of(h * width, width), width)
        for which, (pool, pages, out) in enumerate(((k_ref, mk_ref, ko_ref), (v_ref, mv_ref, vo_ref))):
            full[...] = _dot(pages[:, :, lanes].reshape(n_all, width), mig_ref[...], TN).astype(BF16).reshape(page, dim, n_slots)

            def fill(tok, _, which=which, pool=pool, out=out):
                at = w_off - tok.astype(F32)
                new = [jnp.where(at == -float(t), 1.0, 0.0) for t in range(steps)]
                kept = 1.0 - functools.reduce(jnp.add, new)
                val = full[tok] * kept.astype(BF16) + pool[0, tok, h] * (kept * (1.0 - moved)).astype(BF16)
                rows = pl.ds(pl.multiple_of(h * dim, dim), dim)
                for t in range(steps):
                    val = val + kv_s[which, t, rows, :] * new[t].astype(BF16)
                out[0, tok, h] = val
                return 0

            lax.fori_loop(0, page, fill, 0, unroll=2)
        return 0

    lax.fori_loop(0, heads, head, 0)


def solution(mesh):
    n_rows, n_cols = mesh.shape['kv2'], mesh.shape['kv']
    dev_axes = ('rep', 'kv2', 'kv')
    group_axes = ('kv2', 'kv')
    seq_spec = P(None, dev_axes, None)
    pool_spec = P(dev_axes, None, None, None, None)
    table_spec = P(dev_axes, None)
    vec_spec = P(dev_axes)
    full_spec = P()
    pair = 2
    vmem, hbm = pl.BlockSpec(memory_space=pltpu.VMEM), pl.BlockSpec(memory_space=pl.ANY)
    n_buf, ff = 8, 512
    dma = pltpu.SemaphoreType.DMA

    def per_device(x_embed, w_query, w_key, w_value, w_out, w_up, w_down, k_pool, v_pool, old_table, seq_len, src_slot, dst_slot):
        n_slots, layers, page, kv_heads, dim = k_pool.shape
        steps, seq_dev, width = x_embed.shape
        heads = w_query.shape[2] // dim
        group = heads // kv_heads
        n_pages = old_table.shape[1]
        n_seq = seq_dev * n_cols
        n_move = src_slot.shape[0]
        n_rt = steps * group
        n_grid = kv_heads // pair
        page_w = page * dim
        n_x = n_cols // 2
        n_dev = n_rows * n_cols
        rows = steps * seq_dev
        me = lax.axis_index('kv2') * n_cols + lax.axis_index('kv')
        slot_base = me * n_slots
        k_t, v_t = (pltpu.with_memory_space_constraint(jnp.transpose(a, (1, 2, 3, 4, 0)), pltpu.HBM) for a in (k_pool, v_pool))
        q_w, kv_w, m_w = pair * group * dim, pair * dim, pair * page_w

        def fixed(shape):
            return pl.BlockSpec(shape, lambda i: (0,) * len(shape), pipeline_mode=pl.Buffered(1))

        src_hot = ((src_slot - slot_base)[:, None] == jnp.arange(n_slots, dtype=I32)[None, :]).astype(BF16)
        page_shape = (2, n_move, kv_heads * page_w)

        def pool_blk(layer):
            return pl.BlockSpec((1, page, pair, dim, n_slots), lambda i: (layer, 0, i, 0, 0))

        page_blk = pl.BlockSpec((n_move, m_w), lambda i: (0, i))
        flat = jax.ShapeDtypeStruct((n_move, kv_heads * page_w), BF16)
        packed = pl.pallas_call(
            functools.partial(_pack_kernel, pair),
            grid=(n_grid,),
            in_specs=[pl.BlockSpec((n_move, n_slots), lambda i: (0, 0))] + [pool_blk(l) for l in range(layers) for _ in (k_t, v_t)],
            out_specs=[page_blk] * (2 * layers),
            out_shape=[flat] * (2 * layers),
            cost_estimate=_cost(8, 16),
            name='pack_pages',
        )(src_hot, *[a for _ in range(layers) for a in (k_t, v_t)])

        def whole(i, after):
            page, token = lax.optimization_barrier((packed[i], after))
            return lax.all_gather(page, group_axes), token

        def project(hidden, layer):
            q = jnp.dot(hidden, w_query[layer], preferred_element_type=F32).astype(BF16)
            kv = jnp.concatenate([jnp.dot(hidden, w[layer], preferred_element_type=F32).astype(BF16) for w in (w_key, w_value)], axis=1)
            return q, kv

        hidden = x_embed.reshape(rows, width)
        q, kv = project(hidden, 0)
        y, at = lax.axis_index('kv2'), lax.axis_index('kv')
        n_all = n_dev * n_move
        n_arr = n_rows * n_move

        def own_place(v):
            wide = jnp.tile(v, n_cols)[None, :]
            lane = jnp.arange(n_cols * n_move, dtype=I32)[None, :] // n_move
            return jnp.where((lane == at) & (jnp.arange(8, dtype=I32)[:, None] == y), wide, 0)

        tab = jnp.concatenate([old_table.T.reshape(-1), seq_len])[None, :]
        meta = jnp.concatenate([jnp.where(jnp.arange(8, dtype=I32)[:, None] == 0, tab, 0), own_place(src_slot), own_place(dst_slot)], axis=0)
        pages_all_shape = jax.ShapeDtypeStruct((n_rows,) + page_shape, BF16)
        done_shape = jax.ShapeDtypeStruct((8, 128), F32)
        q_all_shape = jax.ShapeDtypeStruct((n_cols, rows, heads * dim), BF16)
        dims = (n_rows, n_cols, n_slots, n_pages, page, seq_dev)
        pages_y, q_all, q_sel, cells, arr, info, w_sel, mig, w_info = pl.pallas_call(
            functools.partial(_head_kernel, dims),
            in_specs=[vmem] * 6,
            out_specs=[vmem] * 9,
            out_shape=[
                pages_all_shape,
                q_all_shape,
                jax.ShapeDtypeStruct((n_seq, LANES), BF16),
                jax.ShapeDtypeStruct((n_pages * n_seq, LANES), BF16),
                jax.ShapeDtypeStruct((n_arr, LANES), BF16),
                jax.ShapeDtypeStruct((8, LANES), F32),
                jax.ShapeDtypeStruct((n_seq, n_slots), BF16),
                jax.ShapeDtypeStruct((n_all, n_slots), BF16),
                jax.ShapeDtypeStruct((8, n_slots), F32),
            ],
            scratch_shapes=[pltpu.VMEM((n_dev,) + meta.shape, I32), dma((2, n_dev - 1)), dma((2, 6)), dma((2, 13))],
            compiler_params=pltpu.CompilerParams(collective_id=0, has_side_effects=True, vmem_limit_bytes=24 * MIB),
            cost_estimate=_cost(10, 4),
            name='head_gather',
        )(meta, *packed[:2], q, src_slot.reshape(1, -1), src_slot.reshape(-1, 1))

        def attend(layer, q_all, pages):
            blk = pool_blk(layer)
            ml_rows = 2 * LANES // 4
            return pl.pallas_call(
                functools.partial(_attn_kernel, steps, group, pair),
                grid=(n_grid,),
                in_specs=[
                    pl.BlockSpec((n_cols, steps, seq_dev, q_w), lambda i: (0, 0, 0, i)),
                    blk, blk,
                    pl.BlockSpec((n_rows, 1, n_move, m_w), lambda i: (0, 0, 0, i)),
                    pl.BlockSpec((n_rows, 1, n_move, m_w), lambda i: (0, 1, 0, i)),
                    fixed(q_sel.shape), fixed(cells.shape), fixed(arr.shape), fixed(info.shape),
                ],
                out_specs=[
                    pl.BlockSpec((2, n_x, steps, seq_dev, q_w), lambda i: (0, 0, 0, 0, i)),
                    pl.BlockSpec((2, n_x, steps, seq_dev, ml_rows), lambda i: (0, 0, 0, 0, 0)),
                ],
                out_shape=[
                    jax.ShapeDtypeStruct((2, n_x, steps, seq_dev, heads * dim), F32),
                    jax.ShapeDtypeStruct((2, n_x, steps, seq_dev, ml_rows), F32),
                ],
                scratch_shapes=[
                    pltpu.VMEM((steps, q_w, LANES), F32),
                    pltpu.VMEM((page, dim, LANES), F32),
                    pltpu.VMEM((page, dim, LANES), F32),
                    pltpu.VMEM((n_rt, page, LANES), F32),
                    pltpu.VMEM((n_rt * dim, LANES), F32),
                    pltpu.VMEM((2 * n_rt, LANES), F32),
                    pltpu.VMEM((steps, ml_rows, n_seq), F32),
                ],
                compiler_params=pltpu.CompilerParams(vmem_limit_bytes=60 * MIB),
                cost_estimate=_cost(20, 16),
                name='slot_attention',
            )(q_all.reshape(n_cols, steps, seq_dev, heads * dim), k_t, v_t, pages, pages, q_sel, cells, arr, info)

        def exchange(layer, o, ml, q, kv, hidden, pages):
            has = pages is not None
            half = (seq_dev, heads * dim)
            stat = (seq_dev, ml.shape[-1])
            out_shape = [jax.ShapeDtypeStruct((rows, width), BF16), done_shape] + ([pages_all_shape] if has else [])
            return pl.pallas_call(
                functools.partial(_exchange_kernel, n_cols, n_rows, heads, dim, layer, has),
                in_specs=[hbm, hbm, vmem, vmem, vmem, hbm, hbm, hbm] + [vmem] * (2 if has else 0),
                out_specs=[vmem] * len(out_shape),
                out_shape=out_shape,
                scratch_shapes=[
                    pltpu.VMEM((4, steps) + half, F32), pltpu.VMEM((4, steps) + stat, F32),
                    pltpu.VMEM((5, steps) + half, F32), pltpu.VMEM((5, steps) + stat, F32),
                    pltpu.VMEM((2,) + half, F32), pltpu.VMEM((2,) + stat, F32),
                    pltpu.VMEM((2, steps) + half, F32), pltpu.VMEM((2, steps) + stat, F32),
                    pltpu.VMEM((heads, heads * dim), BF16), pltpu.VMEM((kv_w, q_w), BF16),
                    dma((2, 8)), dma((2, 12)), dma((2, 6)),
                    pltpu.VMEM((4, steps) + half, F32), pltpu.VMEM((4, steps) + stat, F32),
                    pltpu.VMEM((rows, heads * dim), BF16), pltpu.VMEM((rows, width), BF16), pltpu.VMEM((rows, width), F32),
                    pltpu.VMEM(w_out.shape[1:], BF16), pltpu.VMEM((n_buf, width, ff), BF16), pltpu.VMEM((n_buf, ff, width), BF16),
                    dma((9,)), dma((2, n_buf)),
                ],
                compiler_params=pltpu.CompilerParams(collective_id=1 + layer, has_side_effects=True, vmem_limit_bytes=56 * MIB),
                cost_estimate=_cost(10, 4),
                name='exchange_partials',
            )(o, ml, q, kv, hidden, w_out, w_up, w_down, *(pages if has else []))

        kv_all, moved, done = [], [], info
        for layer in range(layers):
            if layer:
                q, kv = project(hidden, layer)
                q_all, done = pl.pallas_call(
                    functools.partial(_query_kernel, n_cols),
                    in_specs=[vmem],
                    out_specs=[vmem] * 2,
                    out_shape=[q_all_shape, done_shape],
                    scratch_shapes=[dma((2, 13))],
                    compiler_params=pltpu.CompilerParams(collective_id=1 + layers + layer, has_side_effects=True, vmem_limit_bytes=16 * MIB),
                    cost_estimate=_cost(5, 4),
                    name='query_gather',
                )(q)
            kv_all.append(kv)
            if layer + 1 == layers:
                kv_rows = lax.all_gather(jnp.stack(kv_all), 'kv')
                kv_rows = kv_rows.reshape(n_cols, layers, steps, seq_dev, -1)
            o, ml = attend(layer, q_all, pages_y)
            nxt = packed[2 * (layer + 1):2 * (layer + 2)] if layer + 1 < layers else None
            moved.append(whole(2 * layer, done))
            hidden, done, *more = exchange(layer, o, ml, q, kv, hidden, nxt)
            pages_y = more[0] if more else None
            moved.append(whole(2 * layer + 1, done))
        v_at = kv_heads * dim // kv_w
        outs = []
        for layer in range(layers):
            blk = pool_blk(layer)
            pages, tokens = zip(*moved[2 * layer:2 * layer + 2])
            specs = [
                pl.BlockSpec((n_cols, 1, steps, seq_dev, kv_w), lambda i, layer=layer: (0, layer, 0, 0, i)),
                pl.BlockSpec((n_cols, 1, steps, seq_dev, kv_w), lambda i, layer=layer: (0, layer, 0, 0, v_at + i)),
                blk, blk,
            ] + [pl.BlockSpec((n_dev, n_move, m_w), lambda i: (0, 0, i))] * 2 + [fixed(a.shape) for a in (w_sel, mig, w_info)]
            outs = pl.pallas_call(
                functools.partial(_place_kernel, steps, pair, len(outs)),
                grid=(n_grid,),
                in_specs=specs + [pl.BlockSpec(memory_space=pl.ANY)] * (2 + len(outs)),
                out_specs=[blk, blk],
                out_shape=[jax.ShapeDtypeStruct(a.shape, BF16) for a in (k_t, v_t)],
                scratch_shapes=[pltpu.VMEM((2, steps, kv_w, n_slots), BF16), pltpu.VMEM((page, dim, n_slots), BF16)],
                input_output_aliases={len(specs) + 2 + i: i for i in range(len(outs))},
                compiler_params=pltpu.CompilerParams(vmem_limit_bytes=60 * MIB),
                cost_estimate=_cost(20, 32),
                name='place_pages',
            )(kv_rows, kv_rows, k_t, v_t, *pages, w_sel, mig, w_info, *tokens, *outs)
        k_out, v_out = outs
        y_out = hidden.reshape(steps, seq_dev, width)
        back = (4, 0, 1, 2, 3)
        return y_out, jnp.transpose(k_out, back), jnp.transpose(v_out, back)

    return jax.shard_map(per_device, mesh=mesh, in_specs=(seq_spec, full_spec, full_spec, full_spec, full_spec, full_spec, full_spec, pool_spec, pool_spec, table_spec, vec_spec, vec_spec, vec_spec), out_specs=(seq_spec, pool_spec, pool_spec), check_vma=False)
```

```python
import functools

import jax
import jax.numpy as jnp
from jax import lax
from jax.experimental import pallas as pl
from jax.experimental.pallas import tpu as pltpu
from jax.sharding import PartitionSpec as P


F32 = jnp.float32
BF16 = jnp.bfloat16
I32 = jnp.int32
NEG = -1e30
NN = (((1,), (0,)), ((), ()))
NT = (((1,), (1,)), ((), ()))
TN = (((0,), (0,)), ((), ()))
MESH = pl.DeviceIdType.MESH
LANES = 256
MIB = 2**20
I0, I1, I2, I3, I4, I5 = range(6)


def _cost(gflops, mib):
    return pl.CostEstimate(flops=gflops * 10**9, bytes_accessed=mib * MIB, transcendentals=0)


def _dot(a, b, dims):
    return lax.dot_general(a, b, dims, preferred_element_type=F32)


def _split(x):
    hi = x.astype(BF16)
    rest = x - hi.astype(F32)
    mid = rest.astype(BF16)
    low = (rest - mid.astype(F32)).astype(BF16)
    return hi, mid, low


def _pick_lhs(x, sel, dims):
    hi, mid, low = _split(x)
    return _dot(hi, sel, dims) + _dot(mid, sel, dims) + _dot(low, sel, dims)


def _pick_rhs(sel, x, dims):
    hi, mid, low = _split(x)
    return _dot(sel, hi, dims) + _dot(sel, mid, dims) + _dot(sel, low, dims)


def _columns(rows):
    full = jnp.concatenate([rows, jnp.zeros((LANES // 2 - rows.shape[0], rows.shape[1]), F32)], axis=0).T
    ids = lax.broadcasted_iota(I32, full.shape, 1)

    def column(i):
        return jnp.sum(jnp.where(ids == i, full, 0.0), axis=1, keepdims=True).astype(I32)

    return column


def _tables(dims, meta_all, mysrc_ref, mysrcc_ref, qsel_ref, cell_ref, arr_ref, info_ref, wsel_ref, mig_ref, winfo_ref):
    n_rows, n_cols, n_slots, n_pages, page, seq_dev = dims
    y, my_col = lax.axis_index('kv2'), lax.axis_index('kv')
    base = (y * n_cols + my_col) * n_slots
    n_seq = n_cols * seq_dev
    n_move = mysrc_ref.shape[1]
    n_arr = arr_ref.shape[0]
    spare = LANES - n_slots
    src = jnp.sum(meta_all[:, 8:16, :], axis=0)
    dst = jnp.sum(meta_all[:, 16:24, :], axis=0)
    tab = jnp.concatenate([meta_all[y * n_cols + i, 0:1, :] for i in range(n_cols)], axis=0).astype(F32)
    column = _columns(tab)
    tabs = [column(i) for i in range(n_cols)]
    old = jnp.concatenate([c[j * seq_dev:(j + 1) * seq_dev] for j in range(n_pages) for c in tabs], axis=0)
    lens = jnp.concatenate([c[n_pages * seq_dev:] for c in tabs], axis=0)
    per_row = n_cols * n_move
    ids = lax.broadcasted_iota(I32, (1, per_row), 1)
    entry = jnp.zeros(old.shape, F32)
    to = jnp.zeros(old.shape, F32)
    for r in range(n_rows):
        hit = old == src[r:r + 1]
        entry = entry + jnp.sum(jnp.where(hit, ids + (r * per_row + 1), 0).astype(F32), axis=1, keepdims=True)
        to = to + jnp.sum(jnp.where(hit, dst[r:r + 1] + 1, 0).astype(F32), axis=1, keepdims=True)
    entry = entry.astype(I32) - 1
    to = to.astype(I32) - 1
    is_moved = entry >= 0
    dev = entry // n_move
    nth = entry - dev * n_move
    arrival = (dev // n_cols) * n_move + nth
    free = jnp.sum(jnp.where(nth == lax.broadcasted_iota(I32, (1, n_move), 1), mysrc_ref[...] - base, 0).astype(F32), axis=1, keepdims=True).astype(I32)
    arr_lane = jnp.where(arrival < spare, n_slots + arrival, free)
    here = old - base
    here = jnp.where((here >= 0) & (here < n_slots), here, -1)
    lane = jnp.where(is_moved, jnp.where(dev % n_cols == my_col, arr_lane, -1), here)
    final = jnp.where(is_moved, to, old) - base
    lane_ids = lax.broadcasted_iota(I32, (1, LANES), 1)
    slot_ids = lax.broadcasted_iota(I32, (1, n_slots), 1)
    last = lens // page
    q_sel = jnp.zeros((n_seq, LANES), F32)
    w_sel = jnp.zeros((n_seq, n_slots), F32)
    first = jnp.zeros((1, LANES), F32)
    for j in range(n_pages):
        eq = (lane[j * n_seq:(j + 1) * n_seq] == lane_ids).astype(F32)
        cell_ref[j * n_seq:(j + 1) * n_seq, :] = eq.astype(BF16)
        q_sel = q_sel + eq
        first = first + jnp.sum(eq, axis=0, keepdims=True) * float(j * page)
        w_sel = w_sel + jnp.where((final[j * n_seq:(j + 1) * n_seq] == slot_ids) & (last == j), 1.0, 0.0)
    qsel_ref[...] = q_sel.astype(BF16)
    wsel_ref[...] = w_sel.astype(BF16)
    used = jnp.sum(q_sel, axis=0, keepdims=True)
    slot_len = jnp.sum(q_sel * lens.astype(F32), axis=0, keepdims=True)
    arr_ids = lax.broadcasted_iota(I32, (n_arr, LANES), 0)
    arr_ref[...] = jnp.where(lane_ids == n_slots + arr_ids, 1.0, 0.0).astype(BF16)
    mine = mysrcc_ref[...] - base
    arr_ref[spare:n_arr, :] = jnp.where(lane_ids == mine, 1.0, 0.0).astype(BF16)
    out_lanes = jnp.sum(jnp.where(mine == lane_ids, 1.0, 0.0), axis=0, keepdims=True)
    info_ref[...] = jnp.zeros_like(info_ref)
    info_ref[0:1, :] = used
    info_ref[1:2, :] = jnp.where(used > 0, slot_len - first - 1.0, -100.0)
    info_ref[2:3, :] = jnp.where(lane_ids >= n_slots, 1.0, out_lanes)
    written = jnp.sum(w_sel, axis=0, keepdims=True)
    w_off = jnp.sum(w_sel * (lens - last * page).astype(F32), axis=0, keepdims=True)
    to_col = _columns(dst.astype(F32))
    dst_col = jnp.concatenate([to_col(r) for r in range(n_rows)], axis=0)
    mig = jnp.where(dst_col - base == slot_ids, 1.0, 0.0)
    mig_ref[...] = mig.astype(BF16)
    winfo_ref[...] = jnp.zeros_like(winfo_ref)
    winfo_ref[0:1, :] = jnp.sum(mig, axis=0, keepdims=True)
    winfo_ref[1:2, :] = jnp.where(written > 0, w_off, -100.0)


def _pack_kernel(heads, onehot_ref, *refs):
    n_in = len(refs) * 2 // 3
    for i, src in enumerate(refs[:n_in]):
        page, _, dim, n_slots = src.shape[1:]
        width = page * dim
        out = refs[n_in + i // 2].at[i % 2]
        for h in range(heads):
            rows = src[0, :, h].reshape(width, n_slots)
            out[:, h * width:(h + 1) * width] = _dot(onehot_ref[...], rows, NT).astype(BF16)


def _copy(src, dst, sems, k, dev):
    return pltpu.make_async_remote_copy(src_ref=src, dst_ref=dst, send_sem=sems.at[0, k], recv_sem=sems.at[1, k], device_id=dev, device_id_type=MESH)


def _rows_on_y(own, out, sems, halves):
    n = out.shape[I0]
    y = lax.axis_index('kv2')
    up, dn, far = (y + I1) % n, (y + n - I1) % n, (y + I2) % n
    to_up, to_dn = {'kv2': up}, {'kv2': dn}
    first = [
        _copy(halves(own, I0), halves(out.at[y], I0), sems, I0, to_up),
        _copy(halves(own, I1), halves(out.at[y], I1), sems, I1, to_up),
        _copy(halves(own, I1), halves(out.at[y], I1), sems, I2, to_dn),
        _copy(halves(own, I0), halves(out.at[y], I0), sems, I3, to_dn),
    ]
    relay = [
        _copy(halves(out.at[dn], I0), halves(out.at[dn], I0), sems, I4, to_up),
        _copy(halves(out.at[up], I1), halves(out.at[up], I1), sems, I5, to_dn),
    ]
    lands = [(dn, I0), (dn, I1), (up, I1), (up, I0), (far, I0), (far, I1)]

    def got(k):
        at, h = lands[k]
        _copy(halves(out.at[at], h), halves(out.at[at], h), sems, k, to_up).wait_recv()

    def start():
        for k in (I0, I2, I1, I3):
            first[k].start()

    def forward():
        got(I0)
        relay[I0].start()
        got(I2)
        relay[I1].start()

    def finish():
        for k in (I1, I3, I4, I5):
            got(k)
        for c in first + relay:
            c.wait_send()

    return start, forward, finish


def _signal_all(devs):
    barrier = pltpu.get_barrier_semaphore()
    for dev in devs:
        pl.semaphore_signal(barrier, inc=1, device_id=dev, device_id_type=MESH)
    pl.semaphore_wait(barrier, len(devs))


def _q_gather(n_cols, q_ref, q_all, x_sem):
    n_x = n_cols // I2
    at = lax.axis_index('kv')
    x, core = at // I2, at % I2
    up, dn, far = (x + I1) % n_x, (x + n_x - I1) % n_x, (x + I2) % n_x
    to_up, to_dn, to_pal = {'kv': up * I2 + core}, {'kv': dn * I2 + core}, {'kv': x * I2 + I1 - core}
    n_half = q_ref.shape[I0] // I2

    def half(ref, h):
        return ref.at[pl.ds(h * n_half, n_half)]

    def slot(pos, c):
        return q_all.at[pos * I2 + c]

    first = [
        _copy(half(q_ref, I0), half(slot(x, core), I0), x_sem, I0, to_up),
        _copy(half(q_ref, I1), half(slot(x, core), I1), x_sem, I1, to_up),
        _copy(half(q_ref, I1), half(slot(x, core), I1), x_sem, I2, to_dn),
        _copy(half(q_ref, I0), half(slot(x, core), I0), x_sem, I3, to_dn),
    ]
    relay = [
        _copy(half(slot(dn, core), I0), half(slot(dn, core), I0), x_sem, I4, to_up),
        _copy(half(slot(up, core), I1), half(slot(up, core), I1), x_sem, I5, to_dn),
    ]
    lands = [(dn, I0), (dn, I1), (up, I1), (up, I0), (far, I0), (far, I1)]
    pal = [_copy(half(slot(p, core), h), half(slot(p, core), h), x_sem, 6 + k, to_pal) for k, (p, h) in enumerate(lands)]
    own = _copy(q_ref, slot(x, core), x_sem, 12, to_pal)

    def got(k):
        p, h = lands[k]
        _copy(half(slot(p, core), h), half(slot(p, core), h), x_sem, k, to_up).wait_recv()

    for k in (I0, I2, I1, I3):
        first[k].start()
    own.start()
    q_all[at] = q_ref[...]
    yield
    got(I0)
    relay[I0].start()
    pal[I0].start()
    got(I2)
    relay[I1].start()
    pal[I2].start()
    yield
    for k in (I1, I3, I4, I5):
        got(k)
        pal[k].start()
    yield
    _copy(q_ref, slot(x, I1 - core), x_sem, 12, to_pal).wait_recv()
    for k, (p, h) in enumerate(lands):
        _copy(half(slot(p, I1 - core), h), half(slot(p, I1 - core), h), x_sem, 6 + k, to_pal).wait_recv()
    for c in first + relay + pal + [own]:
        c.wait_send()


def _x_peers(n_cols):
    n_x = n_cols // I2
    at = lax.axis_index('kv')
    x, core = at // I2, at % I2
    return [{'kv': ((x + I1) % n_x) * I2 + core}, {'kv': ((x + n_x - I1) % n_x) * I2 + core}, {'kv': x * I2 + I1 - core}]


def _y_peers(n_rows):
    y = lax.axis_index('kv2')
    return [{'kv2': (y + I1) % n_rows}, {'kv2': (y + n_rows - I1) % n_rows}]


def _half0(ref, h):
    return ref.at[h]


def _head_kernel(dims, meta_ref, pages_ref, q_ref, mysrc_ref, mysrcc_ref, pages_all, q_all, *refs):
    tables, (meta_all, m_sem, y_sem, x_sem) = refs[:7], refs[7:]
    n_rows, n_cols = dims[:2]
    y, at = lax.axis_index('kv2'), lax.axis_index('kv')
    offsets = [(a, b) for a in range(n_rows) for b in range(n_cols) if (a, b) != (0, 0)]
    peers = [{'kv2': (y + a) % n_rows, 'kv': (at + b) % n_cols} for a, b in offsets]
    _signal_all(peers)
    me = y * n_cols + at
    metas = [_copy(meta_ref, meta_all.at[me], m_sem, k, peers[k]) for k in range(len(peers))]
    for c in metas:
        c.start()
    start, forward, finish = _rows_on_y(pages_ref, pages_all, y_sem, _half0)
    start()
    steps = _q_gather(n_cols, q_ref, q_all, x_sem)
    next(steps)
    meta_all[me] = meta_ref[...]
    pages_all[y] = pages_ref[...]
    next(steps)
    forward()
    for k, (a, b) in enumerate(offsets):
        frm = ((y + n_rows - a) % n_rows) * n_cols + (at + n_cols - b) % n_cols
        _copy(meta_ref, meta_all.at[frm], m_sem, k, peers[k]).wait_recv()
    _tables(dims, meta_all, mysrc_ref, mysrcc_ref, *tables)
    next(steps)
    finish()
    for _ in steps:
        pass
    for c in metas:
        c.wait_send()


def _query_kernel(n_cols, q_ref, q_all, x_sem):
    _signal_all(_x_peers(n_cols))
    for _ in _q_gather(n_cols, q_ref, q_all, x_sem):
        pass


def _attn_kernel(steps, group, heads, q_ref, k_ref, v_ref, mk_ref, mv_ref, qsel_ref, cell_ref, arr_ref, info_ref, o_ref, ml_ref, q_s, mk_s, mv_s, s_s, os_s, ml_s, ml_all):
    page, _, dim, n_slots = k_ref.shape[1:]
    n_seq = qsel_ref.shape[0]
    n_core, n_x, _, home = o_ref.shape[:4]
    n_arr = arr_ref.shape[0]
    pid = pl.program_id(0)
    n_rt = steps * group
    width = page * dim
    used = info_ref[0:1, :]
    limit = info_ref[1:2, :]
    freed = info_ref[2:3, 0:n_slots] > 0
    cells = cell_ref[...]
    owned = _dot(jnp.ones((8, LANES), BF16), cells, NT)[0:1] > 0
    scale = dim ** -0.5
    q_sel = qsel_ref[...]

    @pl.when(pid == 0)
    def _():
        ml_all[...] = jnp.zeros_like(ml_all)

    for t in range(steps):
        q_s[t] = _dot(q_ref[:, t].reshape(n_seq, heads * group * dim), q_sel, TN)
    tops, sums = [[] for _ in range(steps)], [[] for _ in range(steps)]
    for h in range(heads):
        for pages, full in ((mk_ref, mk_s), (mv_ref, mv_s)):
            full[...] = _dot(pages[:, 0, :, h * width:(h + 1) * width].reshape(n_arr, width), arr_ref[...], TN).reshape(page, dim, LANES)

        def join(tok, _, h=h):
            for pool, full in ((k_ref, mk_s), (v_ref, mv_s)):
                full[tok, :, 0:n_slots] = jnp.where(freed, full[tok, :, 0:n_slots], pool[0, tok, h].astype(F32))
            return 0

        lax.fori_loop(0, page, join, 0)

        def score(pair, _, h=h):
            toks = [pair * 2, pair * 2 + 1]
            keys = [mk_s[tok] for tok in toks]
            for t in range(steps):
                for r in range(group):
                    q_row = q_s[t, (h * group + r) * dim:(h * group + r + 1) * dim, :]
                    for tok, key in zip(toks, keys):
                        s_s[t * group + r, pl.ds(tok, 1), :] = jnp.sum(key * q_row, axis=0, keepdims=True)
            return 0

        lax.fori_loop(0, page // 2, score, 0)
        visible = lax.broadcasted_iota(I32, (page, LANES), 0).astype(F32) <= limit
        for rt in range(n_rt):
            sc = jnp.where(visible, s_s[rt] * scale, NEG)
            top = jnp.max(sc, axis=0, keepdims=True)
            ex = jnp.where(visible, jnp.exp(sc - top), 0.0)
            s_s[rt] = ex
            ml_s[rt:rt + 1, :] = top
            ml_s[n_rt + rt:n_rt + rt + 1, :] = jnp.sum(ex, axis=0, keepdims=True)
        live = (used > 0) & (limit >= 0)
        m_slot = ml_s[0:n_rt]
        l_slot = ml_s[n_rt:2 * n_rt]
        m_cell = jnp.where(owned, _pick_lhs(m_slot, cells, NT), NEG)
        m_seq = m_cell[:, 0:n_seq]
        for j in range(1, cells.shape[0] // n_seq):
            m_seq = jnp.maximum(m_seq, m_cell[:, j * n_seq:(j + 1) * n_seq])
        m_back = _pick_lhs(m_seq, q_sel, NN)
        w_slot = jnp.where(live, jnp.exp(jnp.minimum(m_slot - m_back, 0.0)), 0.0)
        l_seq = _pick_lhs(l_slot * w_slot, q_sel, NT)
        for t in range(steps):
            tops[t].append(m_seq[t * group:(t + 1) * group])
            sums[t].append(l_seq[t * group:(t + 1) * group])
        for rt in range(n_rt):
            s_s[rt] = s_s[rt] * w_slot[rt:rt + 1]

        def weigh(c, _):
            row = pl.multiple_of(c * 8, 8)
            acc = [jnp.zeros((8, LANES), F32) for _ in range(n_rt)]
            for tok in range(page):
                vals = mv_s[tok, pl.ds(row, 8), :]
                for rt in range(n_rt):
                    acc[rt] = acc[rt] + s_s[rt, tok:tok + 1, :] * vals
            for rt in range(n_rt):
                os_s[pl.ds(rt * dim + row, 8), :] = acc[rt]
            return 0

        lax.fori_loop(0, dim // 8, weigh, 0)
        for t in range(steps):
            part = _pick_rhs(q_sel, os_s[t * group * dim:(t + 1) * group * dim, :], NT).reshape(n_x, n_core, home, group * dim)
            for c in range(n_core):
                o_ref[c, :, t, :, h * group * dim:(h + 1) * group * dim] = part[:, c]

    n_row = heads * group
    for t in range(steps):
        ml_all[t, pl.ds(pl.multiple_of(pid * n_row, n_row), n_row), :] = jnp.concatenate(tops[t], axis=0)
        ml_all[t, pl.ds(pl.multiple_of((pl.num_programs(0) + pid) * n_row, n_row), n_row), :] = jnp.concatenate(sums[t], axis=0)

    @pl.when(pid == pl.num_programs(0) - 1)
    def _():
        for t in range(steps):
            flat = ml_all[t].T.reshape(n_x, n_core, home, ml_all.shape[1])
            for c in range(n_core):
                ml_ref[c, :, t] = flat[:, c]


def _exchange_kernel(n_cols, n_rows, heads, dim, has_pages, *refs):
    o_ref, ml_ref, q_ref, kv_ref = refs[:I4]
    n_in = I5 if has_pages else I4
    n_out = I3 if has_pages else I2
    out_ref, done_ref = refs[n_in:n_in + I2]
    done_ref[...] = jnp.zeros_like(done_ref)
    rp_o, rp_ml, cur_o, cur_ml, rel_o, rel_ml, fin_o, fin_ml, spread, expand, p_sem, r_sem, y_sem = refs[n_in + n_out:]
    n_x = n_cols // I2
    home = q_ref.shape[I0] // I2
    width = heads * dim
    at = lax.axis_index('kv')
    x, core = at // I2, at % I2
    up, dn, far = (x + I1) % n_x, (x + n_x - I1) % n_x, (x + I2) % n_x
    to_up, to_dn, to_pal = {'kv': up * I2 + core}, {'kv': dn * I2 + core}, {'kv': x * I2 + I1 - core}
    _signal_all(_x_peers(n_cols) + (_y_peers(n_rows) if has_pages else []))
    order = [far, up, dn, x]
    pals = []
    for i, pos in enumerate(order):
        pals.append(_copy(o_ref.at[I1 - core, pos], rp_o.at[i], p_sem, i, to_pal))
        pals.append(_copy(ml_ref.at[I1 - core, pos], rp_ml.at[i], p_sem, I4 + i, to_pal))
    for c in pals:
        c.start()
    if has_pages:
        pages_ref, pages_all = refs[I4], refs[n_in + I2]
        y_start, y_forward, y_finish = _rows_on_y(pages_ref, pages_all, y_sem, _half0)
        y_start()
        pages_all[lax.axis_index('kv2')] = pages_ref[...]

    n_chunk = I4
    cw = width // n_chunk
    kv_w = kv_ref.shape[I1] // I2
    kw = kv_w // n_chunk
    spread[...] = (lax.broadcasted_iota(I32, spread.shape, I1) // dim == lax.broadcasted_iota(I32, spread.shape, I0)).astype(F32).astype(BF16)
    lane = lax.broadcasted_iota(I32, expand.shape, I1)
    row = lax.broadcasted_iota(I32, expand.shape, I0)
    group = cw // kw
    expand[...] = ((lane // (dim * group) == row // dim) & (lane % dim == row % dim)).astype(F32).astype(BF16)

    def widen(w, c):
        return _pick_lhs(w, spread[:, c * cw:(c + I1) * cw], NN)

    s = jnp.zeros((I3 * home, heads), F32)
    for c in range(n_chunk):
        q_c = q_ref[:, c * cw:(c + I1) * cw].astype(F32)
        k_c = _dot(kv_ref[:, c * kw:(c + I1) * kw], expand[...], NN)
        prod = jnp.concatenate([q_c[I0:home] * k_c[I0:home], q_c[home:] * k_c[I0:home], q_c[home:] * k_c[home:]], axis=I0)
        s = s + _pick_lhs(prod, spread[:, c * cw:(c + I1) * cw], NT)
    s = s * dim ** -0.5
    s00, s10, s11 = s[I0:home], s[home:I2 * home], s[I2 * home:]
    m1 = jnp.maximum(s10, s11)
    e10, e11 = jnp.exp(s10 - m1), jnp.exp(s11 - m1)
    self_m = [s00, m1]
    self_l = [jnp.ones_like(s00), e10 + e11]
    self_w = [[(I0, None)], [(I0, e10), (I1, e11)]]

    def stats(ref):
        return ref[:, I0:heads], ref[:, heads:I2 * heads]

    def fold(a_o, a_ml, b_o, b_ml, out_o, out_ml):
        am, al = stats(a_ml)
        bm, bl = stats(b_ml)
        top = jnp.maximum(am, bm)
        aw, bw = jnp.exp(am - top), jnp.exp(bm - top)
        out_ml[:, I0:heads] = top
        out_ml[:, heads:I2 * heads] = aw * al + bw * bl
        w = jnp.concatenate([aw, bw], axis=I0)

        def chunk(c, _):
            sl = pl.ds(pl.multiple_of(c * cw, cw), cw)
            wx = _pick_lhs(w, spread[:, sl], NN)
            out_o[:, sl] = a_o[:, sl] * wx[I0:home] + b_o[:, sl] * wx[home:]
            return c

        lax.fori_loop(I0, n_chunk, chunk, I0)

    cur_ml[...] = jnp.zeros_like(cur_ml)

    def fold_pal(i):
        _copy(o_ref.at[I1 - core, order[i]], rp_o.at[i], p_sem, i, to_pal).wait_recv()
        _copy(ml_ref.at[I1 - core, order[i]], rp_ml.at[i], p_sem, I4 + i, to_pal).wait_recv()
        for t in range(I2):
            fold(o_ref.at[core, order[i], t], ml_ref.at[core, order[i], t], rp_o.at[i, t], rp_ml.at[i, t], cur_o.at[i, t], cur_ml.at[i, t])

    sends = []

    def send(i, t, dst_o, dst_ml, k, dev):
        a = _copy(cur_o.at[i, t], dst_o, r_sem, I2 * k, dev)
        b = _copy(cur_ml.at[i, t], dst_ml, r_sem, I2 * k + I1, dev)
        a.start()
        b.start()
        sends.extend([a, b])

    def got(dst_o, dst_ml, k):
        _copy(dst_o, dst_o, r_sem, I2 * k, to_up).wait_recv()
        _copy(dst_ml, dst_ml, r_sem, I2 * k + I1, to_up).wait_recv()

    fold_pal(I0)
    send(I0, I0, rel_o.at[I0], rel_ml.at[I0], I0, to_up)
    send(I0, I1, rel_o.at[I1], rel_ml.at[I1], I1, to_dn)
    fold_pal(I1)
    send(I1, I1, fin_o.at[I0, I1], fin_ml.at[I0, I1], I2, to_up)
    fold_pal(I2)
    send(I2, I0, fin_o.at[I1, I0], fin_ml.at[I1, I0], I3, to_dn)
    got(rel_o.at[I0], rel_ml.at[I0], I0)
    fold(cur_o.at[I1, I0], cur_ml.at[I1, I0], rel_o.at[I0], rel_ml.at[I0], cur_o.at[I4, I0], cur_ml.at[I4, I0])
    send(I4, I0, fin_o.at[I0, I0], fin_ml.at[I0, I0], I4, to_up)
    got(rel_o.at[I1], rel_ml.at[I1], I1)
    fold(cur_o.at[I2, I1], cur_ml.at[I2, I1], rel_o.at[I1], rel_ml.at[I1], cur_o.at[I4, I1], cur_ml.at[I4, I1])
    send(I4, I1, fin_o.at[I1, I1], fin_ml.at[I1, I1], I5, to_dn)
    fold_pal(I3)
    if has_pages:
        y_forward()
    for side, t, k in ((I0, I1, I2), (I1, I0, I3), (I0, I0, I4), (I1, I1, I5)):
        got(fin_o.at[side, t], fin_ml.at[side, t], k)
    for t in range(I2):
        parts = [(cur_o.at[I3, t], cur_ml.at[I3, t]), (fin_o.at[I0, t], fin_ml.at[I0, t]), (fin_o.at[I1, t], fin_ml.at[I1, t])]
        ms = [stats(ml)[I0] for _, ml in parts] + [self_m[t]]
        ls = [stats(ml)[I1] for _, ml in parts] + [self_l[t]]
        top = functools.reduce(jnp.maximum, ms)
        ws = [jnp.exp(m - top) for m in ms]
        total = functools.reduce(jnp.add, [w * l for w, l in zip(ws, ls)])
        ws = [w / total for w in ws]
        own = ws.pop()
        ws += [own if e is None else own * e for _, e in self_w[t]]
        w = jnp.concatenate(ws, axis=I0)
        for c in range(n_chunk):
            wx = widen(w, c)
            sl = slice(c * cw, (c + I1) * cw)
            v_c = _dot(kv_ref[:, kv_w + c * kw:kv_w + (c + I1) * kw], expand[...], NN)
            acc = jnp.zeros((home, cw), F32)
            for i, (o, _) in enumerate(parts):
                acc = acc + o[:, sl] * wx[i * home:(i + I1) * home]
            for i, (step, _) in enumerate(self_w[t]):
                acc = acc + v_c[step * home:(step + I1) * home] * wx[(I3 + i) * home:(I4 + i) * home]
            out_ref[t * home:(t + I1) * home, sl] = acc.astype(BF16)
    if has_pages:
        y_finish()
    for c in pals + sends:
        c.wait_send()


def _place_kernel(steps, heads, n_alias, *refs):
    kn_ref, vn_ref, k_ref, v_ref, mk_ref, mv_ref, wsel_ref, mig_ref, info_ref = refs[:9]
    ko_ref, vo_ref, kv_s, full = refs[10 + n_alias:]
    page, _, dim, n_slots = k_ref.shape[1:]
    n_seq = wsel_ref.shape[0]
    width = page * dim
    n_all = mig_ref.shape[0]
    moved = info_ref[0:1, :]
    w_off = info_ref[1:2, :]
    for t in range(steps):
        for which, ref in enumerate((kn_ref, vn_ref)):
            kv_s[which, t] = _dot(ref[:, 0, t].reshape(n_seq, heads * dim), wsel_ref[...], TN).astype(BF16)

    def head(h, _):
        lanes = pl.ds(pl.multiple_of(h * width, width), width)
        for which, (pool, pages, out) in enumerate(((k_ref, mk_ref, ko_ref), (v_ref, mv_ref, vo_ref))):
            full[...] = _dot(pages[:, 0, :, lanes].reshape(n_all, width), mig_ref[...], TN).astype(BF16).reshape(page, dim, n_slots)

            def fill(tok, _, which=which, pool=pool, out=out):
                at = w_off - tok.astype(F32)
                new = [jnp.where(at == -float(t), 1.0, 0.0) for t in range(steps)]
                kept = 1.0 - functools.reduce(jnp.add, new)
                val = full[tok] * kept.astype(BF16) + pool[0, tok, h] * (kept * (1.0 - moved)).astype(BF16)
                rows = pl.ds(pl.multiple_of(h * dim, dim), dim)
                for t in range(steps):
                    val = val + kv_s[which, t, rows, :] * new[t].astype(BF16)
                out[0, tok, h] = val
                return 0

            lax.fori_loop(0, page, fill, 0)
        return 0

    lax.fori_loop(0, heads, head, 0)


def solution(mesh):
    n_rows, n_cols = mesh.shape['kv2'], mesh.shape['kv']
    dev_axes = ('rep', 'kv2', 'kv')
    group_axes = ('kv2', 'kv')
    seq_spec = P(None, dev_axes, None)
    pool_spec = P(dev_axes, None, None, None, None)
    table_spec = P(dev_axes, None)
    vec_spec = P(dev_axes)
    full_spec = P()
    pair = 2
    vmem = pl.BlockSpec(memory_space=pltpu.VMEM)
    dma = pltpu.SemaphoreType.DMA

    def per_device(x_embed, w_query, w_key, w_value, w_out, w_up, w_down, k_pool, v_pool, old_table, seq_len, src_slot, dst_slot):
        n_slots, layers, page, kv_heads, dim = k_pool.shape
        steps, seq_dev, width = x_embed.shape
        heads = w_query.shape[2] // dim
        group = heads // kv_heads
        n_pages = old_table.shape[1]
        n_seq = seq_dev * n_cols
        n_move = src_slot.shape[0]
        n_rt = steps * group
        n_grid = kv_heads // pair
        page_w = page * dim
        n_x = n_cols // 2
        n_dev = n_rows * n_cols
        rows = steps * seq_dev
        me = lax.axis_index('kv2') * n_cols + lax.axis_index('kv')
        slot_base = me * n_slots
        k_t, v_t = (pltpu.with_memory_space_constraint(jnp.transpose(a, (1, 2, 3, 4, 0)), pltpu.HBM) for a in (k_pool, v_pool))
        q_w, kv_w, m_w = pair * group * dim, pair * dim, pair * page_w

        def fixed(shape):
            return pl.BlockSpec(shape, lambda i: (0,) * len(shape), pipeline_mode=pl.Buffered(1))

        src_hot = ((src_slot - slot_base)[:, None] == jnp.arange(n_slots, dtype=I32)[None, :]).astype(BF16)
        page_shape = (2, n_move, kv_heads * page_w)

        def pool_blk(layer):
            return pl.BlockSpec((1, page, pair, dim, n_slots), lambda i: (layer, 0, i, 0, 0))

        page_blk = pl.BlockSpec((2, n_move, m_w), lambda i: (0, 0, i))
        flat = jax.ShapeDtypeStruct(page_shape, BF16)
        packed = pl.pallas_call(
            functools.partial(_pack_kernel, pair),
            grid=(n_grid,),
            in_specs=[pl.BlockSpec((n_move, n_slots), lambda i: (0, 0))] + [pool_blk(l) for l in range(layers) for _ in (k_t, v_t)],
            out_specs=[page_blk] * layers,
            out_shape=[flat] * layers,
            cost_estimate=_cost(8, 16),
            name='pack_pages',
        )(src_hot, *[a for _ in range(layers) for a in (k_t, v_t)])

        def whole(i, after):
            page, token = (packed[i], src_hot) if after is None else lax.optimization_barrier((packed[i], after))
            return lax.all_gather(page, group_axes), token

        def project(hidden, layer):
            q = jnp.dot(hidden, w_query[layer], preferred_element_type=F32).astype(BF16)
            kv = jnp.concatenate([jnp.dot(hidden, w[layer], preferred_element_type=F32).astype(BF16) for w in (w_key, w_value)], axis=1)
            return q, kv

        hidden = x_embed.reshape(rows, width)
        q, kv = project(hidden, 0)
        y, at = lax.axis_index('kv2'), lax.axis_index('kv')
        n_all = n_dev * n_move
        n_arr = n_rows * n_move

        def own_place(v):
            wide = jnp.tile(v, n_cols)[None, :]
            lane = jnp.arange(n_cols * n_move, dtype=I32)[None, :] // n_move
            return jnp.where((lane == at) & (jnp.arange(8, dtype=I32)[:, None] == y), wide, 0)

        tab = jnp.concatenate([old_table.T.reshape(-1), seq_len])[None, :]
        meta = jnp.concatenate([jnp.where(jnp.arange(8, dtype=I32)[:, None] == 0, tab, 0), own_place(src_slot), own_place(dst_slot)], axis=0)
        pages_all_shape = jax.ShapeDtypeStruct((n_rows,) + page_shape, BF16)
        done_shape = jax.ShapeDtypeStruct((8, 128), F32)
        q_all_shape = jax.ShapeDtypeStruct((n_cols, rows, heads * dim), BF16)
        dims = (n_rows, n_cols, n_slots, n_pages, page, seq_dev)
        pages_y, q_all, q_sel, cells, arr, info, w_sel, mig, w_info = pl.pallas_call(
            functools.partial(_head_kernel, dims),
            in_specs=[vmem] * 5,
            out_specs=[vmem] * 9,
            out_shape=[
                pages_all_shape,
                q_all_shape,
                jax.ShapeDtypeStruct((n_seq, LANES), BF16),
                jax.ShapeDtypeStruct((n_pages * n_seq, LANES), BF16),
                jax.ShapeDtypeStruct((n_arr, LANES), BF16),
                jax.ShapeDtypeStruct((8, LANES), F32),
                jax.ShapeDtypeStruct((n_seq, n_slots), BF16),
                jax.ShapeDtypeStruct((n_all, n_slots), BF16),
                jax.ShapeDtypeStruct((8, n_slots), F32),
            ],
            scratch_shapes=[pltpu.VMEM((n_dev,) + meta.shape, I32), dma((2, n_dev - 1)), dma((2, 6)), dma((2, 13))],
            compiler_params=pltpu.CompilerParams(collective_id=0, has_side_effects=True, vmem_limit_bytes=24 * MIB),
            cost_estimate=_cost(10, 4),
            name='head_gather',
        )(meta, packed[0], q, src_slot.reshape(1, -1), src_slot.reshape(-1, 1))

        def attend(layer, q_all, pages):
            blk = pool_blk(layer)
            ml_rows = 2 * LANES // 4
            return pl.pallas_call(
                functools.partial(_attn_kernel, steps, group, pair),
                grid=(n_grid,),
                in_specs=[
                    pl.BlockSpec((n_cols, steps, seq_dev, q_w), lambda i: (0, 0, 0, i)),
                    blk, blk,
                    pl.BlockSpec((n_rows, 1, n_move, m_w), lambda i: (0, 0, 0, i)),
                    pl.BlockSpec((n_rows, 1, n_move, m_w), lambda i: (0, 1, 0, i)),
                    fixed(q_sel.shape), fixed(cells.shape), fixed(arr.shape), fixed(info.shape),
                ],
                out_specs=[
                    pl.BlockSpec((2, n_x, steps, seq_dev, q_w), lambda i: (0, 0, 0, 0, i)),
                    pl.BlockSpec((2, n_x, steps, seq_dev, ml_rows), lambda i: (0, 0, 0, 0, 0)),
                ],
                out_shape=[
                    jax.ShapeDtypeStruct((2, n_x, steps, seq_dev, heads * dim), F32),
                    jax.ShapeDtypeStruct((2, n_x, steps, seq_dev, ml_rows), F32),
                ],
                scratch_shapes=[
                    pltpu.VMEM((steps, q_w, LANES), F32),
                    pltpu.VMEM((page, dim, LANES), F32),
                    pltpu.VMEM((page, dim, LANES), F32),
                    pltpu.VMEM((n_rt, page, LANES), F32),
                    pltpu.VMEM((n_rt * dim, LANES), F32),
                    pltpu.VMEM((2 * n_rt, LANES), F32),
                    pltpu.VMEM((steps, ml_rows, n_seq), F32),
                ],
                compiler_params=pltpu.CompilerParams(vmem_limit_bytes=32 * MIB),
                cost_estimate=_cost(20, 16),
                name='slot_attention',
            )(q_all.reshape(n_cols, steps, seq_dev, heads * dim), k_t, v_t, pages, pages, q_sel, cells, arr, info)

        def exchange(layer, o, ml, q, kv, pages):
            has = pages is not None
            half = (seq_dev, heads * dim)
            stat = (seq_dev, ml.shape[-1])
            out_shape = [jax.ShapeDtypeStruct((rows, heads * dim), BF16), done_shape] + ([pages_all_shape] if has else [])
            return pl.pallas_call(
                functools.partial(_exchange_kernel, n_cols, n_rows, heads, dim, has),
                in_specs=[vmem] * (5 if has else 4),
                out_specs=[vmem] * len(out_shape),
                out_shape=out_shape,
                scratch_shapes=[
                    pltpu.VMEM((4, steps) + half, F32), pltpu.VMEM((4, steps) + stat, F32),
                    pltpu.VMEM((5, steps) + half, F32), pltpu.VMEM((5, steps) + stat, F32),
                    pltpu.VMEM((2,) + half, F32), pltpu.VMEM((2,) + stat, F32),
                    pltpu.VMEM((2, steps) + half, F32), pltpu.VMEM((2, steps) + stat, F32),
                    pltpu.VMEM((heads, heads * dim), BF16), pltpu.VMEM((kv_w, q_w), BF16),
                    dma((2, 8)), dma((2, 12)), dma((2, 6)),
                ],
                compiler_params=pltpu.CompilerParams(collective_id=1 + layer, has_side_effects=True, vmem_limit_bytes=32 * MIB),
                cost_estimate=_cost(10, 4),
                name='exchange_partials',
            )(o, ml, q, kv, *([pages] if has else []))

        kv_all, moved, done = [], [], None
        for layer in range(layers):
            if layer:
                q, kv = project(hidden, layer)
                [q_all] = pl.pallas_call(
                    functools.partial(_query_kernel, n_cols),
                    in_specs=[vmem],
                    out_specs=[vmem],
                    out_shape=[q_all_shape],
                    scratch_shapes=[dma((2, 13))],
                    compiler_params=pltpu.CompilerParams(collective_id=1 + layers + layer, has_side_effects=True, vmem_limit_bytes=16 * MIB),
                    cost_estimate=_cost(5, 4),
                    name='query_gather',
                )(q)
            kv_all.append(kv)
            if layer + 1 == layers:
                kv_rows = lax.all_gather(jnp.stack(kv_all), 'kv')
                kv_rows = kv_rows.reshape(n_cols, layers, steps, seq_dev, -1)
            o, ml = attend(layer, q_all, pages_y)
            nxt = packed[layer + 1] if layer + 1 < layers else None
            moved.append(whole(layer, done))
            attn, done, *more = exchange(layer, o, ml, q, kv, nxt)
            pages_y = more[0] if more else None
            hidden = (hidden.astype(F32) + jnp.dot(attn, w_out[layer], preferred_element_type=F32)).astype(BF16)
            up_act = jax.nn.gelu(jnp.dot(hidden, w_up[layer], preferred_element_type=F32)).astype(BF16)
            hidden = (hidden.astype(F32) + jnp.dot(up_act, w_down[layer], preferred_element_type=F32)).astype(BF16)
        v_at = kv_heads * dim // kv_w
        outs = []
        for layer in range(layers):
            blk = pool_blk(layer)
            pages, token = moved[layer]
            specs = [
                pl.BlockSpec((n_cols, 1, steps, seq_dev, kv_w), lambda i, layer=layer: (0, layer, 0, 0, i)),
                pl.BlockSpec((n_cols, 1, steps, seq_dev, kv_w), lambda i, layer=layer: (0, layer, 0, 0, v_at + i)),
                blk, blk,
            ] + [pl.BlockSpec((n_dev, 1, n_move, m_w), lambda i, which=which: (0, which, 0, i)) for which in range(2)] + [fixed(a.shape) for a in (w_sel, mig, w_info)]
            outs = pl.pallas_call(
                functools.partial(_place_kernel, steps, pair, len(outs)),
                grid=(n_grid,),
                in_specs=specs + [pl.BlockSpec(memory_space=pl.ANY)] * (1 + len(outs)),
                out_specs=[blk, blk],
                out_shape=[jax.ShapeDtypeStruct(a.shape, BF16) for a in (k_t, v_t)],
                scratch_shapes=[pltpu.VMEM((2, steps, kv_w, n_slots), BF16), pltpu.VMEM((page, dim, n_slots), BF16)],
                input_output_aliases={len(specs) + 1 + i: i for i in range(len(outs))},
                compiler_params=pltpu.CompilerParams(vmem_limit_bytes=60 * MIB),
                cost_estimate=_cost(20, 32),
                name='place_pages',
            )(kv_rows, kv_rows, k_t, v_t, pages, pages, w_sel, mig, w_info, token, *outs)
        k_out, v_out = outs
        y_out = hidden.reshape(steps, seq_dev, width)
        back = (4, 0, 1, 2, 3)
        return y_out, jnp.transpose(k_out, back), jnp.transpose(v_out, back)

    return jax.shard_map(per_device, mesh=mesh, in_specs=(seq_spec, full_spec, full_spec, full_spec, full_spec, full_spec, full_spec, pool_spec, pool_spec, table_spec, vec_spec, vec_spec, vec_spec), out_specs=(seq_spec, pool_spec, pool_spec), check_vma=False)
```

```python
import functools

import jax
import jax.numpy as jnp
from jax import lax
from jax.experimental import pallas as pl
from jax.experimental.pallas import tpu as pltpu
from jax.sharding import PartitionSpec as P


F32 = jnp.float32
BF16 = jnp.bfloat16
I32 = jnp.int32
NEG = -1e30
NN = (((1,), (0,)), ((), ()))
NT = (((1,), (1,)), ((), ()))
TN = (((0,), (0,)), ((), ()))
MESH = pl.DeviceIdType.MESH
LANES = 256
MIB = 2**20
I0, I1, I2, I3, I4, I5 = range(6)


def _cost(gflops, mib):
    return pl.CostEstimate(flops=gflops * 10**9, bytes_accessed=mib * MIB, transcendentals=0)


def _dot(a, b, dims):
    return lax.dot_general(a, b, dims, preferred_element_type=F32)


def _split(x):
    hi = x.astype(BF16)
    rest = x - hi.astype(F32)
    mid = rest.astype(BF16)
    low = (rest - mid.astype(F32)).astype(BF16)
    return hi, mid, low


def _pick_lhs(x, sel, dims):
    hi, mid, low = _split(x)
    return _dot(hi, sel, dims) + _dot(mid, sel, dims) + _dot(low, sel, dims)


def _pick_rhs(sel, x, dims):
    hi, mid, low = _split(x)
    return _dot(sel, hi, dims) + _dot(sel, mid, dims) + _dot(sel, low, dims)


def _columns(rows):
    full = jnp.concatenate([rows, jnp.zeros((LANES // 2 - rows.shape[0], rows.shape[1]), F32)], axis=0).T
    ids = lax.broadcasted_iota(I32, full.shape, 1)

    def column(i):
        return jnp.sum(jnp.where(ids == i, full, 0.0), axis=1, keepdims=True).astype(I32)

    return column


def _tables(dims, meta_all, mysrc_ref, mysrcc_ref, qsel_ref, cell_ref, arr_ref, info_ref, wsel_ref, mig_ref, winfo_ref):
    n_rows, n_cols, n_slots, n_pages, page, seq_dev = dims
    y, my_col = lax.axis_index('kv2'), lax.axis_index('kv')
    base = (y * n_cols + my_col) * n_slots
    n_seq = n_cols * seq_dev
    n_move = mysrc_ref.shape[1]
    n_arr = arr_ref.shape[0]
    spare = LANES - n_slots
    src = jnp.sum(meta_all[:, 8:16, :], axis=0)
    dst = jnp.sum(meta_all[:, 16:24, :], axis=0)
    tab = jnp.concatenate([meta_all[y * n_cols + i, 0:1, :] for i in range(n_cols)], axis=0).astype(F32)
    column = _columns(tab)
    tabs = [column(i) for i in range(n_cols)]
    old = jnp.concatenate([c[j * seq_dev:(j + 1) * seq_dev] for j in range(n_pages) for c in tabs], axis=0)
    lens = jnp.concatenate([c[n_pages * seq_dev:] for c in tabs], axis=0)
    per_row = n_cols * n_move
    ids = lax.broadcasted_iota(I32, (1, per_row), 1)
    entry = jnp.zeros(old.shape, F32)
    to = jnp.zeros(old.shape, F32)
    for r in range(n_rows):
        hit = old == src[r:r + 1]
        entry = entry + jnp.sum(jnp.where(hit, ids + (r * per_row + 1), 0).astype(F32), axis=1, keepdims=True)
        to = to + jnp.sum(jnp.where(hit, dst[r:r + 1] + 1, 0).astype(F32), axis=1, keepdims=True)
    entry = entry.astype(I32) - 1
    to = to.astype(I32) - 1
    is_moved = entry >= 0
    dev = entry // n_move
    nth = entry - dev * n_move
    arrival = (dev // n_cols) * n_move + nth
    free = jnp.sum(jnp.where(nth == lax.broadcasted_iota(I32, (1, n_move), 1), mysrc_ref[...] - base, 0).astype(F32), axis=1, keepdims=True).astype(I32)
    arr_lane = jnp.where(arrival < spare, n_slots + arrival, free)
    here = old - base
    here = jnp.where((here >= 0) & (here < n_slots), here, -1)
    lane = jnp.where(is_moved, jnp.where(dev % n_cols == my_col, arr_lane, -1), here)
    final = jnp.where(is_moved, to, old) - base
    lane_ids = lax.broadcasted_iota(I32, (1, LANES), 1)
    slot_ids = lax.broadcasted_iota(I32, (1, n_slots), 1)
    last = lens // page
    q_sel = jnp.zeros((n_seq, LANES), F32)
    w_sel = jnp.zeros((n_seq, n_slots), F32)
    first = jnp.zeros((1, LANES), F32)
    for j in range(n_pages):
        eq = (lane[j * n_seq:(j + 1) * n_seq] == lane_ids).astype(F32)
        cell_ref[j * n_seq:(j + 1) * n_seq, :] = eq.astype(BF16)
        q_sel = q_sel + eq
        first = first + jnp.sum(eq, axis=0, keepdims=True) * float(j * page)
        w_sel = w_sel + jnp.where((final[j * n_seq:(j + 1) * n_seq] == slot_ids) & (last == j), 1.0, 0.0)
    qsel_ref[...] = q_sel.astype(BF16)
    wsel_ref[...] = w_sel.astype(BF16)
    used = jnp.sum(q_sel, axis=0, keepdims=True)
    slot_len = jnp.sum(q_sel * lens.astype(F32), axis=0, keepdims=True)
    arr_ids = lax.broadcasted_iota(I32, (n_arr, LANES), 0)
    arr_ref[...] = jnp.where(lane_ids == n_slots + arr_ids, 1.0, 0.0).astype(BF16)
    mine = mysrcc_ref[...] - base
    arr_ref[spare:n_arr, :] = jnp.where(lane_ids == mine, 1.0, 0.0).astype(BF16)
    out_lanes = jnp.sum(jnp.where(mine == lane_ids, 1.0, 0.0), axis=0, keepdims=True)
    info_ref[...] = jnp.zeros_like(info_ref)
    info_ref[0:1, :] = used
    info_ref[1:2, :] = jnp.where(used > 0, slot_len - first - 1.0, -100.0)
    info_ref[2:3, :] = jnp.where(lane_ids >= n_slots, 1.0, out_lanes)
    written = jnp.sum(w_sel, axis=0, keepdims=True)
    w_off = jnp.sum(w_sel * (lens - last * page).astype(F32), axis=0, keepdims=True)
    to_col = _columns(dst.astype(F32))
    dst_col = jnp.concatenate([to_col(r) for r in range(n_rows)], axis=0)
    mig = jnp.where(dst_col - base == slot_ids, 1.0, 0.0)
    mig_ref[...] = mig.astype(BF16)
    winfo_ref[...] = jnp.zeros_like(winfo_ref)
    winfo_ref[0:1, :] = jnp.sum(mig, axis=0, keepdims=True)
    winfo_ref[1:2, :] = jnp.where(written > 0, w_off, -100.0)


def _pack_kernel(heads, onehot_ref, *refs):
    n_in = len(refs) * 2 // 3
    for i, src in enumerate(refs[:n_in]):
        page, _, dim, n_slots = src.shape[1:]
        width = page * dim
        out = refs[n_in + i // 2].at[i % 2]
        for h in range(heads):
            rows = src[0, :, h].reshape(width, n_slots)
            out[:, h * width:(h + 1) * width] = _dot(onehot_ref[...], rows, NT).astype(BF16)


def _copy(src, dst, sems, k, dev):
    return pltpu.make_async_remote_copy(src_ref=src, dst_ref=dst, send_sem=sems.at[0, k], recv_sem=sems.at[1, k], device_id=dev, device_id_type=MESH)


def _rows_on_y(own, out, sems, halves):
    n = out.shape[I0]
    y = lax.axis_index('kv2')
    up, dn, far = (y + I1) % n, (y + n - I1) % n, (y + I2) % n
    to_up, to_dn = {'kv2': up}, {'kv2': dn}
    first = [
        _copy(halves(own, I0), halves(out.at[y], I0), sems, I0, to_up),
        _copy(halves(own, I1), halves(out.at[y], I1), sems, I1, to_up),
        _copy(halves(own, I1), halves(out.at[y], I1), sems, I2, to_dn),
        _copy(halves(own, I0), halves(out.at[y], I0), sems, I3, to_dn),
    ]
    relay = [
        _copy(halves(out.at[dn], I0), halves(out.at[dn], I0), sems, I4, to_up),
        _copy(halves(out.at[up], I1), halves(out.at[up], I1), sems, I5, to_dn),
    ]
    lands = [(dn, I0), (dn, I1), (up, I1), (up, I0), (far, I0), (far, I1)]

    def got(k):
        at, h = lands[k]
        _copy(halves(out.at[at], h), halves(out.at[at], h), sems, k, to_up).wait_recv()

    def start():
        for k in (I0, I2, I1, I3):
            first[k].start()

    def forward():
        got(I0)
        relay[I0].start()
        got(I2)
        relay[I1].start()

    def finish():
        for k in (I1, I3, I4, I5):
            got(k)
        for c in first + relay:
            c.wait_send()

    return start, forward, finish


def _signal_all(devs):
    barrier = pltpu.get_barrier_semaphore()
    for dev in devs:
        pl.semaphore_signal(barrier, inc=1, device_id=dev, device_id_type=MESH)
    pl.semaphore_wait(barrier, len(devs))


def _q_gather(n_cols, q_ref, q_all, x_sem):
    n_x = n_cols // I2
    at = lax.axis_index('kv')
    x, core = at // I2, at % I2
    up, dn, far = (x + I1) % n_x, (x + n_x - I1) % n_x, (x + I2) % n_x
    to_up, to_dn, to_pal = {'kv': up * I2 + core}, {'kv': dn * I2 + core}, {'kv': x * I2 + I1 - core}
    n_half = q_ref.shape[I0] // I2

    def half(ref, h):
        return ref.at[pl.ds(h * n_half, n_half)]

    def slot(pos, c):
        return q_all.at[pos * I2 + c]

    first = [
        _copy(half(q_ref, I0), half(slot(x, core), I0), x_sem, I0, to_up),
        _copy(half(q_ref, I1), half(slot(x, core), I1), x_sem, I1, to_up),
        _copy(half(q_ref, I1), half(slot(x, core), I1), x_sem, I2, to_dn),
        _copy(half(q_ref, I0), half(slot(x, core), I0), x_sem, I3, to_dn),
    ]
    relay = [
        _copy(half(slot(dn, core), I0), half(slot(dn, core), I0), x_sem, I4, to_up),
        _copy(half(slot(up, core), I1), half(slot(up, core), I1), x_sem, I5, to_dn),
    ]
    lands = [(dn, I0), (dn, I1), (up, I1), (up, I0), (far, I0), (far, I1)]
    pal = [_copy(half(slot(p, core), h), half(slot(p, core), h), x_sem, 6 + k, to_pal) for k, (p, h) in enumerate(lands)]
    own = _copy(q_ref, slot(x, core), x_sem, 12, to_pal)

    def got(k):
        p, h = lands[k]
        _copy(half(slot(p, core), h), half(slot(p, core), h), x_sem, k, to_up).wait_recv()

    for k in (I0, I2, I1, I3):
        first[k].start()
    own.start()
    q_all[at] = q_ref[...]
    yield
    got(I0)
    relay[I0].start()
    pal[I0].start()
    got(I2)
    relay[I1].start()
    pal[I2].start()
    yield
    for k in (I1, I3, I4, I5):
        got(k)
        pal[k].start()
    yield
    _copy(q_ref, slot(x, I1 - core), x_sem, 12, to_pal).wait_recv()
    for k, (p, h) in enumerate(lands):
        _copy(half(slot(p, I1 - core), h), half(slot(p, I1 - core), h), x_sem, 6 + k, to_pal).wait_recv()
    for c in first + relay + pal + [own]:
        c.wait_send()


def _x_peers(n_cols):
    n_x = n_cols // I2
    at = lax.axis_index('kv')
    x, core = at // I2, at % I2
    return [{'kv': ((x + I1) % n_x) * I2 + core}, {'kv': ((x + n_x - I1) % n_x) * I2 + core}, {'kv': x * I2 + I1 - core}]


def _y_peers(n_rows):
    y = lax.axis_index('kv2')
    return [{'kv2': (y + I1) % n_rows}, {'kv2': (y + n_rows - I1) % n_rows}]


def _half0(ref, h):
    return ref.at[h]


def _head_kernel(dims, meta_ref, pages_ref, q_ref, mysrc_ref, mysrcc_ref, pages_all, q_all, *refs):
    tables, (meta_all, m_sem, y_sem, x_sem) = refs[:7], refs[7:]
    n_rows, n_cols = dims[:2]
    y, at = lax.axis_index('kv2'), lax.axis_index('kv')
    offsets = [(a, b) for a in range(n_rows) for b in range(n_cols) if (a, b) != (0, 0)]
    peers = [{'kv2': (y + a) % n_rows, 'kv': (at + b) % n_cols} for a, b in offsets]
    _signal_all(peers)
    me = y * n_cols + at
    metas = [_copy(meta_ref, meta_all.at[me], m_sem, k, peers[k]) for k in range(len(peers))]
    for c in metas:
        c.start()
    start, forward, finish = _rows_on_y(pages_ref, pages_all, y_sem, _half0)
    start()
    steps = _q_gather(n_cols, q_ref, q_all, x_sem)
    next(steps)
    meta_all[me] = meta_ref[...]
    pages_all[y] = pages_ref[...]
    next(steps)
    forward()
    for k, (a, b) in enumerate(offsets):
        frm = ((y + n_rows - a) % n_rows) * n_cols + (at + n_cols - b) % n_cols
        _copy(meta_ref, meta_all.at[frm], m_sem, k, peers[k]).wait_recv()
    _tables(dims, meta_all, mysrc_ref, mysrcc_ref, *tables)
    next(steps)
    finish()
    for _ in steps:
        pass
    for c in metas:
        c.wait_send()


def _query_kernel(n_cols, q_ref, q_all, x_sem):
    _signal_all(_x_peers(n_cols))
    for _ in _q_gather(n_cols, q_ref, q_all, x_sem):
        pass


def _attn_kernel(steps, group, heads, q_ref, k_ref, v_ref, mk_ref, mv_ref, qsel_ref, cell_ref, arr_ref, info_ref, o_ref, ml_ref, q_s, mk_s, mv_s, s_s, os_s, ml_s, ml_all):
    page, _, dim, n_slots = k_ref.shape[1:]
    n_seq = qsel_ref.shape[0]
    n_core, n_x, _, home = o_ref.shape[:4]
    n_arr = arr_ref.shape[0]
    pid = pl.program_id(0)
    n_rt = steps * group
    width = page * dim
    used = info_ref[0:1, :]
    limit = info_ref[1:2, :]
    freed = info_ref[2:3, 0:n_slots] > 0
    cells = cell_ref[...]
    owned = _dot(jnp.ones((8, LANES), BF16), cells, NT)[0:1] > 0
    scale = dim ** -0.5
    q_sel = qsel_ref[...]

    @pl.when(pid == 0)
    def _():
        ml_all[...] = jnp.zeros_like(ml_all)

    for t in range(steps):
        q_s[t] = _dot(q_ref[:, t].reshape(n_seq, heads * group * dim), q_sel, TN)
    tops, sums = [[] for _ in range(steps)], [[] for _ in range(steps)]
    for h in range(heads):
        for pages, full in ((mk_ref, mk_s), (mv_ref, mv_s)):
            full[...] = _dot(pages[:, 0, :, h * width:(h + 1) * width].reshape(n_arr, width), arr_ref[...], TN).reshape(page, dim, LANES)

        def join(tok, _, h=h):
            for pool, full in ((k_ref, mk_s), (v_ref, mv_s)):
                full[tok, :, 0:n_slots] = jnp.where(freed, full[tok, :, 0:n_slots], pool[0, tok, h].astype(F32))
            return 0

        lax.fori_loop(0, page, join, 0, unroll=4)

        def score(pair, _, h=h):
            toks = [pair * 2, pair * 2 + 1]
            keys = [mk_s[tok] for tok in toks]
            for t in range(steps):
                for r in range(group):
                    q_row = q_s[t, (h * group + r) * dim:(h * group + r + 1) * dim, :]
                    for tok, key in zip(toks, keys):
                        s_s[t * group + r, pl.ds(tok, 1), :] = jnp.sum(key * q_row, axis=0, keepdims=True)
            return 0

        lax.fori_loop(0, page // 2, score, 0)
        visible = lax.broadcasted_iota(I32, (page, LANES), 0).astype(F32) <= limit
        for rt in range(n_rt):
            sc = jnp.where(visible, s_s[rt] * scale, NEG)
            top = jnp.max(sc, axis=0, keepdims=True)
            ex = jnp.where(visible, jnp.exp(sc - top), 0.0)
            s_s[rt] = ex
            ml_s[rt:rt + 1, :] = top
            ml_s[n_rt + rt:n_rt + rt + 1, :] = jnp.sum(ex, axis=0, keepdims=True)
        live = (used > 0) & (limit >= 0)
        m_slot = ml_s[0:n_rt]
        l_slot = ml_s[n_rt:2 * n_rt]
        m_cell = jnp.where(owned, _pick_lhs(m_slot, cells, NT), NEG)
        m_seq = m_cell[:, 0:n_seq]
        for j in range(1, cells.shape[0] // n_seq):
            m_seq = jnp.maximum(m_seq, m_cell[:, j * n_seq:(j + 1) * n_seq])
        m_back = _pick_lhs(m_seq, q_sel, NN)
        w_slot = jnp.where(live, jnp.exp(jnp.minimum(m_slot - m_back, 0.0)), 0.0)
        l_seq = _pick_lhs(l_slot * w_slot, q_sel, NT)
        for t in range(steps):
            tops[t].append(m_seq[t * group:(t + 1) * group])
            sums[t].append(l_seq[t * group:(t + 1) * group])
        for rt in range(n_rt):
            s_s[rt] = s_s[rt] * w_slot[rt:rt + 1]

        def weigh(c, _):
            row = pl.multiple_of(c * 8, 8)
            acc = [jnp.zeros((8, LANES), F32) for _ in range(n_rt)]
            for tok in range(page):
                vals = mv_s[tok, pl.ds(row, 8), :]
                for rt in range(n_rt):
                    acc[rt] = acc[rt] + s_s[rt, tok:tok + 1, :] * vals
            for rt in range(n_rt):
                os_s[pl.ds(rt * dim + row, 8), :] = acc[rt]
            return 0

        lax.fori_loop(0, dim // 8, weigh, 0)
        for t in range(steps):
            part = _pick_rhs(q_sel, os_s[t * group * dim:(t + 1) * group * dim, :], NT).reshape(n_x, n_core, home, group * dim)
            for c in range(n_core):
                o_ref[c, :, t, :, h * group * dim:(h + 1) * group * dim] = part[:, c]

    n_row = heads * group
    for t in range(steps):
        ml_all[t, pl.ds(pl.multiple_of(pid * n_row, n_row), n_row), :] = jnp.concatenate(tops[t], axis=0)
        ml_all[t, pl.ds(pl.multiple_of((pl.num_programs(0) + pid) * n_row, n_row), n_row), :] = jnp.concatenate(sums[t], axis=0)

    @pl.when(pid == pl.num_programs(0) - 1)
    def _():
        for t in range(steps):
            flat = ml_all[t].T.reshape(n_x, n_core, home, ml_all.shape[1])
            for c in range(n_core):
                ml_ref[c, :, t] = flat[:, c]


def _exchange_kernel(n_cols, n_rows, heads, dim, has_pages, *refs):
    o_ref, ml_ref, q_ref, kv_ref = refs[:I4]
    n_in = I5 if has_pages else I4
    n_out = I3 if has_pages else I2
    out_ref, done_ref = refs[n_in:n_in + I2]
    done_ref[...] = jnp.zeros_like(done_ref)
    rp_o, rp_ml, cur_o, cur_ml, rel_o, rel_ml, fin_o, fin_ml, spread, expand, p_sem, r_sem, y_sem = refs[n_in + n_out:]
    n_x = n_cols // I2
    home = q_ref.shape[I0] // I2
    width = heads * dim
    at = lax.axis_index('kv')
    x, core = at // I2, at % I2
    up, dn, far = (x + I1) % n_x, (x + n_x - I1) % n_x, (x + I2) % n_x
    to_up, to_dn, to_pal = {'kv': up * I2 + core}, {'kv': dn * I2 + core}, {'kv': x * I2 + I1 - core}
    _signal_all(_x_peers(n_cols) + (_y_peers(n_rows) if has_pages else []))
    order = [far, up, dn, x]
    pals = []
    for i, pos in enumerate(order):
        pals.append(_copy(o_ref.at[I1 - core, pos], rp_o.at[i], p_sem, i, to_pal))
        pals.append(_copy(ml_ref.at[I1 - core, pos], rp_ml.at[i], p_sem, I4 + i, to_pal))
    for c in pals:
        c.start()
    if has_pages:
        pages_ref, pages_all = refs[I4], refs[n_in + I2]
        y_start, y_forward, y_finish = _rows_on_y(pages_ref, pages_all, y_sem, _half0)
        y_start()
        pages_all[lax.axis_index('kv2')] = pages_ref[...]

    n_chunk = I4
    cw = width // n_chunk
    kv_w = kv_ref.shape[I1] // I2
    kw = kv_w // n_chunk
    spread[...] = (lax.broadcasted_iota(I32, spread.shape, I1) // dim == lax.broadcasted_iota(I32, spread.shape, I0)).astype(F32).astype(BF16)
    lane = lax.broadcasted_iota(I32, expand.shape, I1)
    row = lax.broadcasted_iota(I32, expand.shape, I0)
    group = cw // kw
    expand[...] = ((lane // (dim * group) == row // dim) & (lane % dim == row % dim)).astype(F32).astype(BF16)

    s = jnp.zeros((I3 * home, heads), F32)
    for c in range(n_chunk):
        q_c = q_ref[:, c * cw:(c + I1) * cw].astype(F32)
        k_c = _dot(kv_ref[:, c * kw:(c + I1) * kw], expand[...], NN)
        prod = jnp.concatenate([q_c[I0:home] * k_c[I0:home], q_c[home:] * k_c[I0:home], q_c[home:] * k_c[home:]], axis=I0)
        s = s + _pick_lhs(prod, spread[:, c * cw:(c + I1) * cw], NT)
    s = s * dim ** -0.5
    s00, s10, s11 = s[I0:home], s[home:I2 * home], s[I2 * home:]
    m1 = jnp.maximum(s10, s11)
    e10, e11 = jnp.exp(s10 - m1), jnp.exp(s11 - m1)
    self_m = [s00, m1]
    self_l = [jnp.ones_like(s00), e10 + e11]
    self_w = [[(I0, None)], [(I0, e10), (I1, e11)]]

    def stats(ref):
        return ref[:, I0:heads], ref[:, heads:I2 * heads]

    def fold(a_o, a_ml, b_o, b_ml, out_o, out_ml):
        am, al = stats(a_ml)
        bm, bl = stats(b_ml)
        top = jnp.maximum(am, bm)
        aw, bw = jnp.exp(am - top), jnp.exp(bm - top)
        out_ml[:, I0:heads] = top
        out_ml[:, heads:I2 * heads] = aw * al + bw * bl
        w = jnp.concatenate([aw, bw], axis=I0)

        def chunk(c, _):
            sl = pl.ds(pl.multiple_of(c * cw, cw), cw)
            wx = _pick_lhs(w, spread[:, sl], NN)
            out_o[:, sl] = a_o[:, sl] * wx[I0:home] + b_o[:, sl] * wx[home:]
            return c

        lax.fori_loop(I0, n_chunk, chunk, I0)

    cur_ml[...] = jnp.zeros_like(cur_ml)

    def fold_pal(i):
        _copy(o_ref.at[I1 - core, order[i]], rp_o.at[i], p_sem, i, to_pal).wait_recv()
        _copy(ml_ref.at[I1 - core, order[i]], rp_ml.at[i], p_sem, I4 + i, to_pal).wait_recv()
        for t in range(I2):
            fold(o_ref.at[core, order[i], t], ml_ref.at[core, order[i], t], rp_o.at[i, t], rp_ml.at[i, t], cur_o.at[i, t], cur_ml.at[i, t])

    sends = []

    def send(i, t, dst_o, dst_ml, k, dev):
        a = _copy(cur_o.at[i, t], dst_o, r_sem, I2 * k, dev)
        b = _copy(cur_ml.at[i, t], dst_ml, r_sem, I2 * k + I1, dev)
        a.start()
        b.start()
        sends.extend([a, b])

    def got(dst_o, dst_ml, k):
        _copy(dst_o, dst_o, r_sem, I2 * k, to_up).wait_recv()
        _copy(dst_ml, dst_ml, r_sem, I2 * k + I1, to_up).wait_recv()

    fold_pal(I0)
    send(I0, I0, rel_o.at[I0], rel_ml.at[I0], I0, to_up)
    send(I0, I1, rel_o.at[I1], rel_ml.at[I1], I1, to_dn)
    fold_pal(I1)
    send(I1, I1, fin_o.at[I0, I1], fin_ml.at[I0, I1], I2, to_up)
    fold_pal(I2)
    send(I2, I0, fin_o.at[I1, I0], fin_ml.at[I1, I0], I3, to_dn)
    got(rel_o.at[I0], rel_ml.at[I0], I0)
    fold(cur_o.at[I1, I0], cur_ml.at[I1, I0], rel_o.at[I0], rel_ml.at[I0], cur_o.at[I4, I0], cur_ml.at[I4, I0])
    send(I4, I0, fin_o.at[I0, I0], fin_ml.at[I0, I0], I4, to_up)
    got(rel_o.at[I1], rel_ml.at[I1], I1)
    fold(cur_o.at[I2, I1], cur_ml.at[I2, I1], rel_o.at[I1], rel_ml.at[I1], cur_o.at[I4, I1], cur_ml.at[I4, I1])
    send(I4, I1, fin_o.at[I1, I1], fin_ml.at[I1, I1], I5, to_dn)
    fold_pal(I3)
    if has_pages:
        y_forward()
    for side, t, k in ((I0, I1, I2), (I1, I0, I3), (I0, I0, I4), (I1, I1, I5)):
        got(fin_o.at[side, t], fin_ml.at[side, t], k)
    for t in range(I2):
        parts = [(cur_o.at[I3, t], cur_ml.at[I3, t]), (fin_o.at[I0, t], fin_ml.at[I0, t]), (fin_o.at[I1, t], fin_ml.at[I1, t])]
        ms = [stats(ml)[I0] for _, ml in parts] + [self_m[t]]
        ls = [stats(ml)[I1] for _, ml in parts] + [self_l[t]]
        top = functools.reduce(jnp.maximum, ms)
        ws = [jnp.exp(m - top) for m in ms]
        total = functools.reduce(jnp.add, [w * l for w, l in zip(ws, ls)])
        ws = [w / total for w in ws]
        own = ws.pop()
        ws += [own if e is None else own * e for _, e in self_w[t]]
        w = jnp.concatenate(ws, axis=I0)

        def close(c, _, t=t, parts=parts, w=w):
            sl = pl.ds(pl.multiple_of(c * cw, cw), cw)
            wx = _pick_lhs(w, spread[:, sl], NN)
            v_c = _dot(kv_ref[:, pl.ds(pl.multiple_of(kv_w + c * kw, kw), kw)], expand[...], NN)
            acc = jnp.zeros((home, cw), F32)
            for i, (o, _) in enumerate(parts):
                acc = acc + o[:, sl] * wx[i * home:(i + I1) * home]
            for i, (step, _) in enumerate(self_w[t]):
                acc = acc + v_c[step * home:(step + I1) * home] * wx[(I3 + i) * home:(I4 + i) * home]
            out_ref[t * home:(t + I1) * home, sl] = acc.astype(BF16)
            return c

        lax.fori_loop(I0, n_chunk, close, I0)
    if has_pages:
        y_finish()
    for c in pals + sends:
        c.wait_send()


def _place_kernel(steps, heads, n_alias, *refs):
    kn_ref, vn_ref, k_ref, v_ref, mk_ref, mv_ref, wsel_ref, mig_ref, info_ref = refs[:9]
    ko_ref, vo_ref, kv_s, full = refs[10 + n_alias:]
    page, _, dim, n_slots = k_ref.shape[1:]
    n_seq = wsel_ref.shape[0]
    width = page * dim
    n_all = mig_ref.shape[0]
    moved = info_ref[0:1, :]
    w_off = info_ref[1:2, :]
    for t in range(steps):
        for which, ref in enumerate((kn_ref, vn_ref)):
            kv_s[which, t] = _dot(ref[:, 0, t].reshape(n_seq, heads * dim), wsel_ref[...], TN).astype(BF16)

    def head(h, _):
        lanes = pl.ds(pl.multiple_of(h * width, width), width)
        for which, (pool, pages, out) in enumerate(((k_ref, mk_ref, ko_ref), (v_ref, mv_ref, vo_ref))):
            full[...] = _dot(pages[:, 0, :, lanes].reshape(n_all, width), mig_ref[...], TN).astype(BF16).reshape(page, dim, n_slots)

            def fill(tok, _, which=which, pool=pool, out=out):
                at = w_off - tok.astype(F32)
                new = [jnp.where(at == -float(t), 1.0, 0.0) for t in range(steps)]
                kept = 1.0 - functools.reduce(jnp.add, new)
                val = full[tok] * kept.astype(BF16) + pool[0, tok, h] * (kept * (1.0 - moved)).astype(BF16)
                rows = pl.ds(pl.multiple_of(h * dim, dim), dim)
                for t in range(steps):
                    val = val + kv_s[which, t, rows, :] * new[t].astype(BF16)
                out[0, tok, h] = val
                return 0

            lax.fori_loop(0, page, fill, 0, unroll=4)
        return 0

    lax.fori_loop(0, heads, head, 0)


def solution(mesh):
    n_rows, n_cols = mesh.shape['kv2'], mesh.shape['kv']
    dev_axes = ('rep', 'kv2', 'kv')
    group_axes = ('kv2', 'kv')
    seq_spec = P(None, dev_axes, None)
    pool_spec = P(dev_axes, None, None, None, None)
    table_spec = P(dev_axes, None)
    vec_spec = P(dev_axes)
    full_spec = P()
    pair = 2
    vmem = pl.BlockSpec(memory_space=pltpu.VMEM)
    dma = pltpu.SemaphoreType.DMA

    def per_device(x_embed, w_query, w_key, w_value, w_out, w_up, w_down, k_pool, v_pool, old_table, seq_len, src_slot, dst_slot):
        n_slots, layers, page, kv_heads, dim = k_pool.shape
        steps, seq_dev, width = x_embed.shape
        heads = w_query.shape[2] // dim
        group = heads // kv_heads
        n_pages = old_table.shape[1]
        n_seq = seq_dev * n_cols
        n_move = src_slot.shape[0]
        n_rt = steps * group
        n_grid = kv_heads // pair
        page_w = page * dim
        n_x = n_cols // 2
        n_dev = n_rows * n_cols
        rows = steps * seq_dev
        me = lax.axis_index('kv2') * n_cols + lax.axis_index('kv')
        slot_base = me * n_slots
        k_t, v_t = (pltpu.with_memory_space_constraint(jnp.transpose(a, (1, 2, 3, 4, 0)), pltpu.HBM) for a in (k_pool, v_pool))
        q_w, kv_w, m_w = pair * group * dim, pair * dim, pair * page_w

        def fixed(shape):
            return pl.BlockSpec(shape, lambda i: (0,) * len(shape), pipeline_mode=pl.Buffered(1))

        src_hot = ((src_slot - slot_base)[:, None] == jnp.arange(n_slots, dtype=I32)[None, :]).astype(BF16)
        page_shape = (2, n_move, kv_heads * page_w)

        def pool_blk(layer):
            return pl.BlockSpec((1, page, pair, dim, n_slots), lambda i: (layer, 0, i, 0, 0))

        page_blk = pl.BlockSpec((2, n_move, m_w), lambda i: (0, 0, i))
        flat = jax.ShapeDtypeStruct(page_shape, BF16)
        packed = pl.pallas_call(
            functools.partial(_pack_kernel, pair),
            grid=(n_grid,),
            in_specs=[pl.BlockSpec((n_move, n_slots), lambda i: (0, 0))] + [pool_blk(l) for l in range(layers) for _ in (k_t, v_t)],
            out_specs=[page_blk] * layers,
            out_shape=[flat] * layers,
            cost_estimate=_cost(8, 16),
            name='pack_pages',
        )(src_hot, *[a for _ in range(layers) for a in (k_t, v_t)])

        def whole(i, after):
            page, token = (packed[i], src_hot) if after is None else lax.optimization_barrier((packed[i], after))
            return lax.all_gather(page, group_axes), token

        def project(hidden, layer):
            q = jnp.dot(hidden, w_query[layer], preferred_element_type=F32).astype(BF16)
            kv = jnp.concatenate([jnp.dot(hidden, w[layer], preferred_element_type=F32).astype(BF16) for w in (w_key, w_value)], axis=1)
            return q, kv

        hidden = x_embed.reshape(rows, width)
        q, kv = project(hidden, 0)
        y, at = lax.axis_index('kv2'), lax.axis_index('kv')
        n_all = n_dev * n_move
        n_arr = n_rows * n_move

        def own_place(v):
            wide = jnp.tile(v, n_cols)[None, :]
            lane = jnp.arange(n_cols * n_move, dtype=I32)[None, :] // n_move
            return jnp.where((lane == at) & (jnp.arange(8, dtype=I32)[:, None] == y), wide, 0)

        tab = jnp.concatenate([old_table.T.reshape(-1), seq_len])[None, :]
        meta = jnp.concatenate([jnp.where(jnp.arange(8, dtype=I32)[:, None] == 0, tab, 0), own_place(src_slot), own_place(dst_slot)], axis=0)
        pages_all_shape = jax.ShapeDtypeStruct((n_rows,) + page_shape, BF16)
        done_shape = jax.ShapeDtypeStruct((8, 128), F32)
        q_all_shape = jax.ShapeDtypeStruct((n_cols, rows, heads * dim), BF16)
        dims = (n_rows, n_cols, n_slots, n_pages, page, seq_dev)
        pages_y, q_all, q_sel, cells, arr, info, w_sel, mig, w_info = pl.pallas_call(
            functools.partial(_head_kernel, dims),
            in_specs=[vmem] * 5,
            out_specs=[vmem] * 9,
            out_shape=[
                pages_all_shape,
                q_all_shape,
                jax.ShapeDtypeStruct((n_seq, LANES), BF16),
                jax.ShapeDtypeStruct((n_pages * n_seq, LANES), BF16),
                jax.ShapeDtypeStruct((n_arr, LANES), BF16),
                jax.ShapeDtypeStruct((8, LANES), F32),
                jax.ShapeDtypeStruct((n_seq, n_slots), BF16),
                jax.ShapeDtypeStruct((n_all, n_slots), BF16),
                jax.ShapeDtypeStruct((8, n_slots), F32),
            ],
            scratch_shapes=[pltpu.VMEM((n_dev,) + meta.shape, I32), dma((2, n_dev - 1)), dma((2, 6)), dma((2, 13))],
            compiler_params=pltpu.CompilerParams(collective_id=0, has_side_effects=True, vmem_limit_bytes=24 * MIB),
            cost_estimate=_cost(10, 4),
            name='head_gather',
        )(meta, packed[0], q, src_slot.reshape(1, -1), src_slot.reshape(-1, 1))

        def attend(layer, q_all, pages):
            blk = pool_blk(layer)
            ml_rows = 2 * LANES // 4
            return pl.pallas_call(
                functools.partial(_attn_kernel, steps, group, pair),
                grid=(n_grid,),
                in_specs=[
                    pl.BlockSpec((n_cols, steps, seq_dev, q_w), lambda i: (0, 0, 0, i)),
                    blk, blk,
                    pl.BlockSpec((n_rows, 1, n_move, m_w), lambda i: (0, 0, 0, i)),
                    pl.BlockSpec((n_rows, 1, n_move, m_w), lambda i: (0, 1, 0, i)),
                    fixed(q_sel.shape), fixed(cells.shape), fixed(arr.shape), fixed(info.shape),
                ],
                out_specs=[
                    pl.BlockSpec((2, n_x, steps, seq_dev, q_w), lambda i: (0, 0, 0, 0, i)),
                    pl.BlockSpec((2, n_x, steps, seq_dev, ml_rows), lambda i: (0, 0, 0, 0, 0)),
                ],
                out_shape=[
                    jax.ShapeDtypeStruct((2, n_x, steps, seq_dev, heads * dim), F32),
                    jax.ShapeDtypeStruct((2, n_x, steps, seq_dev, ml_rows), F32),
                ],
                scratch_shapes=[
                    pltpu.VMEM((steps, q_w, LANES), F32),
                    pltpu.VMEM((page, dim, LANES), F32),
                    pltpu.VMEM((page, dim, LANES), F32),
                    pltpu.VMEM((n_rt, page, LANES), F32),
                    pltpu.VMEM((n_rt * dim, LANES), F32),
                    pltpu.VMEM((2 * n_rt, LANES), F32),
                    pltpu.VMEM((steps, ml_rows, n_seq), F32),
                ],
                compiler_params=pltpu.CompilerParams(vmem_limit_bytes=32 * MIB),
                cost_estimate=_cost(20, 16),
                name='slot_attention',
            )(q_all.reshape(n_cols, steps, seq_dev, heads * dim), k_t, v_t, pages, pages, q_sel, cells, arr, info)

        def exchange(layer, o, ml, q, kv, pages):
            has = pages is not None
            half = (seq_dev, heads * dim)
            stat = (seq_dev, ml.shape[-1])
            out_shape = [jax.ShapeDtypeStruct((rows, heads * dim), BF16), done_shape] + ([pages_all_shape] if has else [])
            return pl.pallas_call(
                functools.partial(_exchange_kernel, n_cols, n_rows, heads, dim, has),
                in_specs=[vmem] * (5 if has else 4),
                out_specs=[vmem] * len(out_shape),
                out_shape=out_shape,
                scratch_shapes=[
                    pltpu.VMEM((4, steps) + half, F32), pltpu.VMEM((4, steps) + stat, F32),
                    pltpu.VMEM((5, steps) + half, F32), pltpu.VMEM((5, steps) + stat, F32),
                    pltpu.VMEM((2,) + half, F32), pltpu.VMEM((2,) + stat, F32),
                    pltpu.VMEM((2, steps) + half, F32), pltpu.VMEM((2, steps) + stat, F32),
                    pltpu.VMEM((heads, heads * dim), BF16), pltpu.VMEM((kv_w, q_w), BF16),
                    dma((2, 8)), dma((2, 12)), dma((2, 6)),
                ],
                compiler_params=pltpu.CompilerParams(collective_id=1 + layer, has_side_effects=True, vmem_limit_bytes=32 * MIB),
                cost_estimate=_cost(10, 4),
                name='exchange_partials',
            )(o, ml, q, kv, *([pages] if has else []))

        kv_all, moved, done = [], [], None
        for layer in range(layers):
            if layer:
                q, kv = project(hidden, layer)
                [q_all] = pl.pallas_call(
                    functools.partial(_query_kernel, n_cols),
                    in_specs=[vmem],
                    out_specs=[vmem],
                    out_shape=[q_all_shape],
                    scratch_shapes=[dma((2, 13))],
                    compiler_params=pltpu.CompilerParams(collective_id=1 + layers + layer, has_side_effects=True, vmem_limit_bytes=16 * MIB),
                    cost_estimate=_cost(5, 4),
                    name='query_gather',
                )(q)
            kv_all.append(kv)
            if layer + 1 == layers:
                kv_rows = lax.all_gather(jnp.stack(kv_all), 'kv')
                kv_rows = kv_rows.reshape(n_cols, layers, steps, seq_dev, -1)
            o, ml = attend(layer, q_all, pages_y)
            nxt = packed[layer + 1] if layer + 1 < layers else None
            moved.append(whole(layer, done))
            attn, done, *more = exchange(layer, o, ml, q, kv, nxt)
            pages_y = more[0] if more else None
            hidden = (hidden.astype(F32) + jnp.dot(attn, w_out[layer], preferred_element_type=F32)).astype(BF16)
            up_act = jax.nn.gelu(jnp.dot(hidden, w_up[layer], preferred_element_type=F32)).astype(BF16)
            hidden = (hidden.astype(F32) + jnp.dot(up_act, w_down[layer], preferred_element_type=F32)).astype(BF16)
        v_at = kv_heads * dim // kv_w
        outs = []
        for layer in range(layers):
            blk = pool_blk(layer)
            pages, token = moved[layer]
            specs = [
                pl.BlockSpec((n_cols, 1, steps, seq_dev, kv_w), lambda i, layer=layer: (0, layer, 0, 0, i)),
                pl.BlockSpec((n_cols, 1, steps, seq_dev, kv_w), lambda i, layer=layer: (0, layer, 0, 0, v_at + i)),
                blk, blk,
            ] + [pl.BlockSpec((n_dev, 1, n_move, m_w), lambda i, which=which: (0, which, 0, i)) for which in range(2)] + [fixed(a.shape) for a in (w_sel, mig, w_info)]
            outs = pl.pallas_call(
                functools.partial(_place_kernel, steps, pair, len(outs)),
                grid=(n_grid,),
                in_specs=specs + [pl.BlockSpec(memory_space=pl.ANY)] * (1 + len(outs)),
                out_specs=[blk, blk],
                out_shape=[jax.ShapeDtypeStruct(a.shape, BF16) for a in (k_t, v_t)],
                scratch_shapes=[pltpu.VMEM((2, steps, kv_w, n_slots), BF16), pltpu.VMEM((page, dim, n_slots), BF16)],
                input_output_aliases={len(specs) + 1 + i: i for i in range(len(outs))},
                compiler_params=pltpu.CompilerParams(vmem_limit_bytes=60 * MIB),
                cost_estimate=_cost(20, 32),
                name='place_pages',
            )(kv_rows, kv_rows, k_t, v_t, pages, pages, w_sel, mig, w_info, token, *outs)
        k_out, v_out = outs
        y_out = hidden.reshape(steps, seq_dev, width)
        back = (4, 0, 1, 2, 3)
        return y_out, jnp.transpose(k_out, back), jnp.transpose(v_out, back)

    return jax.shard_map(per_device, mesh=mesh, in_specs=(seq_spec, full_spec, full_spec, full_spec, full_spec, full_spec, full_spec, pool_spec, pool_spec, table_spec, vec_spec, vec_spec, vec_spec), out_specs=(seq_spec, pool_spec, pool_spec), check_vma=False)
```
